32 devices in a mesh: gy: 8 (over z, x), gx: 4 (over y, core).
Axes of the slice: x: 2, y: 2, z: 4, core: 2. Of those that a mesh axis runs over, the one named last changes fastest.
Arguments:
- ensemble: bfloat16 [32, 2, 512, 512], P(None, None, 'gy', 'gx'), may hold values from -1.1953125 to 1.1953125
- obs_cell: int32 [8, 4, 2048], P('gy', 'gx'), may hold values from 0 to 8191
- obs_level: int32 [8, 4, 2048], P('gy', 'gx'), may hold values from 0 to 1
- innovation: float32 [8, 4, 2048], P('gy', 'gx'), may hold values from -6 to 6
- obs_weight: float32 [8, 4, 2048], P('gy', 'gx'), may hold values from 0.5 to 4
Outputs:
- control: float32 [32, 2, 512, 512], P(None, None, 'gy', 'gx')
- increment: float32 [2, 512, 512], P(None, 'gy', 'gx')
The draws below stay inside these ranges and needn't reach their ends.
Inputs may be any that keep to these rules, and one draw needn't show every extreme that they name: obs_cell holds row * 128 + column of the observation within its device's block of 64 x 128 cells.
All inputs are finite; a program needn't handle non-finite values.
Results may differ from the reference program's by a relative error of at most 0.0003.
Values sent between devices are 32-bit elements; how exact they have to be, the bound alone decides.
No kernel may reach another device: no remote copies, remote signals or barrier semaphores. Data moves between devices by JAX's collectives and lax.ppermute only.
A program may use at most 128 MiB of HBM per device.

```python
import math
import jax
import jax.numpy as jnp
from jax import lax

MEMBERS = 32
LEV = 2
SWEEPS = 4
CY = 64
CX = 128
OBS_DEV = 2048
NY = 512
NX = 512
N_GY = 8
N_GX = 4


def place_ends(result, key, smallest, high):
    dims = result.shape
    place = [jax.random.randint(jax.random.fold_in(key, axis), (), 0, dims[axis]) for axis in range(len(dims))]
    result = result.at[tuple(place)].set(smallest)
    longest = dims.index(max(dims))
    place[longest] = (place[longest] + 1) % dims[longest]
    return result.at[tuple(place)].set(high)


def block_scale(stream_key, dims, split, low, top_value):
    level = 1.0
    for axis_at, parts in split:
        draws = jax.random.uniform(jax.random.fold_in(jax.random.fold_in(stream_key, 6), axis_at), (parts,), jnp.float32, low / len(split), top_value / len(split))
        level = level * jnp.repeat(jnp.exp(draws), dims[axis_at] // parts).reshape((-1,) + (1,) * (len(dims) - 1 - axis_at))
    return level


def centred(stream_key, shape, scale, reach, cuts=(), kind=jnp.bfloat16):
    entries = scale * jax.random.normal(stream_key, shape, jnp.float32)
    if cuts:
        entries = entries * block_scale(stream_key, shape, cuts, -0.22, 0.18)
    return jnp.clip(entries, -reach, reach).astype(kind)


def setup_inputs(seed: int = 0) -> dict:
    keys = jax.random.split(jax.random.key(seed), 6)
    return {
        "ensemble": centred(keys[0], (MEMBERS, LEV, NY, NX), 0.2, 1.1953125, ((2, 8), (3, 4))),
        "obs_cell": place_ends(jax.random.randint(keys[1], (N_GY, N_GX, OBS_DEV), 0, CY * CX), jax.random.fold_in(keys[1], 1), 0, (CY * CX) - 1).astype(jnp.int32),
        "obs_level": place_ends(jax.random.randint(keys[2], (N_GY, N_GX, OBS_DEV), 0, LEV), jax.random.fold_in(keys[2], 1), 0, LEV - 1).astype(jnp.int32),
        "innovation": centred(keys[3], (N_GY, N_GX, OBS_DEV), 1.0, 6.0, ((0, 8), (1, 4)), jnp.float32),
        "obs_weight": jnp.clip(jnp.exp(math.log(4.0) - 2.0794415 * jax.random.uniform(keys[4], (N_GY, N_GX, OBS_DEV), jnp.float32) ** block_scale(keys[4], (N_GY, N_GX, OBS_DEV), ((0, 8), (1, 4)), -0.2, 0.2)), 0.5, 4.0),
    }


KAPPA = 0.2
EPS = 1e-06

def smooth_once(field):
    padded = jnp.pad(field, ((0, 0), (0, 0), (1, 1), (1, 1)))
    beside_all = padded[:, :, 2:, 1:-1] + padded[:, :, :-2, 1:-1] + padded[:, :, 1:-1, 2:] + padded[:, :, 1:-1, :-2]
    return field + KAPPA * (beside_all - 4.0 * field)

def filtered(field):
    for sweep in range(SWEEPS):
        field = smooth_once(field)
    return field

def reference(ensemble, obs_cell, obs_level, innovation, obs_weight):
    block_row = jnp.arange(N_GY, dtype=jnp.int32)[:, None, None]
    block_col = jnp.arange(N_GX, dtype=jnp.int32)[None, :, None]
    rows = block_row * CY + obs_cell // CX
    cols = block_col * CX + obs_cell % CX
    points = (obs_level * (NY * NX) + rows * NX + cols).reshape(-1).astype(jnp.int32)
    weights = obs_weight.reshape(-1)
    members = ensemble.astype(jnp.float32)

    def adjoint_obs(values):
        state = jnp.zeros((LEV * NY * NX,), jnp.float32).at[points].add(values)
        return state.reshape(LEV, NY, NX)

    def hessian(vector):
        state = lax.optimization_barrier(jnp.sum(members * filtered(vector), axis=0))
        seen = state.reshape(-1)[points]
        back = filtered(members * adjoint_obs(weights * seen)[None])
        return (vector + back, state)
    gradient = filtered(members * adjoint_obs(weights * innovation.reshape(-1))[None])
    bnorm = jnp.sqrt(jnp.sum(gradient * gradient) + EPS)
    first = gradient / bnorm
    image_one, state_one = hessian(first)
    alpha_one = jnp.sum(first * image_one)
    remain = image_one - alpha_one * first
    beta = jnp.sqrt(jnp.sum(remain * remain) + EPS)
    second = remain / beta
    image_two, state_two = hessian(second)
    alpha_two = jnp.sum(second * image_two)
    determ = alpha_one * alpha_two - beta * beta
    coef_one = bnorm * alpha_two / determ
    coef_two = -bnorm * beta / determ
    control = coef_one * first + coef_two * second
    increment = coef_one * state_one + coef_two * state_two
    return (control, increment)
```

```python
import functools
import math

import jax
import jax.numpy as jnp
import numpy as np
from jax import lax
from jax.experimental import pallas as pl
from jax.experimental.pallas import tpu as pltpu
from jax.sharding import PartitionSpec as P

SWEEPS = 4
KAPPA = 0.2
EPS = 1e-06
HALO = 2 * SWEEPS
SLOT = 4 * HALO
VMEM = pl.BlockSpec(memory_space=pltpu.VMEM)
F32 = jnp.float32
BF16 = jnp.bfloat16


def band_matrices(lanes):
    out = np.zeros((4, 2, lanes, SWEEPS * lanes), np.float32)
    lane = np.arange(lanes)
    for variant in range(4):
        for kind in range(2):
            col = lane - HALO if kind == 0 else lanes - 3 * HALO + lane % SLOT
            inside = np.ones(lanes, bool)
            if variant % 2:
                inside &= col >= 0
            if variant // 2:
                inside &= col < lanes
            near = np.abs(lane[:, None] - lane[None, :]) <= 1
            if kind == 1:
                near &= (lane[:, None] // SLOT) == (lane[None, :] // SLOT)
            band = (near & inside[:, None] & inside[None, :]).astype(np.float64)
            unit = np.diag(inside.astype(np.float64))
            power = [unit]
            for _ in range(SWEEPS):
                power.append(power[-1] @ band)
            for j in range(SWEEPS):
                q = sum(
                    math.comb(SWEEPS, k) * math.comb(SWEEPS - k, (SWEEPS - k - j) // 2) * power[k]
                    for k in range(SWEEPS - j + 1)
                    if (SWEEPS - k - j) % 2 == 0
                )
                out[variant, kind, :, j * lanes : (j + 1) * lanes] = q
    return out


def shift(x, axis, step):
    count = lax.axis_size(axis)
    return lax.ppermute(x, axis, [(i, i + step) for i in range(count) if 0 <= i + step < count])


def scatter_kernel(ens, cell, level, innov, weight, grid, up, down):
    members, levels, rows, cols = ens.shape
    obs = cell.shape[1]
    span = 256
    row_iota = lax.broadcasted_iota(jnp.int32, (levels * rows, span), 0)
    col_iota = lax.broadcasted_iota(jnp.int32, (cols, span), 0)
    acc = jnp.zeros((4 * levels * rows, cols), F32)
    for start in range(0, obs, span):
        at = slice(start, start + span)
        point = level[:, at] * rows + cell[:, at] // cols
        here = row_iota == point
        w = weight[:, at]
        parts = []
        for value in (w * innov[:, at], w):
            high = value.astype(BF16).astype(F32)
            parts += [high, value - high]
        left = jnp.concatenate([jnp.where(here, part, 0.0).astype(BF16) for part in parts], axis=0)
        right = jnp.where(col_iota == cell[:, at] % cols, 1.0, 0.0).astype(BF16)
        acc += lax.dot_general(left, right, (((1,), (1,)), ((), ())), preferred_element_type=F32)
    n = levels * rows
    g = acc[:n] + acc[n : 2 * n]
    d = acc[2 * n : 3 * n] + acc[3 * n :]
    fields = members * levels
    for l in range(levels):
        grid[0, l] = g[l * rows : (l + 1) * rows]
        grid[1, l] = d[l * rows : (l + 1) * rows]
        up[fields + l] = g[l * rows : l * rows + HALO]
        down[fields + l] = g[(l + 1) * rows - HALO : (l + 1) * rows]

    def edge(m, _):
        for l in range(levels):
            up[l * members + m] = ens[m, l, 0:16, :].astype(F32)[:HALO]
            down[l * members + m] = ens[m, l, rows - 16 : rows, :].astype(F32)[16 - HALO :]
        return 0

    lax.fori_loop(0, members, edge, 0)


def slot_lane(t):
    return SLOT * (t % 4) + HALO * (t // 4)


def reflect(ext, first, count, rows, sign):
    me = lax.axis_index("gy")

    def one(f, base, step):
        for j in range(1, HALO):
            ext[f, pl.ds(base - step * j, 1), :] = sign * ext[f, pl.ds(base + step * j, 1), :]
        if sign < 0:
            ext[f, pl.ds(base, 1), :] = jnp.zeros((1, ext.shape[2]), F32)

    def loop(base, step):
        def body(f, _):
            one(first + f, base, step)
            return 0

        lax.fori_loop(0, count, body, 0)

    pl.when(me == 0)(lambda: loop(HALO - 1, 1))
    pl.when(me == lax.axis_size("gy") - 1)(lambda: loop(HALO + rows, -1))


def pack_sides(ext, fields, lane):
    west = jnp.zeros(ext.shape[1:], F32)
    east = west
    for t, f in enumerate(fields):
        base = slot_lane(t)
        here = (lane >= base) & (lane < base + HALO)
        x = ext[f]
        west = jnp.where(here, pltpu.roll(x, base, 1) if base else x, west)
        east = jnp.where(here, pltpu.roll(x, (base + HALO) % x.shape[1], 1), east)
    return west, east


def sides_kernel(ens, grid, north, south, ext, west, east):
    members, levels, rows, cols = ens.shape
    fields = members * levels
    reach = rows + 2 * HALO

    def fill(m, _):
        for l in range(levels):
            ext[l * members + m, HALO : HALO + rows, :] = ens[m, l].astype(F32)
        return 0

    lax.fori_loop(0, members, fill, 0)
    for l in range(levels):
        ext[fields + l, HALO : HALO + rows, :] = grid[0, l]

    def ends(f, _):
        ext[f, 0:HALO, :] = north[f]
        ext[f, HALO + rows : reach, :] = south[f]
        return 0

    lax.fori_loop(0, fields + levels, ends, 0)
    reflect(ext, 0, fields, rows, 1.0)
    reflect(ext, fields, levels, rows, -1.0)
    lane = lax.broadcasted_iota(jnp.int32, (reach, cols), 1)

    def pack(p, _):
        w, e = pack_sides(ext, [p * 16 + t for t in range(16)], lane)
        west[p] = w
        east[p] = e
        return 0

    lax.fori_loop(0, fields // 16, pack, 0)
    w, e = pack_sides(ext, [fields + l for l in range(levels)], lane)
    west[fields // 16] = w
    east[fields // 16] = e


def grid_sides_kernel(p, north, south, ext, west, east):
    levels, rows, cols = p.shape
    for l in range(levels):
        ext[l, HALO : HALO + rows, :] = p[l]
        ext[l, 0:HALO, :] = north[l]
        ext[l, HALO + rows :, :] = south[l]
    reflect(ext, 0, levels, rows, -1.0)
    lane = lax.broadcasted_iota(jnp.int32, ext.shape[1:], 1)
    west[...], east[...] = pack_sides(ext, list(range(levels)), lane)


def spread_grid(gbuf, g, west, east, lane, l, scale):
    base = slot_lane(l)
    cols = g.shape[1]
    main = jnp.where(lane < HALO, pltpu.roll(west, (cols - base) % cols, 1) if base else west, pltpu.roll(g, HALO, 1))
    gbuf[l, 0] = main * scale
    one = jnp.where(lane < 3 * HALO, pltpu.roll(g, 3 * HALO, 1), pltpu.roll(east, (3 * HALO - base) % cols, 1))
    one = jnp.where(lane < SLOT, one, 0.0)
    one = one + pltpu.roll(one, SLOT, 1)
    gbuf[l, 1] = (one + pltpu.roll(one, 2 * SLOT, 1)) * scale


def band_products(lhs, bands, kind, out, count):
    lanes = lhs.shape[1] // 2
    for half in range(SWEEPS // 2):
        r = jnp.dot(
            lhs[0:count, :],
            bands[kind, :, half * 2 * lanes : (half + 1) * 2 * lanes],
            preferred_element_type=F32,
        )
        out[2 * half, 0:count, :] = r[:, :lanes]
        out[2 * half + 1, 0:count, :] = r[:, lanes:]


def split_into(lhs, start, x):
    count, lanes = x.shape
    high = x.astype(BF16)
    lhs[start : start + count, 0:lanes] = high
    lhs[start : start + count, lanes : 2 * lanes] = (x - high.astype(F32)).astype(BF16)


def combine(prod, start, src, f, count):
    def part(k, off):
        return prod[k, pl.ds(start + off, count), :]

    s = SWEEPS
    total = src[f, pl.ds(2 * s, count), :] + src[f, pl.ds(0, count), :]
    for k in range(1, s):
        total += part(k, s + k) + part(k, s - k)
    return total + part(0, s)


def covariance(pack, bands, gbuf, z, fbuf, prod, lhs, xacc, batch, build):
    total, reach, lanes = pack.shape
    inner = reach - HALO
    rows = reach - 2 * HALO
    levels = gbuf.shape[0]
    xacc[...] = jnp.zeros_like(xacc)

    def run(b, kind, level_of):
        for i in range(batch):
            if build is not None:
                pack[b * batch + i] = build(b, i, kind)
            f = pack[b * batch + i] * gbuf[level_of(i), kind]
            fbuf[i] = f
            split_into(lhs, i * reach, f)
        band_products(lhs, bands, kind, prod, batch * reach)
        for i in range(batch):
            v = combine(prod, i * reach, fbuf, i, inner)
            z[b * batch + i] = v
            split_into(lhs, i * inner, v)
        band_products(lhs, bands, kind, prod, batch * inner)
        for i in range(batch):
            v = combine(prod, i * inner, z, b * batch + i, rows)
            xacc[level_of(i), kind] += v * pack[b * batch + i, HALO : HALO + rows, :]

    windows = total // 5
    mains = total - windows
    per_level = mains // levels // batch

    def step(b, _):
        run(b, 0, lambda i: b // per_level)
        return 0

    lax.fori_loop(0, mains // batch, step, 0)
    for b in range(mains // batch, total // batch):
        run(b, 1, lambda i, b=b: (b * batch + i - mains) * levels // windows)


def gather_state(xacc, l, lane):
    main, win = xacc[l, 0], xacc[l, 1]
    cols = main.shape[1]
    win = win + pltpu.roll(win, 2 * SLOT, 1)
    win = win + pltpu.roll(win, SLOT, 1)
    return KAPPA**SWEEPS * jnp.where(lane < cols - 2 * HALO, pltpu.roll(main, cols - HALO, 1), pltpu.roll(win, HALO, 1))


def first_kernel(ext, grid, west, east, bands, pack, z, x, p, up, down, sums, gbuf, fbuf, prod, lhs, xacc, *, batch):
    fields = ext.shape[0] - grid.shape[1]
    levels = grid.shape[1]
    members = fields // levels
    reach, cols = ext.shape[1:]
    rows = reach - 2 * HALO
    lane = lax.broadcasted_iota(jnp.int32, (reach, cols), 1)
    lane_in = lane[:rows]
    for l in range(levels):
        spread_grid(gbuf, ext[fields + l], west[fields // 16], east[fields // 16], lane, l, KAPPA**SWEEPS)

    def build(b, i, kind):
        if kind == 0:
            base = slot_lane(i)
            side = west[b]
            side = pltpu.roll(side, cols - base, 1) if base else side
            return jnp.where(lane < HALO, side, pltpu.roll(ext[b * batch + i], HALO, 1))
        w = b * batch + i - fields
        first = 4 * w
        side = east[w // 4]
        turn = (3 * HALO - HALO * (w % 4)) % cols
        out = pltpu.roll(side, turn, 1) if turn else side
        for q in range(4):
            here = (lane >= SLOT * q) & (lane < SLOT * q + 3 * HALO)
            out = jnp.where(here, pltpu.roll(ext[first + q], (SLOT * q + 3 * HALO) % cols, 1), out)
        return out

    covariance(pack, bands, gbuf, z, fbuf, prod, lhs, xacc, batch, build)
    norm = jnp.zeros((8, cols), F32)
    curve = norm
    for l in range(levels):
        state = gather_state(xacc, l, lane_in)
        push = grid[1, l] * state
        x[l] = state
        p[l] = push
        up[l] = push[:HALO]
        down[l] = push[rows - HALO :]
        norm += jnp.sum((grid[0, l] * state).reshape(rows // 8, 8, cols), axis=0)
        curve += jnp.sum((push * state).reshape(rows // 8, 8, cols), axis=0)
    sums[0] = norm
    sums[1] = curve


def second_kernel(pack, ext, grid, west, east, bands, sums, z, x, share, gbuf, fbuf, prod, lhs, xacc, *, batch):
    levels = grid.shape[1]
    reach, cols = ext.shape[1:]
    rows = reach - 2 * HALO
    lane = lax.broadcasted_iota(jnp.int32, (reach, cols), 1)
    lane_in = lane[:rows]
    for l in range(levels):
        spread_grid(gbuf, ext[l], west[...], east[...], lane, l, KAPPA**SWEEPS)
    covariance(pack, bands, gbuf, z, fbuf, prod, lhs, xacc, batch, None)
    cross = jnp.zeros((8, cols), F32)
    curve = cross
    for l in range(levels):
        state = gather_state(xacc, l, lane_in)
        x[l] = state
        cross += jnp.sum((ext[l, HALO : HALO + rows, :] * state).reshape(rows // 8, 8, cols), axis=0)
        curve += jnp.sum((grid[1, l] * state * state).reshape(rows // 8, 8, cols), axis=0)
    out = jnp.zeros((1, cols), F32)
    place = lax.broadcasted_iota(jnp.int32, (1, cols), 1)
    for i, part in enumerate((sums[0], sums[1], cross, curve)):
        out = jnp.where(place == i, jnp.sum(jnp.sum(part, axis=0, keepdims=True), axis=1, keepdims=True), out)
    share[...] = jnp.broadcast_to(out, share.shape)


def final_kernel(share, z_one, z_two, x_one, x_two, control, increment):
    level = pl.program_id(0)
    group = pl.program_id(1)
    batch, _, rows, cols = control.shape
    total = jnp.sum(share[...], axis=0, keepdims=True)
    place = lax.broadcasted_iota(jnp.int32, (1, cols), 1)
    n0, c1, c2, c3 = (jnp.sum(jnp.where(place == i, total, 0.0), axis=1, keepdims=True) for i in range(4))
    bn2 = n0 + EPS
    alpha_one = (n0 + c1) / bn2
    t = (EPS - c1) / bn2
    rr = jnp.maximum((c2 + 2.0 * t * c1 + t * t * n0) / bn2, 0.0)
    beta_sq = rr + EPS
    alpha_two = (rr + jnp.maximum((c3 + 2.0 * t * c2 + t * t * c1) / bn2, 0.0)) / beta_sq
    det = alpha_one * alpha_two - beta_sq
    coef_b = -1.0 / det
    coef_a = (alpha_two - t) / det
    lane = lax.broadcasted_iota(jnp.int32, (rows, cols), 1)
    levels = x_one.shape[0]
    mains = z_one.shape[0] * 4 // 5
    groups = mains // levels // batch

    def mixed(f):
        return coef_a * z_one[f, SWEEPS : SWEEPS + rows, :] + coef_b * z_two[f, SWEEPS : SWEEPS + rows, :]

    first = (level * groups + group) * batch
    for w in range(batch // 4):
        win = mixed(mains + first // 4 + w)
        for q in range(4):
            i = 4 * w + q
            turn = (cols - 3 * HALO - SLOT * q) % cols
            side = pltpu.roll(win, turn, 1) if turn else win
            control[i, 0] = jnp.where(
                lane < cols - 2 * HALO, pltpu.roll(mixed(first + i), cols - HALO, 1), side
            )

    @pl.when((level == 0) & (group == 0))
    def _():
        for l in range(levels):
            increment[l] = coef_a * x_one[l] + coef_b * x_two[l]


def on_device(ensemble, obs_cell, obs_level, innovation, obs_weight):
    members, levels, rows, cols = ensemble.shape
    fields = members * levels
    reach = rows + 2 * HALO
    batch = 16
    packed = fields + fields // 4
    sides = fields // 16
    devices = lax.axis_size("gy") * lax.axis_size("gx")

    def struct(*shape):
        return jax.ShapeDtypeStruct(shape, F32)

    def call(kernel, outs, n_in, scratch=(), limit=32, **kw):
        return pl.pallas_call(
            kernel,
            out_shape=outs,
            in_specs=[VMEM] * n_in,
            out_specs=jax.tree.map(lambda _: VMEM, outs),
            scratch_shapes=scratch,
            compiler_params=pltpu.CompilerParams(vmem_limit_bytes=limit * 2**20),
            **kw,
        )

    gx = lax.axis_index("gx")
    variant = (gx == 0).astype(jnp.int32) + 2 * (gx == lax.axis_size("gx") - 1).astype(jnp.int32)
    bands = lax.dynamic_index_in_dim(jnp.asarray(band_matrices(cols), BF16), variant, 0, keepdims=False)
    bands = jnp.concatenate([bands, bands], axis=1)

    flat = [a.reshape(1, -1) for a in (obs_cell, obs_level, innovation, obs_weight)]
    grid, up, down = call(
        scatter_kernel,
        (struct(2, levels, rows, cols), struct(fields + levels, HALO, cols), struct(fields + levels, HALO, cols)),
        5,
    )(ensemble, *flat)
    north, south = shift(down, "gy", 1), shift(up, "gy", -1)
    ext, west, east = call(
        sides_kernel,
        (struct(fields + levels, reach, cols), struct(sides + 1, reach, cols), struct(sides + 1, reach, cols)),
        4,
    )(ensemble, grid, north, south)
    from_west, from_east = shift(east, "gx", 1), shift(west, "gx", -1)
    scratch = (
        pltpu.VMEM((levels, 2, reach, cols), F32),
        pltpu.VMEM((batch, reach, cols), F32),
        pltpu.VMEM((SWEEPS, batch * reach, cols), F32),
        pltpu.VMEM((batch * reach, 2 * cols), BF16),
        pltpu.VMEM((levels, 2, rows, cols), F32),
    )
    pack, z_one, x_one, p, up, down, sums = call(
        functools.partial(first_kernel, batch=batch),
        (
            struct(packed, reach, cols),
            struct(packed, reach - HALO, cols),
            struct(levels, rows, cols),
            struct(levels, rows, cols),
            struct(levels, HALO, cols),
            struct(levels, HALO, cols),
            struct(2, 8, cols),
        ),
        5,
        scratch,
    )(ext, grid, from_west, from_east, bands)
    north, south = shift(down, "gy", 1), shift(up, "gy", -1)
    p_ext, west, east = call(
        grid_sides_kernel, (struct(levels, reach, cols), struct(reach, cols), struct(reach, cols)), 3
    )(p, north, south)
    from_west, from_east = shift(east, "gx", 1), shift(west, "gx", -1)
    z_two, x_two, share = call(
        functools.partial(second_kernel, batch=batch),
        (struct(packed, reach - HALO, cols), struct(levels, rows, cols), struct(devices, cols)),
        7,
        scratch,
    )(pack, p_ext, grid, from_west, from_east, bands, sums)
    share = lax.all_to_all(share, ("gy", "gx"), 0, 0, tiled=True)
    return pl.pallas_call(
        final_kernel,
        grid=(levels, members // batch),
        out_shape=(struct(members, levels, rows, cols), struct(levels, rows, cols)),
        in_specs=[VMEM] * 5,
        out_specs=(
            pl.BlockSpec((batch, 1, rows, cols), lambda l, g: (g, l, 0, 0)),
            pl.BlockSpec((levels, rows, cols), lambda l, g: (0, 0, 0)),
        ),
        compiler_params=pltpu.CompilerParams(vmem_limit_bytes=32 * 2**20),
    )(share, z_one, z_two, x_one, x_two)


def solution(mesh):
    return jax.shard_map(
        on_device,
        mesh=mesh,
        in_specs=(
            P(None, None, "gy", "gx"),
            P("gy", "gx", None),
            P("gy", "gx", None),
            P("gy", "gx", None),
            P("gy", "gx", None),
        ),
        out_specs=(P(None, None, "gy", "gx"), P(None, "gy", "gx")),
        check_vma=False,
    )
```

```python
import functools
import math

import jax
import jax.numpy as jnp
import numpy as np
from jax import lax
from jax.experimental import pallas as pl
from jax.experimental.pallas import tpu as pltpu
from jax.sharding import PartitionSpec as P

SWEEPS = 4
KAPPA = 0.2
EPS = 1e-06
HALO = 2 * SWEEPS
WIDE = 2 * HALO
PAIR = 4 * WIDE
VMEM = pl.BlockSpec(memory_space=pltpu.VMEM)
F32 = jnp.float32
BF16 = jnp.bfloat16


def band_matrices(lanes):
    out = np.zeros((4, 2, lanes, SWEEPS * lanes), np.float32)
    lane = np.arange(lanes)
    for variant in range(4):
        for kind in range(2):
            col, part = lane, 0 * lane
            if kind == 1:
                j = lane % PAIR
                col = np.where(j < 2 * WIDE, j - WIDE, lanes - 3 * WIDE + j)
                part = lane // (2 * WIDE)
            inside = np.ones(lanes, bool)
            if variant % 2:
                inside &= col >= 0
            if variant // 2:
                inside &= col < lanes
            near = (np.abs(lane[:, None] - lane[None, :]) <= 1) & (part[:, None] == part[None, :])
            band = (near & inside[:, None] & inside[None, :]).astype(np.float64)
            power = [np.diag(inside.astype(np.float64))]
            for _ in range(SWEEPS):
                power.append(power[-1] @ band)
            for j in range(SWEEPS):
                q = sum(
                    math.comb(SWEEPS, k) * math.comb(SWEEPS - k, (SWEEPS - k - j) // 2) * power[k]
                    for k in range(SWEEPS - j + 1)
                    if (SWEEPS - k - j) % 2 == 0
                )
                out[variant, kind, :, j * lanes : (j + 1) * lanes] = q
    return out


def shift(x, axis, step):
    count = lax.axis_size(axis)
    return lax.ppermute(x, axis, [(i, i + step) for i in range(count) if 0 <= i + step < count])


def turn(x, amount):
    amount %= x.shape[-1]
    return pltpu.roll(x, amount, x.ndim - 1) if amount else x


def lanes_of(x):
    return lax.broadcasted_iota(jnp.int32, x.shape, x.ndim - 1)


def scatter_kernel(ens, cell_in, level_in, innov_in, weight_in, grid, up, down, cell, level, innov, weight, first, last, sem):
    members, levels, rows, cols = ens.shape
    obs = cell.shape[-1]
    copies = [
        pltpu.make_async_copy(a, b, sem.at[i])
        for i, (a, b) in enumerate(
            (
                (cell_in, cell),
                (level_in, level),
                (innov_in, innov),
                (weight_in, weight),
                (ens.at[:, :, 0:16, :], first),
                (ens.at[:, :, rows - 16 : rows, :], last),
            )
        )
    ]
    for c in copies:
        c.start()
    for c in copies[:4]:
        c.wait()
    span = 256
    row_iota = lax.broadcasted_iota(jnp.int32, (levels * rows, span), 0)
    col_iota = lax.broadcasted_iota(jnp.int32, (cols, span), 0)
    acc = jnp.zeros((4 * levels * rows, cols), F32)
    for start in range(0, obs, span):
        at = slice(start, start + span)
        spot = cell[0, :, at]
        here = row_iota == level[0, :, at] * rows + spot // cols
        w = weight[0, :, at]
        parts = []
        for value in (w * innov[0, :, at], w):
            high = value.astype(BF16).astype(F32)
            parts += [high, value - high]
        left = jnp.concatenate([jnp.where(here, part, 0.0).astype(BF16) for part in parts], axis=0)
        right = jnp.where(col_iota == spot % cols, 1.0, 0.0).astype(BF16)
        acc += lax.dot_general(left, right, (((1,), (1,)), ((), ())), preferred_element_type=F32)
    n = levels * rows
    g = acc[:n] + acc[n : 2 * n]
    d = acc[2 * n : 3 * n] + acc[3 * n :]
    fields = members * levels
    for l in range(levels):
        grid[0, l] = g[l * rows : (l + 1) * rows]
        grid[1, l] = d[l * rows : (l + 1) * rows]
        up[fields + l] = g[l * rows : l * rows + HALO]
        down[fields + l] = g[(l + 1) * rows - HALO : (l + 1) * rows]
    for c in copies[4:]:
        c.wait()

    def edge(m, _):
        for l in range(levels):
            up[l * members + m] = first[m, l].astype(F32)[:HALO]
            down[l * members + m] = last[m, l].astype(F32)[16 - HALO :]
        return 0

    lax.fori_loop(0, members, edge, 0)


def arrange(u, get, mains, wins, west, east, spans):
    xs = [get(8 * u + t) for t in range(8)]
    lane = lanes_of(xs[0])

    def put(ref, f, value):
        at = 0
        for start, count in spans:
            ref[f, start : start + count, :] = value[at : at + count]
            at += count

    w_strip = e_strip = jnp.zeros_like(xs[0])
    for t, x in enumerate(xs):
        put(mains, 8 * u + t, x)
        here = (lane >= WIDE * t) & (lane < WIDE * (t + 1))
        w_strip = jnp.where(here, turn(x, WIDE * t), w_strip)
        e_strip = jnp.where(here, turn(x, WIDE * (t + 1)), e_strip)
    put(west, u, w_strip)
    put(east, u, e_strip)
    for v in range(4):
        win = jnp.zeros_like(xs[0])
        for q in range(2):
            x = xs[2 * v + q]
            at = lane - PAIR * q
            win = jnp.where((at >= WIDE) & (at < 2 * WIDE), turn(x, PAIR * q + WIDE), win)
            win = jnp.where((at >= 2 * WIDE) & (at < 3 * WIDE), turn(x, PAIR * q + 3 * WIDE), win)
        put(wins, 4 * u + v, win)


def strip_grid(fields, west, east, at, spans):
    w_strip = e_strip = jnp.zeros_like(fields[0])
    lane = lanes_of(w_strip)
    for t, x in enumerate(fields):
        here = (lane >= WIDE * t) & (lane < WIDE * (t + 1))
        w_strip = jnp.where(here, turn(x, WIDE * t), w_strip)
        e_strip = jnp.where(here, turn(x, WIDE * (t + 1)), e_strip)
    row = 0
    for start, count in spans:
        west[at, start : start + count, :] = w_strip[row : row + count]
        east[at, start : start + count, :] = e_strip[row : row + count]
        row += count


def own_kernel(ens_in, grid, bands_in, mains, wins, west, east, g_ext, mirror, bands, ens, sem):
    members, levels, rows, cols = ens.shape
    fields = members * levels
    gx = lax.axis_index("gx")
    variant = jnp.where(gx == 0, 1, 0) + jnp.where(gx == lax.axis_size("gx") - 1, 2, 0)
    copies = [pltpu.make_async_copy(ens_in, ens, sem.at[0])]
    for half in range(2):
        part = bands.at[:, half * cols : (half + 1) * cols, :]
        copies.append(pltpu.make_async_copy(bands_in.at[variant], part, sem.at[1 + half]))
    for c in copies:
        c.start()
    for c in copies:
        c.wait()
    spans = ((HALO, rows),)

    def group(u, _):
        l = 8 * u // members
        arrange(u, lambda f: ens[f - l * members, l].astype(F32), mains, wins, west, east, spans)
        return 0

    lax.fori_loop(0, fields // 8, group, 0)
    strip_grid([grid[k, l] for k in range(2) for l in range(levels)], west, east, fields // 8, spans)
    for l in range(levels):
        g_ext[l, HALO : HALO + rows, :] = grid[0, l]
    mirror[...] = jnp.zeros_like(mirror)
    me = lax.axis_index("gy")
    row = lax.broadcasted_iota(jnp.int32, (HALO, cols), 0)

    def flip(x, step):
        out = jnp.zeros((HALO, cols), F32)
        for j in range(1, HALO):
            if step > 0:
                out = jnp.where(row == HALO - 1 - j, x[j - 1 : j], out)
            else:
                out = jnp.where(row == j, x[HALO - j : HALO - j + 1], out)
        return out

    def side(step):
        at = 0 if step > 0 else rows - HALO
        slot = 0 if step > 0 else 1
        start = 0 if step > 0 else rows - 16
        skip = 0 if step > 0 else 16 - HALO

        def body(m, _):
            for l in range(levels):
                x = ens[m, l, start : start + 16, :].astype(F32)[skip : skip + HALO]
                mirror[slot, l * members + m] = flip(x, step)
            return 0

        lax.fori_loop(0, members, body, 0)
        for l in range(levels):
            mirror[slot, fields + l] = -flip(grid[0, l, at : at + HALO, :], step)

    pl.when(me == 0)(lambda: side(1))
    pl.when(me == lax.axis_size("gy") - 1)(lambda: side(-1))


def halo_kernel(north, south, mirror, *refs):
    mains, wins, west, east, g_ext = refs[5:]
    levels, reach, cols = g_ext.shape
    fields = north.shape[0] - levels
    spans = ((0, HALO), (reach - HALO, HALO))

    def get(f):
        return jnp.concatenate([north[f] + mirror[0, f], south[f] + mirror[1, f]], axis=0)

    def group(u, _):
        arrange(u, get, mains, wins, west, east, spans)
        return 0

    lax.fori_loop(0, fields // 8, group, 0)
    ends = [get(fields + l) for l in range(levels)]
    strip_grid(ends, west, east, fields // 8, spans)
    for l in range(levels):
        g_ext[l, 0:HALO, :] = ends[l][:HALO]
        g_ext[l, reach - HALO :, :] = ends[l][HALO:]


def band_products(lhs, bands, kind, out, count):
    lanes = lhs.shape[1] // 2
    for half in range(SWEEPS // 2):
        r = jnp.dot(
            lhs[0:count, :],
            bands[kind, :, half * 2 * lanes : (half + 1) * 2 * lanes],
            preferred_element_type=F32,
        )
        out[2 * half, 0:count, :] = r[:, :lanes]
        out[2 * half + 1, 0:count, :] = r[:, lanes:]


def split_into(lhs, start, x):
    count, lanes = x.shape
    high = x.astype(BF16)
    lhs[start : start + count, 0:lanes] = high
    lhs[start : start + count, lanes : 2 * lanes] = (x - high.astype(F32)).astype(BF16)


def combine(prod, start, src, f, count):
    def part(k, off):
        return prod[k, pl.ds(start + off, count), :]

    s = SWEEPS
    total = src[f, pl.ds(2 * s, count), :] + src[f, pl.ds(0, count), :]
    for k in range(1, s):
        total += part(k, s + k) + part(k, s - k)
    return total + part(0, s)


def covariance(pack, bands, kind, g, z, xacc, fbuf, prod, lhs, batch, build=None):
    count, reach, _ = pack.shape
    inner, rows = reach - HALO, reach - 2 * HALO
    per_level = count // g.shape[0]
    xacc[...] = jnp.zeros_like(xacc)

    def step(b, _):
        level = b * batch // per_level
        for i in range(batch):
            at = b * batch + i
            if build is not None:
                pack[at] = build(b, i, pack[at])
            f = pack[at] * g[level]
            fbuf[i] = f
            split_into(lhs, i * reach, f)
        band_products(lhs, bands, kind, prod, batch * reach)
        for i in range(batch):
            v = combine(prod, i * reach, fbuf, i, inner)
            z[b * batch + i] = v
            split_into(lhs, i * inner, v)
        band_products(lhs, bands, kind, prod, batch * inner)
        for i in range(batch):
            v = combine(prod, i * inner, z, b * batch + i, rows)
            xacc[level] += v * pack[b * batch + i, HALO : HALO + rows, :]
        return 0

    lax.fori_loop(0, count // batch, step, 0)


def window_grid(g, west, east):
    lane = lanes_of(g)
    win = jnp.where(lane < WIDE, west, turn(g, WIDE))
    win = jnp.where(lane < 2 * WIDE, win, turn(g, 3 * WIDE))
    win = jnp.where(lane < 3 * WIDE, win, turn(east, 3 * WIDE))
    win = jnp.where(lane < PAIR, win, 0.0)
    return (win + turn(win, PAIR)) * KAPPA**SWEEPS


def fold(x):
    return jnp.sum(x.reshape(x.shape[0] // 8, 8, x.shape[1]), axis=0)


def main_kernel(pack, g_ext, bands, z, xacc, gbuf, fbuf, prod, lhs, *, batch):
    gbuf[...] = g_ext[...] * KAPPA**SWEEPS
    covariance(pack, bands, 0, gbuf, z, xacc, fbuf, prod, lhs, batch)


def join(main, win, cols):
    win = (win + turn(win, PAIR)) * KAPPA**SWEEPS
    lane = lanes_of(win)
    state = jnp.where(lane < HALO, turn(win, -WIDE), main * KAPPA**SWEEPS)
    return jnp.where(lane < cols - HALO, state, turn(win, cols - 3 * WIDE)), win


def first_kernel(pack_in, g_ext, grid, west, east, bands, xmain, pack, z, x, p, up, down, side, sums, gbuf, fbuf, prod, lhs, xacc, *, batch):
    del pack_in
    levels, reach, cols = g_ext.shape
    rows = reach - 2 * HALO
    last = west.shape[0] - 1
    for l in range(levels):
        gbuf[l] = window_grid(g_ext[l], turn(west[last], -WIDE * l), turn(east[last], -WIDE * l))
    lane = lax.broadcasted_iota(jnp.int32, (reach, cols), 1)

    def window(b, i, old):
        u = b * (batch // 4) + i // 4
        for q in range(2):
            slot = WIDE * (2 * (i % 4) + q)
            at = lane - PAIR * q
            old = jnp.where((at >= 0) & (at < WIDE), turn(west[u], PAIR * q - slot), old)
            old = jnp.where((at >= 3 * WIDE) & (at < PAIR), turn(east[u], PAIR * q + 3 * WIDE - slot), old)
        return old

    covariance(pack, bands, 1, gbuf, z, xacc, fbuf, prod, lhs, batch, window)
    norm = jnp.zeros((8, cols), F32)
    curve = norm
    lane = lane[:rows]
    d_west, d_east = west[last, HALO : HALO + rows, :], east[last, HALO : HALO + rows, :]
    sides = jnp.zeros((rows, cols), F32)
    for l in range(levels):
        state, win = join(xmain[l], xacc[l], cols)
        push = grid[1, l] * state
        x[l] = state
        p[l] = push
        up[l] = push[:HALO]
        down[l] = push[rows - HALO :]
        norm += fold(grid[0, l] * state)
        curve += fold(push * state)
        base = WIDE * l
        far = WIDE * (levels + l)
        beside = turn(win, base - HALO) * turn(d_west, base - far - HALO)
        sides = jnp.where((lane >= base) & (lane < base + HALO), beside, sides)
        beside = turn(win, base + HALO - 3 * WIDE) * turn(d_east, base + HALO - far)
        sides = jnp.where((lane >= base + HALO) & (lane < base + WIDE), beside, sides)
    side[...] = sides
    up[levels] = sides[:HALO]
    down[levels] = sides[rows - HALO :]
    sums[0] = norm
    sums[1] = curve


def second_kernel(mains, wins, p, side, north, south, grid, bands, sums, zm, zw, x, share, ext, gbuf, fbuf, prod, lhs, xacc, *, batch):
    levels, rows, cols = p.shape
    reach = rows + 2 * HALO
    for l in range(levels + 1):
        ext[l, HALO : HALO + rows, :] = p[l] if l < levels else side[...]
        ext[l, 0:HALO, :] = north[l]
        ext[l, HALO + rows :, :] = south[l]
    me = lax.axis_index("gy")

    def reflect(base, step):
        for l in range(levels + 1):
            for j in range(1, HALO):
                ext[l, base - step * j : base - step * j + 1, :] = -ext[l, base + step * j : base + step * j + 1, :]

    pl.when(me == 0)(lambda: reflect(HALO - 1, 1))
    pl.when(me == lax.axis_size("gy") - 1)(lambda: reflect(HALO + rows, -1))
    lane = lax.broadcasted_iota(jnp.int32, (reach, cols), 1)
    for l in range(levels):
        gbuf[0, l] = ext[l] * KAPPA**SWEEPS
        west = jnp.where(lane < HALO, 0.0, turn(ext[levels], HALO - WIDE * l))
        east = jnp.where(lane < HALO, turn(ext[levels], -HALO - WIDE * l), 0.0)
        gbuf[1, l] = window_grid(ext[l], west, east)
    covariance(mains, bands, 0, gbuf.at[0], zm, xacc.at[0], fbuf, prod, lhs, batch)
    covariance(wins, bands, 1, gbuf.at[1], zw, xacc.at[1], fbuf, prod, lhs, batch)
    cross = jnp.zeros((8, cols), F32)
    curve = cross
    for l in range(levels):
        state, _ = join(xacc[0, l], xacc[1, l], cols)
        x[l] = state
        cross += fold(p[l] * state)
        curve += fold(grid[1, l] * state * state)
    out = jnp.zeros((1, cols), F32)
    place = lax.broadcasted_iota(jnp.int32, (1, cols), 1)
    for i, part in enumerate((sums[0], sums[1], cross, curve)):
        out = jnp.where(place == i, jnp.sum(jnp.sum(part, axis=0, keepdims=True), axis=1, keepdims=True), out)
    share[...] = jnp.broadcast_to(out, share.shape)


def final_kernel(share, zm_one, zw_one, zm_two, zw_two, x_one, x_two, control, increment):
    level = pl.program_id(0)
    group = pl.program_id(1)
    batch, _, rows, cols = control.shape
    total = jnp.sum(share[...], axis=0, keepdims=True)
    place = lax.broadcasted_iota(jnp.int32, (1, cols), 1)
    n0, c1, c2, c3 = (jnp.sum(jnp.where(place == i, total, 0.0), axis=1, keepdims=True) for i in range(4))
    bn2 = n0 + EPS
    alpha_one = (n0 + c1) / bn2
    t = (EPS - c1) / bn2
    rr = jnp.maximum((c2 + 2.0 * t * c1 + t * t * n0) / bn2, 0.0)
    beta_sq = rr + EPS
    alpha_two = (rr + jnp.maximum((c3 + 2.0 * t * c2 + t * t * c1) / bn2, 0.0)) / beta_sq
    det = alpha_one * alpha_two - beta_sq
    coef_b = -1.0 / det
    coef_a = (alpha_two - t) / det
    lane = lax.broadcasted_iota(jnp.int32, (rows, cols), 1)
    groups = zm_one.shape[0] // x_one.shape[0] // batch

    def mixed(one, two, f):
        return coef_a * one[f, SWEEPS : SWEEPS + rows, :] + coef_b * two[f, SWEEPS : SWEEPS + rows, :]

    first = (level * groups + group) * batch
    for w in range(batch // 2):
        win = mixed(zw_one, zw_two, first // 2 + w)
        for q in range(2):
            i = 2 * w + q
            main = jnp.where(lane < HALO, turn(win, -WIDE - PAIR * q), mixed(zm_one, zm_two, first + i))
            control[i, 0] = jnp.where(lane < cols - HALO, main, turn(win, cols - 3 * WIDE - PAIR * q))

    @pl.when((level == 0) & (group == 0))
    def _():
        for l in range(x_one.shape[0]):
            increment[l] = coef_a * x_one[l] + coef_b * x_two[l]


def on_device(ensemble, obs_cell, obs_level, innovation, obs_weight):
    members, levels, rows, cols = ensemble.shape
    fields = members * levels
    reach = rows + 2 * HALO
    batch = 16
    strips = fields // 8 + 1
    devices = lax.axis_size("gy") * lax.axis_size("gx")
    hbm = pl.BlockSpec(memory_space=pltpu.HBM)

    def struct(*shape):
        return jax.ShapeDtypeStruct(shape, F32)

    def call(kernel, outs, ins, scratch=(), limit=16, work=2, **kw):
        return pl.pallas_call(
            kernel,
            out_shape=outs,
            in_specs=[VMEM] * ins if isinstance(ins, int) else ins,
            out_specs=jax.tree.map(lambda _: VMEM, outs),
            scratch_shapes=scratch,
            compiler_params=pltpu.CompilerParams(vmem_limit_bytes=limit * 2**20),
            cost_estimate=pl.CostEstimate(flops=work * 10**9, bytes_accessed=10**6, transcendentals=0),
            **kw,
        )

    bands = jnp.asarray(band_matrices(cols), BF16)
    obs = obs_cell.shape
    edge = pltpu.VMEM((members, levels, 16, cols), BF16)
    grid, up, down = call(
        scatter_kernel,
        (struct(2, levels, rows, cols), struct(fields + levels, HALO, cols), struct(fields + levels, HALO, cols)),
        [hbm] * 5,
        [pltpu.VMEM(obs, jnp.int32)] * 2 + [pltpu.VMEM(obs, F32)] * 2 + [edge, edge, pltpu.SemaphoreType.DMA((6,))],
        limit=60,
    )(ensemble, obs_cell, obs_level, innovation, obs_weight)
    north, south = shift(down, "gy", 1), shift(up, "gy", -1)
    main_shape, win_shape = struct(fields, reach, cols), struct(fields // 2, reach, cols)
    laid = (
        main_shape,
        win_shape,
        struct(strips, reach, cols),
        struct(strips, reach, cols),
        struct(levels, reach, cols),
    )
    *own, mirror, bands = call(
        own_kernel,
        (
            *laid,
            struct(2, fields + levels, HALO, cols),
            jax.ShapeDtypeStruct((2, 2 * cols, SWEEPS * cols), BF16),
        ),
        [hbm, VMEM, hbm],
        [pltpu.VMEM(ensemble.shape, BF16), pltpu.SemaphoreType.DMA((3,))],
    )(ensemble, grid, bands)
    mains, wins, west, east, g_ext = call(halo_kernel, laid, 8, input_output_aliases={3 + i: i for i in range(5)})(
        north, south, mirror, *own
    )
    from_west, from_east = shift(east, "gx", 1), shift(west, "gx", -1)
    work = (
        pltpu.VMEM((batch, reach, cols), F32),
        pltpu.VMEM((SWEEPS, batch * reach, cols), F32),
        pltpu.VMEM((batch * reach, 2 * cols), BF16),
    )
    gbuf = pltpu.VMEM((levels, reach, cols), F32)
    zm_shape, zw_shape = struct(fields, reach - HALO, cols), struct(fields // 2, reach - HALO, cols)
    zm_one, xmain = call(
        functools.partial(main_kernel, batch=batch), (zm_shape, struct(levels, rows, cols)), 3, (gbuf, *work)
    )(mains, g_ext, bands)
    wins, zw_one, x_one, p, up, down, side, sums = call(
        functools.partial(first_kernel, batch=batch),
        (
            win_shape,
            zw_shape,
            struct(levels, rows, cols),
            struct(levels, rows, cols),
            struct(levels + 1, HALO, cols),
            struct(levels + 1, HALO, cols),
            struct(rows, cols),
            struct(2, 8, cols),
        ),
        7,
        (gbuf, *work, pltpu.VMEM((levels, rows, cols), F32)),
        input_output_aliases={0: 0},
    )(wins, g_ext, grid, from_west, from_east, bands, xmain)
    north, south = shift(down, "gy", 1), shift(up, "gy", -1)
    zm_two, zw_two, x_two, share = call(
        functools.partial(second_kernel, batch=batch),
        (zm_shape, zw_shape, struct(levels, rows, cols), struct(devices, cols)),
        9,
        (
            pltpu.VMEM((levels + 1, reach, cols), F32),
            pltpu.VMEM((2, levels, reach, cols), F32),
            *work,
            pltpu.VMEM((2, levels, rows, cols), F32),
        ),
    )(mains, wins, p, side, north, south, grid, bands, sums)
    share = lax.all_to_all(share, ("gy", "gx"), 0, 0, tiled=True)
    return pl.pallas_call(
        final_kernel,
        grid=(levels, members // batch),
        out_shape=(struct(members, levels, rows, cols), struct(levels, rows, cols)),
        in_specs=[VMEM] * 7,
        out_specs=(
            pl.BlockSpec((batch, 1, rows, cols), lambda l, g: (g, l, 0, 0)),
            pl.BlockSpec((levels, rows, cols), lambda l, g: (0, 0, 0)),
        ),
        compiler_params=pltpu.CompilerParams(vmem_limit_bytes=32 * 2**20),
    )(share, zm_one, zw_one, zm_two, zw_two, x_one, x_two)


def solution(mesh):
    return jax.shard_map(
        on_device,
        mesh=mesh,
        in_specs=(
            P(None, None, "gy", "gx"),
            P("gy", "gx", None),
            P("gy", "gx", None),
            P("gy", "gx", None),
            P("gy", "gx", None),
        ),
        out_specs=(P(None, None, "gy", "gx"), P(None, "gy", "gx")),
        check_vma=False,
    )
```

```python
import functools
import math

import jax
import jax.numpy as jnp
import numpy as np
from jax import lax
from jax.experimental import pallas as pl
from jax.experimental.pallas import tpu as pltpu
from jax.sharding import PartitionSpec as P

SWEEPS = 4
KAPPA = 0.2
EPS = 1e-06
HALO = 2 * SWEEPS
WIDE = 2 * HALO
PAIR = 4 * WIDE
VMEM = pl.BlockSpec(memory_space=pltpu.VMEM)
F32 = jnp.float32
BF16 = jnp.bfloat16


def band_matrices(lanes):
    out = np.zeros((4, 2, lanes, SWEEPS * lanes), np.float32)
    lane = np.arange(lanes)
    for variant in range(4):
        for kind in range(2):
            col, part = lane, 0 * lane
            if kind == 1:
                j = lane % PAIR
                col = np.where(j < 2 * WIDE, j - WIDE, lanes - 3 * WIDE + j)
                part = lane // (2 * WIDE)
            inside = np.ones(lanes, bool)
            if variant % 2:
                inside &= col >= 0
            if variant // 2:
                inside &= col < lanes
            near = (np.abs(lane[:, None] - lane[None, :]) <= 1) & (part[:, None] == part[None, :])
            band = (near & inside[:, None] & inside[None, :]).astype(np.float64)
            power = [np.diag(inside.astype(np.float64))]
            for _ in range(SWEEPS):
                power.append(power[-1] @ band)
            for j in range(SWEEPS):
                q = sum(
                    math.comb(SWEEPS, k) * math.comb(SWEEPS - k, (SWEEPS - k - j) // 2) * power[k]
                    for k in range(SWEEPS - j + 1)
                    if (SWEEPS - k - j) % 2 == 0
                )
                out[variant, kind, :, j * lanes : (j + 1) * lanes] = q
    return out


def swap(x, axis, odd):
    count = lax.axis_size(axis)
    return lax.ppermute(x, axis, [(i + a, i + 1 - a) for i in range(odd, count - 1, 2) for a in range(2)])


def by_parity(axis, even, odd):
    me = jnp.full(even.shape, lax.axis_index(axis), jnp.int32)
    return jnp.where((me & 1) == 0, even, odd)


def turn(x, amount):
    amount %= x.shape[-1]
    return pltpu.roll(x, amount, x.ndim - 1) if amount else x


def lanes_of(x):
    return lax.broadcasted_iota(jnp.int32, x.shape, x.ndim - 1)


def scatter_kernel(ens, cell_in, level_in, innov_in, weight_in, grid, near, far, cell, level, innov, weight, first, last, sem):
    members, levels, rows, cols = ens.shape
    obs = cell.shape[-1]
    copies = [
        pltpu.make_async_copy(a, b, sem.at[i])
        for i, (a, b) in enumerate(
            (
                (cell_in, cell),
                (level_in, level),
                (innov_in, innov),
                (weight_in, weight),
                (ens.at[:, :, 0:16, :], first),
                (ens.at[:, :, rows - 16 : rows, :], last),
            )
        )
    ]
    for c in copies:
        c.start()
    for c in copies[:4]:
        c.wait()
    span = 256
    row_iota = lax.broadcasted_iota(jnp.int32, (levels * rows, span), 0)
    col_iota = lax.broadcasted_iota(jnp.int32, (cols, span), 0)
    acc = jnp.zeros((4 * levels * rows, cols), F32)
    for start in range(0, obs, span):
        at = slice(start, start + span)
        spot = cell[0, :, at]
        here = row_iota == level[0, :, at] * rows + spot // cols
        w = weight[0, :, at]
        parts = []
        for value in (w * innov[0, :, at], w):
            high = value.astype(BF16).astype(F32)
            parts += [high, value - high]
        left = jnp.concatenate([jnp.where(here, part, 0.0).astype(BF16) for part in parts], axis=0)
        right = jnp.where(col_iota == spot % cols, 1.0, 0.0).astype(BF16)
        acc += lax.dot_general(left, right, (((1,), (1,)), ((), ())), preferred_element_type=F32)
    n = levels * rows
    g = acc[:n] + acc[n : 2 * n]
    d = acc[2 * n : 3 * n] + acc[3 * n :]
    fields = members * levels
    for l in range(levels):
        grid[0, l] = g[l * rows : (l + 1) * rows]
        grid[1, l] = d[l * rows : (l + 1) * rows]
        up = g[l * rows : l * rows + HALO]
        down = g[(l + 1) * rows - HALO : (l + 1) * rows]
        near[fields + l] = by_parity("gy", down, up)
        far[fields + l] = by_parity("gy", up, down)
    for c in copies[4:]:
        c.wait()

    def edge(m, _):
        for l in range(levels):
            up = first[m, l].astype(F32)[:HALO]
            down = last[m, l].astype(F32)[16 - HALO :]
            near[l * members + m] = by_parity("gy", down, up)
            far[l * members + m] = by_parity("gy", up, down)
        return 0

    lax.fori_loop(0, members, edge, 0)


def slot_lane(t):
    return PAIR * (t % 2) + WIDE * (t // 2)


def strip(xs, at, near, far):
    lane = lanes_of(xs[0])
    west = east = jnp.zeros_like(xs[0])
    for t, x in enumerate(xs):
        base = slot_lane(t)
        here = (lane >= base) & (lane < base + WIDE)
        west = jnp.where(here, turn(x, base), west)
        east = jnp.where(here, turn(x, base + WIDE), east)
    near[at] = by_parity("gx", east, west)
    far[at] = by_parity("gx", west, east)


def arrange(u, get, mains, wins, near, far, spans):
    xs = [get(8 * u + t) for t in range(8)]
    lane = lanes_of(xs[0])

    def put(ref, f, value):
        at = 0
        for start, count in spans:
            ref[f, start : start + count, :] = value[at : at + count]
            at += count

    for t, x in enumerate(xs):
        put(mains, 8 * u + t, x)
    strip(xs, u, near, far)
    for v in range(4):
        win = jnp.zeros_like(xs[0])
        for q in range(2):
            x = xs[2 * v + q]
            at = lane - PAIR * q
            win = jnp.where((at >= WIDE) & (at < 2 * WIDE), turn(x, PAIR * q + WIDE), win)
            win = jnp.where((at >= 2 * WIDE) & (at < 3 * WIDE), turn(x, PAIR * q + 3 * WIDE), win)
        put(wins, 4 * u + v, win)


def own_kernel(ens_in, grid, bands_in, mains, wins, near, far, g_ext, mirror, bands, ens, sem):
    members, levels, rows, cols = ens.shape
    fields = members * levels
    gx = lax.axis_index("gx")
    variant = jnp.where(gx == 0, 1, 0) + jnp.where(gx == lax.axis_size("gx") - 1, 2, 0)
    copies = [pltpu.make_async_copy(ens_in, ens, sem.at[0])]
    for half in range(2):
        part = bands.at[:, half * cols : (half + 1) * cols, :]
        copies.append(pltpu.make_async_copy(bands_in.at[variant], part, sem.at[1 + half]))
    for c in copies:
        c.start()
    for c in copies:
        c.wait()
    spans = ((HALO, rows),)

    def group(u, _):
        l = 8 * u // members
        arrange(u, lambda f: ens[f - l * members, l].astype(F32), mains, wins, near, far, spans)
        return 0

    lax.fori_loop(0, fields // 8, group, 0)
    strip([grid[k, l] for k in range(2) for l in range(levels)], fields // 8, near, far)
    for l in range(levels):
        g_ext[l, HALO : HALO + rows, :] = grid[0, l]
    mirror[...] = jnp.zeros_like(mirror)
    me = lax.axis_index("gy")
    row = lax.broadcasted_iota(jnp.int32, (HALO, cols), 0)

    def flip(x, step):
        out = jnp.zeros((HALO, cols), F32)
        for j in range(1, HALO):
            if step > 0:
                out = jnp.where(row == HALO - 1 - j, x[j - 1 : j], out)
            else:
                out = jnp.where(row == j, x[HALO - j : HALO - j + 1], out)
        return out

    def side(step):
        at = 0 if step > 0 else rows - HALO
        slot = 0 if step > 0 else 1
        start = 0 if step > 0 else rows - 16
        skip = 0 if step > 0 else 16 - HALO

        def body(m, _):
            for l in range(levels):
                x = ens[m, l, start : start + 16, :].astype(F32)[skip : skip + HALO]
                mirror[slot, l * members + m] = flip(x, step)
            return 0

        lax.fori_loop(0, members, body, 0)
        for l in range(levels):
            mirror[slot, fields + l] = -flip(grid[0, l, at : at + HALO, :], step)

    pl.when(me == 0)(lambda: side(1))
    pl.when(me == lax.axis_size("gy") - 1)(lambda: side(-1))


def halo_kernel(from_near, from_far, mirror, *refs):
    mains, wins, g_ext, near, far = refs[3:]
    levels, reach, cols = g_ext.shape
    fields = mirror.shape[1] - levels
    spans = ((0, HALO), (reach - HALO, HALO))

    def get(f):
        a, b = from_near[f], from_far[f]
        return jnp.concatenate([by_parity("gy", b, a) + mirror[0, f], by_parity("gy", a, b) + mirror[1, f]], axis=0)

    def group(u, _):
        arrange(u, get, mains, wins, near, far, spans)
        return 0

    lax.fori_loop(0, fields // 8, group, 0)
    ends = [get(fields + l) for l in range(levels)]
    strip(ends, fields // 8, near, far)
    for l in range(levels):
        g_ext[l, 0:HALO, :] = ends[l][:HALO]
        g_ext[l, reach - HALO :, :] = ends[l][HALO:]


def band_products(lhs, bands, kind, out, count):
    lanes = lhs.shape[1] // 2
    for half in range(SWEEPS // 2):
        r = jnp.dot(
            lhs[0:count, :],
            bands[kind, :, half * 2 * lanes : (half + 1) * 2 * lanes],
            preferred_element_type=F32,
        )
        out[2 * half, 0:count, :] = r[:, :lanes]
        out[2 * half + 1, 0:count, :] = r[:, lanes:]


def split_into(lhs, start, x):
    count, lanes = x.shape
    high = x.astype(BF16)
    lhs[start : start + count, 0:lanes] = high
    lhs[start : start + count, lanes : 2 * lanes] = (x - high.astype(F32)).astype(BF16)


def combine(prod, start, src, f, count):
    def part(k, off):
        return prod[k, pl.ds(start + off, count), :]

    s = SWEEPS
    total = src[f, pl.ds(2 * s, count), :] + src[f, pl.ds(0, count), :]
    for k in range(1, s):
        total += part(k, s + k) + part(k, s - k)
    return total + part(0, s)


def covariance(pack, bands, kind, g, z, xacc, fbuf, prod, lhs, batch, build=None, also=None):
    count, reach, _ = pack.shape
    inner, rows = reach - HALO, reach - 2 * HALO
    per_level = count // g.shape[0]
    xacc[...] = jnp.zeros_like(xacc)

    def step(b, _):
        level = b * batch // per_level
        for i in range(batch):
            at = b * batch + i
            if build is not None:
                pack[at] = build(b, i, pack[at])
            f = pack[at] * g[level]
            fbuf[i] = f
            split_into(lhs, i * reach, f)
        band_products(lhs, bands, kind, prod, batch * reach)
        for i in range(batch):
            v = combine(prod, i * reach, fbuf, i, inner)
            z[b * batch + i] = v
            split_into(lhs, i * inner, v)
            if also is not None:
                also(b, i, v)
        band_products(lhs, bands, kind, prod, batch * inner)
        for i in range(batch):
            v = combine(prod, i * inner, z, b * batch + i, rows)
            xacc[level] += v * pack[b * batch + i, HALO : HALO + rows, :]
        return 0

    lax.fori_loop(0, count // batch, step, 0)


def window_grid(g, west, east):
    lane = lanes_of(g)
    win = jnp.where(lane < WIDE, west, turn(g, WIDE))
    win = jnp.where(lane < 2 * WIDE, win, turn(g, 3 * WIDE))
    win = jnp.where(lane < 3 * WIDE, win, turn(east, 3 * WIDE))
    win = jnp.where(lane < PAIR, win, 0.0)
    return (win + turn(win, PAIR)) * KAPPA**SWEEPS


def fold(x):
    return jnp.sum(x.reshape(x.shape[0] // 8, 8, x.shape[1]), axis=0)


def main_kernel(pack, g_ext, bands, z, xacc, gbuf, fbuf, prod, lhs, *, batch):
    gbuf[...] = g_ext[...] * KAPPA**SWEEPS
    covariance(pack, bands, 0, gbuf, z, xacc, fbuf, prod, lhs, batch)


def join(main, win, cols):
    win = (win + turn(win, PAIR)) * KAPPA**SWEEPS
    lane = lanes_of(win)
    state = jnp.where(lane < HALO, turn(win, -WIDE), main * KAPPA**SWEEPS)
    return jnp.where(lane < cols - HALO, state, turn(win, cols - 3 * WIDE)), win


def first_kernel(
    pack_in, g_ext, grid, near, far, near_ends, far_ends, bands, xmain,
    pack, z, x, p, near_out, far_out, side, sums,
    gbuf, fbuf, prod, lhs, xacc, west, east, *, batch,
):
    del pack_in
    levels, reach, cols = g_ext.shape
    rows = reach - 2 * HALO
    last = west.shape[0] - 1
    west[:, HALO : HALO + rows, :] = by_parity("gx", far[...], near[...])
    east[:, HALO : HALO + rows, :] = by_parity("gx", near[...], far[...])
    for start, at in ((0, 0), (HALO + rows, HALO)):
        a, b = near_ends[:, at : at + HALO, :], far_ends[:, at : at + HALO, :]
        west[:, start : start + HALO, :] = by_parity("gx", b, a)
        east[:, start : start + HALO, :] = by_parity("gx", a, b)
    for l in range(levels):
        gbuf[l] = window_grid(g_ext[l], turn(west[last], -slot_lane(l)), turn(east[last], -slot_lane(l)))
    lane = lax.broadcasted_iota(jnp.int32, (reach, cols), 1)

    def window(b, i, old):
        u = b * (batch // 4) + i // 4
        at = lane & (PAIR - 1)
        old = jnp.where(at < WIDE, turn(west[u], -WIDE * (i % 4)), old)
        return jnp.where(at >= 3 * WIDE, turn(east[u], 3 * WIDE - WIDE * (i % 4)), old)

    covariance(pack, bands, 1, gbuf, z, xacc, fbuf, prod, lhs, batch, window)
    norm = jnp.zeros((8, cols), F32)
    curve = norm
    lane = lane[:rows]
    d_west, d_east = west[last, HALO : HALO + rows, :], east[last, HALO : HALO + rows, :]
    sides = jnp.zeros((rows, cols), F32)
    for l in range(levels):
        state, win = join(xmain[l], xacc[l], cols)
        push = grid[1, l] * state
        x[l] = state
        p[l] = push
        near_out[l] = by_parity("gy", push[rows - HALO :], push[:HALO])
        far_out[l] = by_parity("gy", push[:HALO], push[rows - HALO :])
        norm += fold(grid[0, l] * state)
        curve += fold(push * state)
        base = WIDE * l
        mine = slot_lane(levels + l)
        beside = turn(win, base - HALO) * turn(d_west, base - mine - HALO)
        sides = jnp.where((lane >= base) & (lane < base + HALO), beside, sides)
        beside = turn(win, base + HALO - 3 * WIDE) * turn(d_east, base + HALO - mine)
        sides = jnp.where((lane >= base + HALO) & (lane < base + WIDE), beside, sides)
    side[...] = sides
    near_out[levels] = by_parity("gy", sides[rows - HALO :], sides[:HALO])
    far_out[levels] = by_parity("gy", sides[:HALO], sides[rows - HALO :])
    sums[0] = norm
    sums[1] = curve


def second_kernel(
    mains, wins, p, side, near, far, grid, bands, sums, z_one, zw_one,
    zm, x, share, z_out,
    ext, gbuf, fbuf, prod, lhs, xacc, zw, *, batch,
):
    del z_one
    levels, rows, cols = p.shape
    reach = rows + 2 * HALO
    for l in range(levels + 1):
        ext[l, HALO : HALO + rows, :] = p[l] if l < levels else side[...]
        ext[l, 0:HALO, :] = by_parity("gy", far[l], near[l])
        ext[l, HALO + rows :, :] = by_parity("gy", near[l], far[l])
    me = lax.axis_index("gy")

    def reflect(base, step):
        for l in range(levels + 1):
            for j in range(1, HALO):
                ext[l, base - step * j : base - step * j + 1, :] = -ext[l, base + step * j : base + step * j + 1, :]

    pl.when(me == 0)(lambda: reflect(HALO - 1, 1))
    pl.when(me == lax.axis_size("gy") - 1)(lambda: reflect(HALO + rows, -1))
    lane = lax.broadcasted_iota(jnp.int32, (reach, cols), 1)
    for l in range(levels):
        gbuf[0, l] = ext[l] * KAPPA**SWEEPS
        west = jnp.where(lane < HALO, 0.0, turn(ext[levels], HALO - WIDE * l))
        east = jnp.where(lane < HALO, turn(ext[levels], -HALO - WIDE * l), 0.0)
        gbuf[1, l] = window_grid(ext[l], west, east)
    place = lax.broadcasted_iota(jnp.int32, (rows + HALO, cols), 1)

    def edges(old, win, q):
        new = jnp.where(place < HALO, turn(win, -WIDE - PAIR * q), old)
        return jnp.where(place < cols - HALO, new, turn(win, cols - 3 * WIDE - PAIR * q))

    def first_edges(b, i, _):
        at = b * batch + i
        z_out[at] = edges(z_out[at], zw_one[b * (batch // 2) + i // 2], i % 2)

    def second_edges(b, i, v):
        for q in range(2):
            at = 2 * (b * batch + i) + q
            zm[at] = edges(zm[at], v, q)

    covariance(mains, bands, 0, gbuf.at[0], zm, xacc.at[0], fbuf, prod, lhs, batch, None, first_edges)
    covariance(wins, bands, 1, gbuf.at[1], zw, xacc.at[1], fbuf, prod, lhs, batch, None, second_edges)
    cross = jnp.zeros((8, cols), F32)
    curve = cross
    for l in range(levels):
        state, _ = join(xacc[0, l], xacc[1, l], cols)
        x[l] = state
        cross += fold(p[l] * state)
        curve += fold(grid[1, l] * state * state)
    out = jnp.zeros((1, cols), F32)
    place = lax.broadcasted_iota(jnp.int32, (1, cols), 1)
    for i, part in enumerate((sums[0], sums[1], cross, curve)):
        out = jnp.where(place == i, jnp.sum(jnp.sum(part, axis=0, keepdims=True), axis=1, keepdims=True), out)
    share[...] = jnp.broadcast_to(out, share.shape)


def final_kernel(share, z_one, z_two, x_one, x_two, control, increment, stage, x_stage, sems):
    members, levels, rows, cols = control.shape
    total = jnp.sum(share[...], axis=0, keepdims=True)
    place = lax.broadcasted_iota(jnp.int32, (1, cols), 1)
    n0, c1, c2, c3 = (jnp.sum(jnp.where(place == i, total, 0.0), axis=1, keepdims=True) for i in range(4))
    bn2 = n0 + EPS
    alpha_one = (n0 + c1) / bn2
    t = (EPS - c1) / bn2
    rr = jnp.maximum((c2 + 2.0 * t * c1 + t * t * n0) / bn2, 0.0)
    beta_sq = rr + EPS
    alpha_two = (rr + jnp.maximum((c3 + 2.0 * t * c2 + t * t * c1) / bn2, 0.0)) / beta_sq
    det = alpha_one * alpha_two - beta_sq
    coef_b = -1.0 / det
    coef_a = (alpha_two - t) / det
    copies = []
    part = stage.shape[0] // (sems.shape[0] - 1)
    for c in range(sems.shape[0] - 1):

        def body(i, _):
            f = c * part + i
            one, two = z_one[f, SWEEPS : SWEEPS + rows, :], z_two[f, SWEEPS : SWEEPS + rows, :]
            stage[f] = coef_a * one + coef_b * two
            return 0

        lax.fori_loop(0, part, body, 0, unroll=4)
        level, first = divmod(c * part, members)
        copies.append(
            pltpu.make_async_copy(
                stage.at[pl.ds(c * part, part)], control.at[pl.ds(first, part), level], sems.at[c]
            )
        )
        copies[-1].start()
    x_stage[...] = coef_a * x_one[...] + coef_b * x_two[...]
    copies.append(pltpu.make_async_copy(x_stage, increment, sems.at[sems.shape[0] - 1]))
    copies[-1].start()
    for copy in copies:
        copy.wait()


def on_device(ensemble, obs_cell, obs_level, innovation, obs_weight):
    members, levels, rows, cols = ensemble.shape
    fields = members * levels
    reach = rows + 2 * HALO
    batch = 16
    strips = fields // 8 + 1
    devices = lax.axis_size("gy") * lax.axis_size("gx")
    hbm = pl.BlockSpec(memory_space=pltpu.HBM)

    def struct(*shape):
        return jax.ShapeDtypeStruct(shape, F32)

    def call(kernel, outs, ins, scratch=(), limit=16, work=2, **kw):
        return pl.pallas_call(
            kernel,
            out_shape=outs,
            in_specs=[VMEM] * ins if isinstance(ins, int) else ins,
            out_specs=jax.tree.map(lambda _: VMEM, outs),
            scratch_shapes=scratch,
            compiler_params=pltpu.CompilerParams(vmem_limit_bytes=limit * 2**20),
            cost_estimate=pl.CostEstimate(flops=work * 10**9, bytes_accessed=10**6, transcendentals=0),
            **kw,
        )

    bands = jnp.asarray(band_matrices(cols), BF16)
    obs = obs_cell.shape
    edge = pltpu.VMEM((members, levels, 16, cols), BF16)
    grid, near, far = call(
        scatter_kernel,
        (struct(2, levels, rows, cols), struct(fields + levels, HALO, cols), struct(fields + levels, HALO, cols)),
        [hbm] * 5,
        [pltpu.VMEM(obs, jnp.int32)] * 2 + [pltpu.VMEM(obs, F32)] * 2 + [edge, edge, pltpu.SemaphoreType.DMA((6,))],
        limit=60,
    )(ensemble, obs_cell, obs_level, innovation, obs_weight)
    near, far = swap(near, "gy", 0), swap(far, "gy", 1)
    main_shape, win_shape = struct(fields, reach, cols), struct(fields // 2, reach, cols)
    g_shape = struct(levels, reach, cols)
    own_shape, end_shape = struct(strips, rows, cols), struct(strips, 2 * HALO, cols)
    mains, wins, near_own, far_own, g_ext, mirror, bands = call(
        own_kernel,
        (
            main_shape,
            win_shape,
            own_shape,
            own_shape,
            g_shape,
            struct(2, fields + levels, HALO, cols),
            jax.ShapeDtypeStruct((2, 2 * cols, SWEEPS * cols), BF16),
        ),
        [hbm, VMEM, hbm],
        [pltpu.VMEM(ensemble.shape, BF16), pltpu.SemaphoreType.DMA((3,))],
    )(ensemble, grid, bands)
    near_own, far_own = swap(near_own, "gx", 0), swap(far_own, "gx", 1)
    mains, wins, g_ext, near, far = call(
        halo_kernel, (main_shape, win_shape, g_shape, end_shape, end_shape), 6, input_output_aliases={3: 0, 4: 1, 5: 2}
    )(near, far, mirror, mains, wins, g_ext)
    near, far = swap(near, "gx", 0), swap(far, "gx", 1)
    work = (
        pltpu.VMEM((batch, reach, cols), F32),
        pltpu.VMEM((SWEEPS, batch * reach, cols), F32),
        pltpu.VMEM((batch * reach, 2 * cols), BF16),
    )
    gbuf = pltpu.VMEM((levels, reach, cols), F32)
    zm_shape, zw_shape = struct(fields, reach - HALO, cols), struct(fields // 2, reach - HALO, cols)
    zm_one, xmain = call(
        functools.partial(main_kernel, batch=batch), (zm_shape, struct(levels, rows, cols)), 3, (gbuf, *work)
    )(mains, g_ext, bands)
    wins, zw_one, x_one, p, near, far, side, sums = call(
        functools.partial(first_kernel, batch=batch),
        (
            win_shape,
            zw_shape,
            struct(levels, rows, cols),
            struct(levels, rows, cols),
            struct(levels + 1, HALO, cols),
            struct(levels + 1, HALO, cols),
            struct(rows, cols),
            struct(2, 8, cols),
        ),
        9,
        (gbuf, *work, pltpu.VMEM((levels, rows, cols), F32), *[pltpu.VMEM((strips, reach, cols), F32)] * 2),
        input_output_aliases={0: 0},
    )(wins, g_ext, grid, near_own, far_own, near, far, bands, xmain)
    near, far = swap(near, "gy", 0), swap(far, "gy", 1)
    zm_two, x_two, share, zm_one = call(
        functools.partial(second_kernel, batch=batch),
        (zm_shape, struct(levels, rows, cols), struct(devices, cols), zm_shape),
        11,
        (
            pltpu.VMEM((levels + 1, reach, cols), F32),
            pltpu.VMEM((2, levels, reach, cols), F32),
            *work,
            pltpu.VMEM((2, levels, rows, cols), F32),
            pltpu.VMEM((fields // 2, reach - HALO, cols), F32),
        ),
        input_output_aliases={9: 3},
    )(mains, wins, p, side, near, far, grid, bands, sums, zm_one, zw_one)
    share = lax.all_to_all(share, ("gy", "gx"), 0, 0, tiled=True)
    chunks = 8
    return pl.pallas_call(
        final_kernel,
        out_shape=(struct(members, levels, rows, cols), struct(levels, rows, cols)),
        in_specs=[VMEM] * 5,
        out_specs=(hbm, hbm),
        scratch_shapes=[
            pltpu.VMEM((fields, rows, cols), F32),
            pltpu.VMEM((levels, rows, cols), F32),
            pltpu.SemaphoreType.DMA((chunks + 1,)),
        ],
        compiler_params=pltpu.CompilerParams(vmem_limit_bytes=16 * 2**20),
    )(share, zm_one, zm_two, x_one, x_two)


def solution(mesh):
    return jax.shard_map(
        on_device,
        mesh=mesh,
        in_specs=(
            P(None, None, "gy", "gx"),
            P("gy", "gx", None),
            P("gy", "gx", None),
            P("gy", "gx", None),
            P("gy", "gx", None),
        ),
        out_specs=(P(None, None, "gy", "gx"), P(None, "gy", "gx")),
        check_vma=False,
    )
```

```python
import functools
import math

import jax
import jax.numpy as jnp
import numpy as np
from jax import lax
from jax.experimental import pallas as pl
from jax.experimental.pallas import tpu as pltpu
from jax.sharding import PartitionSpec as P

SWEEPS = 4
KAPPA = 0.2
EPS = 1e-06
HALO = 2 * SWEEPS
WIDE = 2 * HALO
PAIR = 4 * WIDE
VMEM = pl.BlockSpec(memory_space=pltpu.VMEM)
F32 = jnp.float32
BF16 = jnp.bfloat16


def band_matrices(lanes):
    out = np.zeros((4, 2, lanes, SWEEPS * lanes), np.float32)
    lane = np.arange(lanes)
    for variant in range(4):
        for kind in range(2):
            col, part = lane, 0 * lane
            if kind == 1:
                j = lane % PAIR
                col = np.where(j < 2 * WIDE, j - WIDE, lanes - 3 * WIDE + j)
                part = lane // (2 * WIDE)
            inside = np.ones(lanes, bool)
            if variant % 2:
                inside &= col >= 0
            if variant // 2:
                inside &= col < lanes
            near = (np.abs(lane[:, None] - lane[None, :]) <= 1) & (part[:, None] == part[None, :])
            band = (near & inside[:, None] & inside[None, :]).astype(np.float64)
            power = [np.diag(inside.astype(np.float64))]
            for _ in range(SWEEPS):
                power.append(power[-1] @ band)
            for j in range(SWEEPS):
                q = sum(
                    math.comb(SWEEPS, k) * math.comb(SWEEPS - k, (SWEEPS - k - j) // 2) * power[k]
                    for k in range(SWEEPS - j + 1)
                    if (SWEEPS - k - j) % 2 == 0
                )
                out[variant, kind, :, j * lanes : (j + 1) * lanes] = q
    return out


def swap(x, axis, odd):
    count = lax.axis_size(axis)
    return lax.ppermute(x, axis, [(i + a, i + 1 - a) for i in range(odd, count - 1, 2) for a in range(2)])


def by_parity(axis, even, odd):
    me = jnp.full(even.shape, lax.axis_index(axis), jnp.int32)
    return jnp.where((me & 1) == 0, even, odd)


def turn(x, amount):
    amount %= x.shape[-1]
    return pltpu.roll(x, amount, x.ndim - 1) if amount else x


def lanes_of(x):
    return lax.broadcasted_iota(jnp.int32, x.shape, x.ndim - 1)


def scatter_kernel(ens, cell_in, level_in, innov_in, weight_in, grid, near, far, cell, level, innov, weight, first, last, sem):
    members, levels, rows, cols = ens.shape
    obs = cell.shape[-1]
    copies = [
        pltpu.make_async_copy(a, b, sem.at[i])
        for i, (a, b) in enumerate(
            (
                (cell_in, cell),
                (level_in, level),
                (innov_in, innov),
                (weight_in, weight),
                (ens.at[:, :, 0:16, :], first),
                (ens.at[:, :, rows - 16 : rows, :], last),
            )
        )
    ]
    for c in copies:
        c.start()
    for c in copies[:4]:
        c.wait()
    span = 256
    row_iota = lax.broadcasted_iota(jnp.int32, (levels * rows, span), 0)
    col_iota = lax.broadcasted_iota(jnp.int32, (cols, span), 0)
    acc = jnp.zeros((4 * levels * rows, cols), F32)
    for start in range(0, obs, span):
        at = slice(start, start + span)
        spot = cell[0, :, at]
        here = row_iota == level[0, :, at] * rows + spot // cols
        w = weight[0, :, at]
        parts = []
        for value in (w * innov[0, :, at], w):
            high = value.astype(BF16).astype(F32)
            parts += [high, value - high]
        left = jnp.concatenate([jnp.where(here, part, 0.0).astype(BF16) for part in parts], axis=0)
        right = jnp.where(col_iota == spot % cols, 1.0, 0.0).astype(BF16)
        acc += lax.dot_general(left, right, (((1,), (1,)), ((), ())), preferred_element_type=F32)
    n = levels * rows
    g = acc[:n] + acc[n : 2 * n]
    d = acc[2 * n : 3 * n] + acc[3 * n :]
    fields = members * levels
    for l in range(levels):
        grid[0, l] = g[l * rows : (l + 1) * rows]
        grid[1, l] = d[l * rows : (l + 1) * rows]
        up = g[l * rows : l * rows + HALO]
        down = g[(l + 1) * rows - HALO : (l + 1) * rows]
        near[fields + l] = by_parity("gy", down, up)
        far[fields + l] = by_parity("gy", up, down)
    for c in copies[4:]:
        c.wait()

    def edge(m, _):
        for l in range(levels):
            up = first[m, l].astype(F32)[:HALO]
            down = last[m, l].astype(F32)[16 - HALO :]
            near[l * members + m] = by_parity("gy", down, up)
            far[l * members + m] = by_parity("gy", up, down)
        return 0

    lax.fori_loop(0, members, edge, 0)


def slot_lane(t):
    return PAIR * (t % 2) + WIDE * (t // 2)


def strip(xs, at, near, far):
    lane = lanes_of(xs[0])
    west = east = jnp.zeros_like(xs[0])
    for t, x in enumerate(xs):
        base = slot_lane(t)
        here = (lane >= base) & (lane < base + WIDE)
        west = jnp.where(here, turn(x, base), west)
        east = jnp.where(here, turn(x, base + WIDE), east)
    near[at] = by_parity("gx", east, west)
    far[at] = by_parity("gx", west, east)


def arrange(u, get, mains, wins, near, far, spans):
    xs = [get(8 * u + t) for t in range(8)]
    lane = lanes_of(xs[0])

    def put(ref, f, value):
        at = 0
        for start, count in spans:
            ref[f, start : start + count, :] = value[at : at + count]
            at += count

    for t, x in enumerate(xs):
        put(mains, 8 * u + t, x)
    strip(xs, u, near, far)
    for v in range(4):
        win = jnp.zeros_like(xs[0])
        for q in range(2):
            x = xs[2 * v + q]
            at = lane - PAIR * q
            win = jnp.where((at >= WIDE) & (at < 2 * WIDE), turn(x, PAIR * q + WIDE), win)
            win = jnp.where((at >= 2 * WIDE) & (at < 3 * WIDE), turn(x, PAIR * q + 3 * WIDE), win)
        put(wins, 4 * u + v, win)


def own_kernel(ens_in, grid, bands_in, mains, wins, near, far, g_ext, mirror, bands, ens, sem):
    members, levels, rows, cols = ens.shape
    fields = members * levels
    gx = lax.axis_index("gx")
    variant = jnp.where(gx == 0, 1, 0) + jnp.where(gx == lax.axis_size("gx") - 1, 2, 0)
    copies = [pltpu.make_async_copy(ens_in, ens, sem.at[0])]
    for half in range(2):
        part = bands.at[:, half * cols : (half + 1) * cols, :]
        copies.append(pltpu.make_async_copy(bands_in.at[variant], part, sem.at[1 + half]))
    for c in copies:
        c.start()
    for c in copies:
        c.wait()
    spans = ((HALO, rows),)

    def group(u, _):
        l = 8 * u // members
        arrange(u, lambda f: ens[f - l * members, l].astype(F32), mains, wins, near, far, spans)
        return 0

    lax.fori_loop(0, fields // 8, group, 0)
    strip([grid[k, l] for k in range(2) for l in range(levels)], fields // 8, near, far)
    for l in range(levels):
        g_ext[l, HALO : HALO + rows, :] = grid[0, l]
    mirror[...] = jnp.zeros_like(mirror)
    me = lax.axis_index("gy")
    row = lax.broadcasted_iota(jnp.int32, (HALO, cols), 0)

    def flip(x, step):
        out = jnp.zeros((HALO, cols), F32)
        for j in range(1, HALO):
            if step > 0:
                out = jnp.where(row == HALO - 1 - j, x[j - 1 : j], out)
            else:
                out = jnp.where(row == j, x[HALO - j : HALO - j + 1], out)
        return out

    def side(step):
        at = 0 if step > 0 else rows - HALO
        slot = 0 if step > 0 else 1
        start = 0 if step > 0 else rows - 16
        skip = 0 if step > 0 else 16 - HALO

        def body(m, _):
            for l in range(levels):
                x = ens[m, l, start : start + 16, :].astype(F32)[skip : skip + HALO]
                mirror[slot, l * members + m] = flip(x, step)
            return 0

        lax.fori_loop(0, members, body, 0)
        for l in range(levels):
            mirror[slot, fields + l] = -flip(grid[0, l, at : at + HALO, :], step)

    pl.when(me == 0)(lambda: side(1))
    pl.when(me == lax.axis_size("gy") - 1)(lambda: side(-1))


def halo_kernel(from_near, from_far, mirror, *refs):
    mains, wins, g_ext, near, far = refs[4:]
    levels, reach, cols = g_ext.shape
    fields = mirror.shape[1] - levels
    spans = ((0, HALO), (reach - HALO, HALO))

    def get(f):
        a, b = from_near[f], from_far[f]
        return jnp.concatenate([by_parity("gy", b, a) + mirror[0, f], by_parity("gy", a, b) + mirror[1, f]], axis=0)

    def group(u, _):
        arrange(u, get, mains, wins, near, far, spans)
        return 0

    lax.fori_loop(0, fields // 8, group, 0)
    ends = [get(fields + l) for l in range(levels)]
    strip(ends, fields // 8, near, far)
    for l in range(levels):
        g_ext[l, 0:HALO, :] = ends[l][:HALO]
        g_ext[l, reach - HALO :, :] = ends[l][HALO:]


def band_products(lhs, bands, kind, out, count):
    lanes = lhs.shape[1] // 2
    for half in range(SWEEPS // 2):
        r = jnp.dot(
            lhs[0:count, :],
            bands[kind, :, half * 2 * lanes : (half + 1) * 2 * lanes],
            preferred_element_type=F32,
        )
        out[2 * half, 0:count, :] = r[:, :lanes]
        out[2 * half + 1, 0:count, :] = r[:, lanes:]


def split_into(lhs, start, x):
    count, lanes = x.shape
    high = x.astype(BF16)
    lhs[start : start + count, 0:lanes] = high
    lhs[start : start + count, lanes : 2 * lanes] = (x - high.astype(F32)).astype(BF16)


def combine(part, src, count):
    total = src(2 * SWEEPS) + src(0)
    for k in range(1, SWEEPS):
        total += part(k, SWEEPS + k) + part(k, SWEEPS - k)
    return total + part(0, SWEEPS)


def rows_of(prod, start, count):
    return lambda k, off: prod[k, pl.ds(start + off, count), :]


def field_rows(ref, f, count, base=0):
    return lambda off: ref[f, pl.ds(base + off, count), :]


def interior(pack, g, bands, z, first_edge, second_edge, xacc, fbuf, prod, lhs, batch, also):
    count, reach, _ = pack.shape
    rows = reach - 2 * HALO
    mid, core = rows - HALO, rows - 2 * HALO
    per_level = count // g.shape[0]
    xacc[...] = jnp.zeros_like(xacc)

    def keep(edge, at, start, size):
        for k in range(SWEEPS):
            edge[k, at, HALO : 2 * HALO, :] = prod[k, start : start + HALO, :]
            edge[k, count + at, 0:HALO, :] = prod[k, start + size - HALO : start + size, :]

    def step(b, _):
        level = b * batch // per_level
        for i in range(batch):
            f = pack[b * batch + i, HALO : HALO + rows, :] * g[level]
            fbuf[i, 0:rows, :] = f
            split_into(lhs, i * rows, f)
        band_products(lhs, bands, 0, prod, batch * rows)
        for i in range(batch):
            at = b * batch + i
            v = combine(rows_of(prod, i * rows, mid), field_rows(fbuf, i, mid), mid)
            z[at, HALO : HALO + mid, :] = v
            keep(first_edge, at, i * rows, rows)
            split_into(lhs, i * mid, v)
            if also is not None:
                also(b, i)
        band_products(lhs, bands, 0, prod, batch * mid)
        for i in range(batch):
            at = b * batch + i
            v = combine(rows_of(prod, i * mid, core), field_rows(z, at, core, HALO), core)
            keep(second_edge, at, i * mid, mid)
            xacc[level, HALO : HALO + core, :] += v * pack[at, 2 * HALO : 2 * HALO + core, :]
        return 0

    lax.fori_loop(0, count // batch, step, 0)


def edge_rows(pack, g, bands, z, first_edge, second_edge, xacc, ends, lhs):
    count, reach, lanes = pack.shape
    rows = reach - 2 * HALO
    per_level = count // g.shape[0]
    sides = [(side, f) for side in range(2) for f in range(count)]

    def products(edge):
        for half in range(SWEEPS // 2):
            r = jnp.dot(
                lhs[0 : 2 * count * HALO, :],
                bands[0, :, half * 2 * lanes : (half + 1) * 2 * lanes],
                preferred_element_type=F32,
            )
            for t in range(2):
                part = r[:, t * lanes : (t + 1) * lanes].reshape(2 * count, HALO, lanes)
                edge[2 * half + t, 0:count, 0:HALO, :] = part[:count]
                edge[2 * half + t, count:, HALO : 2 * HALO, :] = part[count:]

    def near(edge, j):
        return lambda k, off: edge[k, j, pl.ds(off, HALO), :]

    for side, f in sides:
        base = side * rows
        x = pack[f, base : base + 2 * HALO, :] * g[f // per_level, base : base + 2 * HALO, :]
        j = side * count + f
        ends[j] = x
        split_into(lhs, j * HALO, x[side * HALO : (side + 1) * HALO])
    products(first_edge)
    for side, f in sides:
        j = side * count + f
        v = combine(near(first_edge, j), field_rows(ends, j, HALO), HALO)
        z[f, side * rows : side * rows + HALO, :] = v
        split_into(lhs, j * HALO, v)
    products(second_edge)
    for side in range(2):
        for level in range(g.shape[0]):
            total = jnp.zeros((HALO, lanes), F32)
            for f in range(level * per_level, (level + 1) * per_level):
                base = side * (rows - HALO)
                v = combine(near(second_edge, side * count + f), field_rows(z, f, HALO, base), HALO)
                total += v * pack[f, HALO + base : 2 * HALO + base, :]
            xacc[level, base : base + HALO, :] = total


def covariance(pack, bands, kind, g, z, xacc, fbuf, prod, lhs, batch, build=None, also=None):
    count, reach, _ = pack.shape
    inner, rows = reach - HALO, reach - 2 * HALO
    per_level = count // g.shape[0]
    xacc[...] = jnp.zeros_like(xacc)

    def step(b, _):
        level = b * batch // per_level
        for i in range(batch):
            at = b * batch + i
            if build is not None:
                pack[at] = build(b, i, pack[at])
            f = pack[at] * g[level]
            fbuf[i] = f
            split_into(lhs, i * reach, f)
        band_products(lhs, bands, kind, prod, batch * reach)
        for i in range(batch):
            v = combine(rows_of(prod, i * reach, inner), field_rows(fbuf, i, inner), inner)
            z[b * batch + i] = v
            split_into(lhs, i * inner, v)
            if also is not None:
                also(b, i, v)
        band_products(lhs, bands, kind, prod, batch * inner)
        for i in range(batch):
            v = combine(rows_of(prod, i * inner, rows), field_rows(z, b * batch + i, rows), rows)
            xacc[level] += v * pack[b * batch + i, HALO : HALO + rows, :]
        return 0

    lax.fori_loop(0, count // batch, step, 0)


def window_grid(g, west, east):
    lane = lanes_of(g)
    win = jnp.where(lane < WIDE, west, turn(g, WIDE))
    win = jnp.where(lane < 2 * WIDE, win, turn(g, 3 * WIDE))
    win = jnp.where(lane < 3 * WIDE, win, turn(east, 3 * WIDE))
    win = jnp.where(lane < PAIR, win, 0.0)
    return (win + turn(win, PAIR)) * KAPPA**SWEEPS


def fold(x):
    return jnp.sum(x.reshape(x.shape[0] // 8, 8, x.shape[1]), axis=0)


def interior_kernel(pack, g, bands, z, first_edge, second_edge, xacc, gbuf, fbuf, prod, lhs, *, batch):
    gbuf[...] = g[0] * KAPPA**SWEEPS
    interior(pack, gbuf, bands, z, first_edge, second_edge, xacc, fbuf, prod, lhs, batch, None)


def edge_kernel(pack, g_ext, bands, *refs):
    z, first_edge, second_edge, xacc, gbuf, ends, lhs = refs[4:]
    gbuf[...] = g_ext[...] * KAPPA**SWEEPS
    edge_rows(pack, gbuf, bands, z, first_edge, second_edge, xacc, ends, lhs)


def put_edges(old, win, q):
    lane = lanes_of(old)
    cols = old.shape[1]
    new = jnp.where(lane < HALO, turn(win, -WIDE - PAIR * q), old)
    return jnp.where(lane < cols - HALO, new, turn(win, cols - 3 * WIDE - PAIR * q))


def second_interior_kernel(
    pack, p, bands, z_one, zw_one,
    z, first_edge, second_edge, xacc, z_out,
    gbuf, fbuf, prod, lhs, *, batch,
):
    del z_one
    gbuf[...] = p[...] * KAPPA**SWEEPS

    def first_edges(b, i):
        at = b * batch + i
        z_out[at] = put_edges(z_out[at], zw_one[b * (batch // 2) + i // 2], i % 2)

    interior(pack, gbuf, bands, z, first_edge, second_edge, xacc, fbuf, prod, lhs, batch, first_edges)


def join(main, win, cols):
    win = (win + turn(win, PAIR)) * KAPPA**SWEEPS
    lane = lanes_of(win)
    state = jnp.where(lane < HALO, turn(win, -WIDE), main * KAPPA**SWEEPS)
    return jnp.where(lane < cols - HALO, state, turn(win, cols - 3 * WIDE)), win


def first_kernel(
    pack_in, g_ext, grid, near, far, near_ends, far_ends, bands, xmain,
    pack, z, x, p, near_out, far_out, side, sums,
    gbuf, fbuf, prod, lhs, xacc, west, east, *, batch,
):
    del pack_in
    levels, reach, cols = g_ext.shape
    rows = reach - 2 * HALO
    last = west.shape[0] - 1
    west[:, HALO : HALO + rows, :] = by_parity("gx", far[...], near[...])
    east[:, HALO : HALO + rows, :] = by_parity("gx", near[...], far[...])
    for start, at in ((0, 0), (HALO + rows, HALO)):
        a, b = near_ends[:, at : at + HALO, :], far_ends[:, at : at + HALO, :]
        west[:, start : start + HALO, :] = by_parity("gx", b, a)
        east[:, start : start + HALO, :] = by_parity("gx", a, b)
    for l in range(levels):
        gbuf[l] = window_grid(g_ext[l], turn(west[last], -slot_lane(l)), turn(east[last], -slot_lane(l)))
    lane = lax.broadcasted_iota(jnp.int32, (reach, cols), 1)

    def window(b, i, old):
        u = b * (batch // 4) + i // 4
        at = lane & (PAIR - 1)
        old = jnp.where(at < WIDE, turn(west[u], -WIDE * (i % 4)), old)
        return jnp.where(at >= 3 * WIDE, turn(east[u], 3 * WIDE - WIDE * (i % 4)), old)

    covariance(pack, bands, 1, gbuf, z, xacc, fbuf, prod, lhs, batch, window)
    norm = jnp.zeros((8, cols), F32)
    curve = norm
    lane = lane[:rows]
    d_west, d_east = west[last, HALO : HALO + rows, :], east[last, HALO : HALO + rows, :]
    sides = jnp.zeros((rows, cols), F32)
    for l in range(levels):
        state, win = join(xmain[l], xacc[l], cols)
        push = grid[1, l] * state
        x[l] = state
        p[l] = push
        near_out[l] = by_parity("gy", push[rows - HALO :], push[:HALO])
        far_out[l] = by_parity("gy", push[:HALO], push[rows - HALO :])
        norm += fold(grid[0, l] * state)
        curve += fold(push * state)
        base = WIDE * l
        mine = slot_lane(levels + l)
        beside = turn(win, base - HALO) * turn(d_west, base - mine - HALO)
        sides = jnp.where((lane >= base) & (lane < base + HALO), beside, sides)
        beside = turn(win, base + HALO - 3 * WIDE) * turn(d_east, base + HALO - mine)
        sides = jnp.where((lane >= base + HALO) & (lane < base + WIDE), beside, sides)
    side[...] = sides
    near_out[levels] = by_parity("gy", sides[rows - HALO :], sides[:HALO])
    far_out[levels] = by_parity("gy", sides[:HALO], sides[rows - HALO :])
    sums[0] = norm
    sums[1] = curve


def second_kernel(
    mains, wins, p, side, near, far, grid, bands, sums, z_in, first_in, second_in, xmain_in,
    x, share, zm, first_edge, second_edge, xmain,
    ext, gbuf, fbuf, prod, lhs, xacc, zw, ends, *, batch,
):
    del z_in, first_in, second_in, xmain_in
    levels, rows, cols = p.shape
    reach = rows + 2 * HALO
    for l in range(levels + 1):
        ext[l, HALO : HALO + rows, :] = p[l] if l < levels else side[...]
        ext[l, 0:HALO, :] = by_parity("gy", far[l], near[l])
        ext[l, HALO + rows :, :] = by_parity("gy", near[l], far[l])
    me = lax.axis_index("gy")

    def reflect(base, step):
        for l in range(levels + 1):
            for j in range(1, HALO):
                ext[l, base - step * j : base - step * j + 1, :] = -ext[l, base + step * j : base + step * j + 1, :]

    pl.when(me == 0)(lambda: reflect(HALO - 1, 1))
    pl.when(me == lax.axis_size("gy") - 1)(lambda: reflect(HALO + rows, -1))
    lane = lax.broadcasted_iota(jnp.int32, (reach, cols), 1)
    for l in range(levels):
        gbuf[0, l] = ext[l] * KAPPA**SWEEPS
        west = jnp.where(lane < HALO, 0.0, turn(ext[levels], HALO - WIDE * l))
        east = jnp.where(lane < HALO, turn(ext[levels], -HALO - WIDE * l), 0.0)
        gbuf[1, l] = window_grid(ext[l], west, east)

    def second_edges(b, i, v):
        for q in range(2):
            at = 2 * (b * batch + i) + q
            zm[at] = put_edges(zm[at], v, q)

    edge_rows(mains, gbuf.at[0], bands, zm, first_edge, second_edge, xmain, ends, lhs)
    covariance(wins, bands, 1, gbuf.at[1], zw, xacc, fbuf, prod, lhs, batch, None, second_edges)
    cross = jnp.zeros((8, cols), F32)
    curve = cross
    for l in range(levels):
        state, _ = join(xmain[l], xacc[l], cols)
        x[l] = state
        cross += fold(p[l] * state)
        curve += fold(grid[1, l] * state * state)
    out = jnp.zeros((1, cols), F32)
    place = lax.broadcasted_iota(jnp.int32, (1, cols), 1)
    for i, part in enumerate((sums[0], sums[1], cross, curve)):
        out = jnp.where(place == i, jnp.sum(jnp.sum(part, axis=0, keepdims=True), axis=1, keepdims=True), out)
    share[...] = jnp.broadcast_to(out, share.shape)


def final_kernel(share, z_one, z_two, x_one, x_two, control, increment, stage, x_stage, sems):
    members, levels, rows, cols = control.shape
    total = jnp.sum(share[...], axis=0, keepdims=True)
    place = lax.broadcasted_iota(jnp.int32, (1, cols), 1)
    n0, c1, c2, c3 = (jnp.sum(jnp.where(place == i, total, 0.0), axis=1, keepdims=True) for i in range(4))
    bn2 = n0 + EPS
    alpha_one = (n0 + c1) / bn2
    t = (EPS - c1) / bn2
    rr = jnp.maximum((c2 + 2.0 * t * c1 + t * t * n0) / bn2, 0.0)
    beta_sq = rr + EPS
    alpha_two = (rr + jnp.maximum((c3 + 2.0 * t * c2 + t * t * c1) / bn2, 0.0)) / beta_sq
    det = alpha_one * alpha_two - beta_sq
    coef_b = -1.0 / det
    coef_a = (alpha_two - t) / det
    copies = []
    part = stage.shape[0] // (sems.shape[0] - 1)
    for c in range(sems.shape[0] - 1):

        def body(i, _):
            f = c * part + i
            one, two = z_one[f, SWEEPS : SWEEPS + rows, :], z_two[f, SWEEPS : SWEEPS + rows, :]
            stage[f] = coef_a * one + coef_b * two
            return 0

        lax.fori_loop(0, part, body, 0, unroll=4)
        level, first = divmod(c * part, members)
        copies.append(
            pltpu.make_async_copy(
                stage.at[pl.ds(c * part, part)], control.at[pl.ds(first, part), level], sems.at[c]
            )
        )
        copies[-1].start()
    x_stage[...] = coef_a * x_one[...] + coef_b * x_two[...]
    copies.append(pltpu.make_async_copy(x_stage, increment, sems.at[sems.shape[0] - 1]))
    copies[-1].start()
    for copy in copies:
        copy.wait()


def on_device(ensemble, obs_cell, obs_level, innovation, obs_weight):
    members, levels, rows, cols = ensemble.shape
    fields = members * levels
    reach = rows + 2 * HALO
    batch = 16
    strips = fields // 8 + 1
    devices = lax.axis_size("gy") * lax.axis_size("gx")
    hbm = pl.BlockSpec(memory_space=pltpu.HBM)

    def struct(*shape):
        return jax.ShapeDtypeStruct(shape, F32)

    def call(kernel, outs, ins, scratch=(), limit=16, work=2, **kw):
        return pl.pallas_call(
            kernel,
            out_shape=outs,
            in_specs=[VMEM] * ins if isinstance(ins, int) else ins,
            out_specs=jax.tree.map(lambda _: VMEM, outs),
            scratch_shapes=scratch,
            compiler_params=pltpu.CompilerParams(vmem_limit_bytes=limit * 2**20),
            cost_estimate=pl.CostEstimate(flops=work * 10**9, bytes_accessed=10**6, transcendentals=0),
            **kw,
        )

    bands = jnp.asarray(band_matrices(cols), BF16)
    obs = obs_cell.shape
    edge = pltpu.VMEM((members, levels, 16, cols), BF16)
    grid, near, far = call(
        scatter_kernel,
        (struct(2, levels, rows, cols), struct(fields + levels, HALO, cols), struct(fields + levels, HALO, cols)),
        [hbm] * 5,
        [pltpu.VMEM(obs, jnp.int32)] * 2 + [pltpu.VMEM(obs, F32)] * 2 + [edge, edge, pltpu.SemaphoreType.DMA((6,))],
        limit=60,
    )(ensemble, obs_cell, obs_level, innovation, obs_weight)
    near, far = swap(near, "gy", 0), swap(far, "gy", 1)
    main_shape, win_shape = struct(fields, reach, cols), struct(fields // 2, reach, cols)
    g_shape = struct(levels, reach, cols)
    own_shape, end_shape = struct(strips, rows, cols), struct(strips, 2 * HALO, cols)
    mains, wins, near_own, far_own, g_ext, mirror, bands = call(
        own_kernel,
        (
            main_shape,
            win_shape,
            own_shape,
            own_shape,
            g_shape,
            struct(2, fields + levels, HALO, cols),
            jax.ShapeDtypeStruct((2, 2 * cols, SWEEPS * cols), BF16),
        ),
        [hbm, VMEM, hbm],
        [pltpu.VMEM(ensemble.shape, BF16), pltpu.SemaphoreType.DMA((3,))],
    )(ensemble, grid, bands)
    near_own, far_own = swap(near_own, "gx", 0), swap(far_own, "gx", 1)
    work = (
        pltpu.VMEM((batch, reach, cols), F32),
        pltpu.VMEM((SWEEPS, batch * reach, cols), F32),
        pltpu.VMEM((batch * reach, 2 * cols), BF16),
    )
    zm_shape, zw_shape = struct(fields, reach - HALO, cols), struct(fields // 2, reach - HALO, cols)
    state_shape = struct(levels, rows, cols)
    edge_shape = struct(SWEEPS, 2 * fields, 2 * HALO, cols)
    part_shapes = (zm_shape, edge_shape, edge_shape, state_shape)
    ends = pltpu.VMEM((2 * fields, 2 * HALO, cols), F32)
    part = call(
        functools.partial(interior_kernel, batch=batch),
        part_shapes,
        3,
        (pltpu.VMEM((levels, rows, cols), F32), *work),
    )(mains, grid, bands)
    mains, wins, g_ext, near, far = call(
        halo_kernel, (main_shape, win_shape, g_shape, end_shape, end_shape), 7, input_output_aliases={3: 0, 4: 1, 5: 2}
    )(near, far, mirror, mains, wins, g_ext, part[3])
    near, far = swap(near, "gx", 0), swap(far, "gx", 1)
    gbuf = pltpu.VMEM((levels, reach, cols), F32)
    zm_one, _, _, xmain = call(
        edge_kernel, part_shapes, 7, (gbuf, ends, work[2]), input_output_aliases={3: 0, 4: 1, 5: 2, 6: 3}
    )(mains, g_ext, bands, *part)
    wins, zw_one, x_one, p, near, far, side, sums = call(
        functools.partial(first_kernel, batch=batch),
        (
            win_shape,
            zw_shape,
            struct(levels, rows, cols),
            struct(levels, rows, cols),
            struct(levels + 1, HALO, cols),
            struct(levels + 1, HALO, cols),
            struct(rows, cols),
            struct(2, 8, cols),
        ),
        9,
        (gbuf, *work, pltpu.VMEM((levels, rows, cols), F32), *[pltpu.VMEM((strips, reach, cols), F32)] * 2),
        input_output_aliases={0: 0},
    )(wins, g_ext, grid, near_own, far_own, near, far, bands, xmain)
    near, far = swap(near, "gy", 0), swap(far, "gy", 1)
    *part, zm_one = call(
        functools.partial(second_interior_kernel, batch=batch),
        (*part_shapes, zm_shape),
        5,
        (pltpu.VMEM((levels, rows, cols), F32), *work),
        input_output_aliases={3: 4},
    )(mains, p, bands, zm_one, zw_one)
    x_two, share, zm_two, _, _, _ = call(
        functools.partial(second_kernel, batch=batch),
        (state_shape, struct(devices, cols), *part_shapes),
        13,
        (
            pltpu.VMEM((levels + 1, reach, cols), F32),
            pltpu.VMEM((2, levels, reach, cols), F32),
            *work,
            pltpu.VMEM((levels, rows, cols), F32),
            pltpu.VMEM((fields // 2, reach - HALO, cols), F32),
            ends,
        ),
        input_output_aliases={9: 2, 10: 3, 11: 4, 12: 5},
    )(mains, wins, p, side, near, far, grid, bands, sums, *part)
    share = lax.all_to_all(share, ("gy", "gx"), 0, 0, tiled=True)
    chunks = 8
    return pl.pallas_call(
        final_kernel,
        out_shape=(struct(members, levels, rows, cols), struct(levels, rows, cols)),
        in_specs=[VMEM] * 5,
        out_specs=(hbm, hbm),
        scratch_shapes=[
            pltpu.VMEM((fields, rows, cols), F32),
            pltpu.VMEM((levels, rows, cols), F32),
            pltpu.SemaphoreType.DMA((chunks + 1,)),
        ],
        compiler_params=pltpu.CompilerParams(vmem_limit_bytes=16 * 2**20),
    )(share, zm_one, zm_two, x_one, x_two)


def solution(mesh):
    return jax.shard_map(
        on_device,
        mesh=mesh,
        in_specs=(
            P(None, None, "gy", "gx"),
            P("gy", "gx", None),
            P("gy", "gx", None),
            P("gy", "gx", None),
            P("gy", "gx", None),
        ),
        out_specs=(P(None, None, "gy", "gx"), P(None, "gy", "gx")),
        check_vma=False,
    )
```

```python
import functools
import math

import jax
import jax.numpy as jnp
import numpy as np
from jax import lax
from jax.experimental import pallas as pl
from jax.experimental.pallas import tpu as pltpu
from jax.sharding import PartitionSpec as P

SWEEPS = 4
KAPPA = 0.2
EPS = 1e-06
HALO = 2 * SWEEPS
WIDE = 2 * HALO
PAIR = 4 * WIDE
VMEM = pl.BlockSpec(memory_space=pltpu.VMEM)
F32 = jnp.float32
BF16 = jnp.bfloat16


def band_matrices(lanes):
    out = np.zeros((4, 2, lanes, SWEEPS * lanes), np.float32)
    lane = np.arange(lanes)
    for variant in range(4):
        for kind in range(2):
            col, part = lane, 0 * lane
            if kind == 1:
                j = lane % PAIR
                col = np.where(j < 2 * WIDE, j - WIDE, lanes - 3 * WIDE + j)
                part = lane // (2 * WIDE)
            inside = np.ones(lanes, bool)
            if variant % 2:
                inside &= col >= 0
            if variant // 2:
                inside &= col < lanes
            near = (np.abs(lane[:, None] - lane[None, :]) <= 1) & (part[:, None] == part[None, :])
            band = (near & inside[:, None] & inside[None, :]).astype(np.float64)
            power = [np.diag(inside.astype(np.float64))]
            for _ in range(SWEEPS):
                power.append(power[-1] @ band)
            for j in range(SWEEPS):
                q = sum(
                    math.comb(SWEEPS, k) * math.comb(SWEEPS - k, (SWEEPS - k - j) // 2) * power[k]
                    for k in range(SWEEPS - j + 1)
                    if (SWEEPS - k - j) % 2 == 0
                )
                out[variant, kind, :, j * lanes : (j + 1) * lanes] = q
    return out


def swap(x, axis, odd):
    count = lax.axis_size(axis)
    return lax.ppermute(x, axis, [(i + a, i + 1 - a) for i in range(odd, count - 1, 2) for a in range(2)])


def by_parity(axis, even, odd):
    me = jnp.full(even.shape, lax.axis_index(axis), jnp.int32)
    return jnp.where((me & 1) == 0, even, odd)


def turn(x, amount):
    amount %= x.shape[-1]
    return pltpu.roll(x, amount, x.ndim - 1) if amount else x


def lanes_of(x):
    return lax.broadcasted_iota(jnp.int32, x.shape, x.ndim - 1)


def scatter_kernel(ens, cell_in, level_in, innov_in, weight_in, grid, near, far, cell, level, innov, weight, first, last, sem):
    members, levels, rows, cols = ens.shape
    obs = cell.shape[-1]
    copies = [
        pltpu.make_async_copy(a, b, sem.at[i])
        for i, (a, b) in enumerate(
            (
                (cell_in, cell),
                (level_in, level),
                (innov_in, innov),
                (weight_in, weight),
                (ens.at[:, :, 0:16, :], first),
                (ens.at[:, :, rows - 16 : rows, :], last),
            )
        )
    ]
    for c in copies:
        c.start()
    for c in copies[:4]:
        c.wait()
    span = 256
    row_iota = lax.broadcasted_iota(jnp.int32, (levels * rows, span), 0)
    col_iota = lax.broadcasted_iota(jnp.int32, (cols, span), 0)
    acc = jnp.zeros((4 * levels * rows, cols), F32)
    for start in range(0, obs, span):
        at = slice(start, start + span)
        spot = cell[0, :, at]
        here = row_iota == level[0, :, at] * rows + spot // cols
        w = weight[0, :, at]
        parts = []
        for value in (w * innov[0, :, at], w):
            high = value.astype(BF16).astype(F32)
            parts += [high, value - high]
        left = jnp.concatenate([jnp.where(here, part, 0.0).astype(BF16) for part in parts], axis=0)
        right = jnp.where(col_iota == spot % cols, 1.0, 0.0).astype(BF16)
        acc += lax.dot_general(left, right, (((1,), (1,)), ((), ())), preferred_element_type=F32)
    n = levels * rows
    g = acc[:n] + acc[n : 2 * n]
    d = acc[2 * n : 3 * n] + acc[3 * n :]
    fields = members * levels
    for l in range(levels):
        grid[0, l] = g[l * rows : (l + 1) * rows]
        grid[1, l] = d[l * rows : (l + 1) * rows]
        up = g[l * rows : l * rows + HALO]
        down = g[(l + 1) * rows - HALO : (l + 1) * rows]
        near[fields + l] = by_parity("gy", down, up)
        far[fields + l] = by_parity("gy", up, down)
    for c in copies[4:]:
        c.wait()

    def edge(m, _):
        for l in range(levels):
            up = first[m, l].astype(F32)[:HALO]
            down = last[m, l].astype(F32)[16 - HALO :]
            near[l * members + m] = by_parity("gy", down, up)
            far[l * members + m] = by_parity("gy", up, down)
        return 0

    lax.fori_loop(0, members, edge, 0)


def slot_lane(t):
    return PAIR * (t % 2) + WIDE * (t // 2)


def strip(xs, at, near, far):
    lane = lanes_of(xs[0])
    west = east = jnp.zeros_like(xs[0])
    for t, x in enumerate(xs):
        base = slot_lane(t)
        here = (lane >= base) & (lane < base + WIDE)
        west = jnp.where(here, turn(x, base), west)
        east = jnp.where(here, turn(x, base + WIDE), east)
    near[at] = by_parity("gx", east, west)
    far[at] = by_parity("gx", west, east)


def arrange(u, get, mains, wins, near, far, spans):
    xs = [get(8 * u + t) for t in range(8)]
    lane = lanes_of(xs[0])

    def put(ref, f, value):
        at = 0
        for start, count in spans:
            ref[f, start : start + count, :] = value[at : at + count]
            at += count

    for t, x in enumerate(xs):
        put(mains, 8 * u + t, x)
    strip(xs, u, near, far)
    for v in range(4):
        win = jnp.zeros_like(xs[0])
        for q in range(2):
            x = xs[2 * v + q]
            at = lane - PAIR * q
            win = jnp.where((at >= WIDE) & (at < 2 * WIDE), turn(x, PAIR * q + WIDE), win)
            win = jnp.where((at >= 2 * WIDE) & (at < 3 * WIDE), turn(x, PAIR * q + 3 * WIDE), win)
        put(wins, 4 * u + v, win)


def own_kernel(ens_in, grid, bands_in, mains, wins, near, far, g_ext, mirror, bands, ens, sem):
    members, levels, rows, cols = ens.shape
    fields = members * levels
    gx = lax.axis_index("gx")
    variant = jnp.where(gx == 0, 1, 0) + jnp.where(gx == lax.axis_size("gx") - 1, 2, 0)
    copies = [pltpu.make_async_copy(ens_in, ens, sem.at[0])]
    for half in range(2):
        part = bands.at[:, half * cols : (half + 1) * cols, :]
        copies.append(pltpu.make_async_copy(bands_in.at[variant], part, sem.at[1 + half]))
    for c in copies:
        c.start()
    for c in copies:
        c.wait()
    spans = ((HALO, rows),)

    def group(u, _):
        l = 8 * u // members
        arrange(u, lambda f: ens[f - l * members, l].astype(F32), mains, wins, near, far, spans)
        return 0

    lax.fori_loop(0, fields // 8, group, 0)
    strip([grid[k, l] for k in range(2) for l in range(levels)], fields // 8, near, far)
    for l in range(levels):
        g_ext[l, HALO : HALO + rows, :] = grid[0, l]
    mirror[...] = jnp.zeros_like(mirror)
    me = lax.axis_index("gy")
    row = lax.broadcasted_iota(jnp.int32, (HALO, cols), 0)

    def flip(x, step):
        out = jnp.zeros((HALO, cols), F32)
        for j in range(1, HALO):
            if step > 0:
                out = jnp.where(row == HALO - 1 - j, x[j - 1 : j], out)
            else:
                out = jnp.where(row == j, x[HALO - j : HALO - j + 1], out)
        return out

    def side(step):
        at = 0 if step > 0 else rows - HALO
        slot = 0 if step > 0 else 1
        start = 0 if step > 0 else rows - 16
        skip = 0 if step > 0 else 16 - HALO

        def body(m, _):
            for l in range(levels):
                x = ens[m, l, start : start + 16, :].astype(F32)[skip : skip + HALO]
                mirror[slot, l * members + m] = flip(x, step)
            return 0

        lax.fori_loop(0, members, body, 0)
        for l in range(levels):
            mirror[slot, fields + l] = -flip(grid[0, l, at : at + HALO, :], step)

    pl.when(me == 0)(lambda: side(1))
    pl.when(me == lax.axis_size("gy") - 1)(lambda: side(-1))


def halo_kernel(from_near, from_far, mirror, *refs):
    mains, wins, g_ext, near, far = refs[4:]
    levels, reach, cols = g_ext.shape
    fields = mirror.shape[1] - levels
    spans = ((0, HALO), (reach - HALO, HALO))

    def get(f):
        a, b = from_near[f], from_far[f]
        return jnp.concatenate([by_parity("gy", b, a) + mirror[0, f], by_parity("gy", a, b) + mirror[1, f]], axis=0)

    def group(u, _):
        arrange(u, get, mains, wins, near, far, spans)
        return 0

    lax.fori_loop(0, fields // 8, group, 0)
    ends = [get(fields + l) for l in range(levels)]
    strip(ends, fields // 8, near, far)
    for l in range(levels):
        g_ext[l, 0:HALO, :] = ends[l][:HALO]
        g_ext[l, reach - HALO :, :] = ends[l][HALO:]


def band_products(lhs, bands, kind, out, count):
    lanes = lhs.shape[1] // 2
    for half in range(SWEEPS // 2):
        r = jnp.dot(
            lhs[0:count, :],
            bands[kind, :, half * 2 * lanes : (half + 1) * 2 * lanes],
            preferred_element_type=F32,
        )
        out[2 * half, 0:count, :] = r[:, :lanes]
        out[2 * half + 1, 0:count, :] = r[:, lanes:]


def split_into(lhs, start, x):
    count, lanes = x.shape
    high = x.astype(BF16)
    lhs[start : start + count, 0:lanes] = high
    lhs[start : start + count, lanes : 2 * lanes] = (x - high.astype(F32)).astype(BF16)


def combine(part, src, count):
    total = src(2 * SWEEPS) + src(0)
    for k in range(1, SWEEPS):
        total += part(k, SWEEPS + k) + part(k, SWEEPS - k)
    return total + part(0, SWEEPS)


def rows_of(prod, start, count):
    return lambda k, off: prod[k, pl.ds(start + off, count), :]


def field_rows(ref, f, count, base=0):
    return lambda off: ref[f, pl.ds(base + off, count), :]


def interior(pack, g, bands, z, first_edge, second_edge, xacc, fbuf, prod, lhs, batch, also):
    count, reach, _ = pack.shape
    rows = reach - 2 * HALO
    mid, core = rows - HALO, rows - 2 * HALO
    per_level = count // g.shape[0]
    xacc[...] = jnp.zeros_like(xacc)

    def keep(edge, at, start, size):
        for k in range(SWEEPS):
            edge[k, at, HALO : 2 * HALO, :] = prod[k, start : start + HALO, :]
            edge[k, count + at, 0:HALO, :] = prod[k, start + size - HALO : start + size, :]

    def step(b, _):
        level = b * batch // per_level
        for i in range(batch):
            f = pack[b * batch + i, HALO : HALO + rows, :] * g[level]
            fbuf[i, 0:rows, :] = f
            split_into(lhs, i * rows, f)
        band_products(lhs, bands, 0, prod, batch * rows)
        for i in range(batch):
            at = b * batch + i
            v = combine(rows_of(prod, i * rows, mid), field_rows(fbuf, i, mid), mid)
            z[at, HALO : HALO + mid, :] = v
            keep(first_edge, at, i * rows, rows)
            split_into(lhs, i * mid, v)
            if also is not None:
                also(b, i)
        band_products(lhs, bands, 0, prod, batch * mid)
        for i in range(batch):
            at = b * batch + i
            v = combine(rows_of(prod, i * mid, core), field_rows(z, at, core, HALO), core)
            keep(second_edge, at, i * mid, mid)
            xacc[level, HALO : HALO + core, :] += v * pack[at, 2 * HALO : 2 * HALO + core, :]
        return 0

    lax.fori_loop(0, count // batch, step, 0)


def edge_rows(pack, g, bands, z, first_edge, second_edge, xacc, ends, lhs):
    count, reach, lanes = pack.shape
    rows = reach - 2 * HALO
    per_level = count // g.shape[0]
    sides = [(side, f) for side in range(2) for f in range(count)]

    def products(edge):
        for half in range(SWEEPS // 2):
            r = jnp.dot(
                lhs[0 : 2 * count * HALO, :],
                bands[0, :, half * 2 * lanes : (half + 1) * 2 * lanes],
                preferred_element_type=F32,
            )
            for t in range(2):
                part = r[:, t * lanes : (t + 1) * lanes].reshape(2 * count, HALO, lanes)
                edge[2 * half + t, 0:count, 0:HALO, :] = part[:count]
                edge[2 * half + t, count:, HALO : 2 * HALO, :] = part[count:]

    def near(edge, j):
        return lambda k, off: edge[k, j, pl.ds(off, HALO), :]

    for side, f in sides:
        base = side * rows
        x = pack[f, base : base + 2 * HALO, :] * g[f // per_level, base : base + 2 * HALO, :]
        j = side * count + f
        ends[j] = x
        split_into(lhs, j * HALO, x[side * HALO : (side + 1) * HALO])
    products(first_edge)
    for side, f in sides:
        j = side * count + f
        v = combine(near(first_edge, j), field_rows(ends, j, HALO), HALO)
        z[f, side * rows : side * rows + HALO, :] = v
        split_into(lhs, j * HALO, v)
    products(second_edge)
    for side in range(2):
        for level in range(g.shape[0]):
            total = jnp.zeros((HALO, lanes), F32)
            for f in range(level * per_level, (level + 1) * per_level):
                base = side * (rows - HALO)
                v = combine(near(second_edge, side * count + f), field_rows(z, f, HALO, base), HALO)
                total += v * pack[f, HALO + base : 2 * HALO + base, :]
            xacc[level, base : base + HALO, :] = total


def level_at(b, i, batch, per_level):
    return b * batch // per_level if batch <= per_level else i // per_level


def covariance(pack, bands, kind, g, z, xacc, fbuf, prod, lhs, batch, build=None, also=None):
    count, reach, _ = pack.shape
    inner, rows = reach - HALO, reach - 2 * HALO
    per_level = count // g.shape[0]
    xacc[...] = jnp.zeros_like(xacc)

    def step(b, _):
        for i in range(batch):
            at = b * batch + i
            level = level_at(b, i, batch, per_level)
            if build is not None:
                pack[at] = build(b, i, pack[at])
            f = pack[at] * g[level]
            fbuf[i] = f
            split_into(lhs, i * reach, f)
        band_products(lhs, bands, kind, prod, batch * reach)
        for i in range(batch):
            v = combine(rows_of(prod, i * reach, inner), field_rows(fbuf, i, inner), inner)
            z[b * batch + i] = v
            split_into(lhs, i * inner, v)
            if also is not None:
                also(b, i, v)
        band_products(lhs, bands, kind, prod, batch * inner)
        for i in range(batch):
            level = level_at(b, i, batch, per_level)
            v = combine(rows_of(prod, i * inner, rows), field_rows(z, b * batch + i, rows), rows)
            xacc[level] += v * pack[b * batch + i, HALO : HALO + rows, :]
        return 0

    lax.fori_loop(0, count // batch, step, 0)


def window_grid(g, west, east):
    lane = lanes_of(g)
    win = jnp.where(lane < WIDE, west, turn(g, WIDE))
    win = jnp.where(lane < 2 * WIDE, win, turn(g, 3 * WIDE))
    win = jnp.where(lane < 3 * WIDE, win, turn(east, 3 * WIDE))
    win = jnp.where(lane < PAIR, win, 0.0)
    return (win + turn(win, PAIR)) * KAPPA**SWEEPS


def fold(x):
    return jnp.sum(x.reshape(x.shape[0] // 8, 8, x.shape[1]), axis=0)


def interior_kernel(pack, g, bands, z, first_edge, second_edge, xacc, gbuf, fbuf, prod, lhs, *, batch):
    gbuf[...] = g[0] * KAPPA**SWEEPS
    interior(pack, gbuf, bands, z, first_edge, second_edge, xacc, fbuf, prod, lhs, batch, None)


def edge_kernel(pack, g_ext, bands, *refs):
    z, first_edge, second_edge, xacc, gbuf, ends, lhs = refs[4:]
    gbuf[...] = g_ext[...] * KAPPA**SWEEPS
    edge_rows(pack, gbuf, bands, z, first_edge, second_edge, xacc, ends, lhs)


def put_edges(old, win, q):
    lane = lanes_of(old)
    cols = old.shape[1]
    new = jnp.where(lane < HALO, turn(win, -WIDE - PAIR * q), old)
    return jnp.where(lane < cols - HALO, new, turn(win, cols - 3 * WIDE - PAIR * q))


def second_interior_kernel(
    pack, p, bands, z_one, zw_one,
    z, first_edge, second_edge, xacc, z_out,
    gbuf, fbuf, prod, lhs, *, batch,
):
    del z_one
    gbuf[...] = p[...] * KAPPA**SWEEPS

    def first_edges(b, i):
        at = b * batch + i
        z_out[at] = put_edges(z_out[at], zw_one[b * (batch // 2) + i // 2], i % 2)

    interior(pack, gbuf, bands, z, first_edge, second_edge, xacc, fbuf, prod, lhs, batch, first_edges)


def join(main, win, cols):
    win = (win + turn(win, PAIR)) * KAPPA**SWEEPS
    lane = lanes_of(win)
    state = jnp.where(lane < HALO, turn(win, -WIDE), main * KAPPA**SWEEPS)
    return jnp.where(lane < cols - HALO, state, turn(win, cols - 3 * WIDE)), win


def first_kernel(
    pack_in, g_ext, grid, near, far, near_ends, far_ends, bands, xmain,
    pack, z, x, p, near_out, far_out, side, sums,
    gbuf, fbuf, prod, lhs, xacc, west, east, *, batch,
):
    del pack_in
    levels, reach, cols = g_ext.shape
    rows = reach - 2 * HALO
    last = west.shape[0] - 1
    west[:, HALO : HALO + rows, :] = by_parity("gx", far[...], near[...])
    east[:, HALO : HALO + rows, :] = by_parity("gx", near[...], far[...])
    for start, at in ((0, 0), (HALO + rows, HALO)):
        a, b = near_ends[:, at : at + HALO, :], far_ends[:, at : at + HALO, :]
        west[:, start : start + HALO, :] = by_parity("gx", b, a)
        east[:, start : start + HALO, :] = by_parity("gx", a, b)
    for l in range(levels):
        gbuf[l] = window_grid(g_ext[l], turn(west[last], -slot_lane(l)), turn(east[last], -slot_lane(l)))
    lane = lax.broadcasted_iota(jnp.int32, (reach, cols), 1)

    def window(b, i, old):
        u = b * (batch // 4) + i // 4
        at = lane & (PAIR - 1)
        old = jnp.where(at < WIDE, turn(west[u], -WIDE * (i % 4)), old)
        return jnp.where(at >= 3 * WIDE, turn(east[u], 3 * WIDE - WIDE * (i % 4)), old)

    covariance(pack, bands, 1, gbuf, z, xacc, fbuf, prod, lhs, batch, window)
    norm = jnp.zeros((8, cols), F32)
    curve = norm
    lane = lane[:rows]
    d_west, d_east = west[last, HALO : HALO + rows, :], east[last, HALO : HALO + rows, :]
    sides = jnp.zeros((rows, cols), F32)
    for l in range(levels):
        state, win = join(xmain[l], xacc[l], cols)
        push = grid[1, l] * state
        x[l] = state
        p[l] = push
        near_out[l] = by_parity("gy", push[rows - HALO :], push[:HALO])
        far_out[l] = by_parity("gy", push[:HALO], push[rows - HALO :])
        norm += fold(grid[0, l] * state)
        curve += fold(push * state)
        base = WIDE * l
        mine = slot_lane(levels + l)
        beside = turn(win, base - HALO) * turn(d_west, base - mine - HALO)
        sides = jnp.where((lane >= base) & (lane < base + HALO), beside, sides)
        beside = turn(win, base + HALO - 3 * WIDE) * turn(d_east, base + HALO - mine)
        sides = jnp.where((lane >= base + HALO) & (lane < base + WIDE), beside, sides)
    side[...] = sides
    near_out[levels] = by_parity("gy", sides[rows - HALO :], sides[:HALO])
    far_out[levels] = by_parity("gy", sides[:HALO], sides[rows - HALO :])
    sums[0] = norm
    sums[1] = curve


def second_kernel(
    mains, wins, p, side, near, far, grid, bands, sums, z_in, first_in, second_in, xmain_in,
    x, share, zm, first_edge, second_edge, xmain,
    ext, gbuf, fbuf, prod, lhs, xacc, zw, ends, *, batch,
):
    del z_in, first_in, second_in, xmain_in
    levels, rows, cols = p.shape
    reach = rows + 2 * HALO
    for l in range(levels + 1):
        ext[l, HALO : HALO + rows, :] = p[l] if l < levels else side[...]
        ext[l, 0:HALO, :] = by_parity("gy", far[l], near[l])
        ext[l, HALO + rows :, :] = by_parity("gy", near[l], far[l])
    me = lax.axis_index("gy")

    def reflect(base, step):
        for l in range(levels + 1):
            for j in range(1, HALO):
                ext[l, base - step * j : base - step * j + 1, :] = -ext[l, base + step * j : base + step * j + 1, :]

    pl.when(me == 0)(lambda: reflect(HALO - 1, 1))
    pl.when(me == lax.axis_size("gy") - 1)(lambda: reflect(HALO + rows, -1))
    lane = lax.broadcasted_iota(jnp.int32, (reach, cols), 1)
    for l in range(levels):
        gbuf[0, l] = ext[l] * KAPPA**SWEEPS
        west = jnp.where(lane < HALO, 0.0, turn(ext[levels], HALO - WIDE * l))
        east = jnp.where(lane < HALO, turn(ext[levels], -HALO - WIDE * l), 0.0)
        gbuf[1, l] = window_grid(ext[l], west, east)

    def second_edges(b, i, v):
        for q in range(2):
            at = 2 * (b * batch + i) + q
            zm[at] = put_edges(zm[at], v, q)

    edge_rows(mains, gbuf.at[0], bands, zm, first_edge, second_edge, xmain, ends, lhs)
    covariance(wins, bands, 1, gbuf.at[1], zw, xacc, fbuf, prod, lhs, batch, None, second_edges)
    cross = jnp.zeros((8, cols), F32)
    curve = cross
    for l in range(levels):
        state, _ = join(xmain[l], xacc[l], cols)
        x[l] = state
        cross += fold(p[l] * state)
        curve += fold(grid[1, l] * state * state)
    out = jnp.zeros((1, cols), F32)
    place = lax.broadcasted_iota(jnp.int32, (1, cols), 1)
    for i, part in enumerate((sums[0], sums[1], cross, curve)):
        out = jnp.where(place == i, jnp.sum(jnp.sum(part, axis=0, keepdims=True), axis=1, keepdims=True), out)
    share[...] = jnp.broadcast_to(out, share.shape)


def final_kernel(share, z_one, z_two, x_one, x_two, control, increment, stage, x_stage, sems):
    members, levels, rows, cols = control.shape
    total = jnp.sum(share[...], axis=0, keepdims=True)
    place = lax.broadcasted_iota(jnp.int32, (1, cols), 1)
    n0, c1, c2, c3 = (jnp.sum(jnp.where(place == i, total, 0.0), axis=1, keepdims=True) for i in range(4))
    bn2 = n0 + EPS
    alpha_one = (n0 + c1) / bn2
    t = (EPS - c1) / bn2
    rr = jnp.maximum((c2 + 2.0 * t * c1 + t * t * n0) / bn2, 0.0)
    beta_sq = rr + EPS
    alpha_two = (rr + jnp.maximum((c3 + 2.0 * t * c2 + t * t * c1) / bn2, 0.0)) / beta_sq
    det = alpha_one * alpha_two - beta_sq
    coef_b = -1.0 / det
    coef_a = (alpha_two - t) / det
    copies = []
    part = stage.shape[0] // (sems.shape[0] - 1)
    for c in range(sems.shape[0] - 1):

        def body(i, _):
            f = c * part + i
            one, two = z_one[f, SWEEPS : SWEEPS + rows, :], z_two[f, SWEEPS : SWEEPS + rows, :]
            stage[f] = coef_a * one + coef_b * two
            return 0

        lax.fori_loop(0, part, body, 0, unroll=4)
        level, first = divmod(c * part, members)
        copies.append(
            pltpu.make_async_copy(
                stage.at[pl.ds(c * part, part)], control.at[pl.ds(first, part), level], sems.at[c]
            )
        )
        copies[-1].start()
    x_stage[...] = coef_a * x_one[...] + coef_b * x_two[...]
    copies.append(pltpu.make_async_copy(x_stage, increment, sems.at[sems.shape[0] - 1]))
    copies[-1].start()
    for copy in copies:
        copy.wait()


def on_device(ensemble, obs_cell, obs_level, innovation, obs_weight):
    members, levels, rows, cols = ensemble.shape
    fields = members * levels
    reach = rows + 2 * HALO
    batch = 32
    strips = fields // 8 + 1
    devices = lax.axis_size("gy") * lax.axis_size("gx")
    hbm = pl.BlockSpec(memory_space=pltpu.HBM)

    def struct(*shape):
        return jax.ShapeDtypeStruct(shape, F32)

    def call(kernel, outs, ins, scratch=(), limit=24, work=2, **kw):
        return pl.pallas_call(
            kernel,
            out_shape=outs,
            in_specs=[VMEM] * ins if isinstance(ins, int) else ins,
            out_specs=jax.tree.map(lambda _: VMEM, outs),
            scratch_shapes=scratch,
            compiler_params=pltpu.CompilerParams(vmem_limit_bytes=limit * 2**20),
            cost_estimate=pl.CostEstimate(flops=work * 10**9, bytes_accessed=10**6, transcendentals=0),
            **kw,
        )

    bands = jnp.asarray(band_matrices(cols), BF16)
    obs = obs_cell.shape
    edge = pltpu.VMEM((members, levels, 16, cols), BF16)
    grid, near, far = call(
        scatter_kernel,
        (struct(2, levels, rows, cols), struct(fields + levels, HALO, cols), struct(fields + levels, HALO, cols)),
        [hbm] * 5,
        [pltpu.VMEM(obs, jnp.int32)] * 2 + [pltpu.VMEM(obs, F32)] * 2 + [edge, edge, pltpu.SemaphoreType.DMA((6,))],
        limit=60,
    )(ensemble, obs_cell, obs_level, innovation, obs_weight)
    near, far = swap(near, "gy", 0), swap(far, "gy", 1)
    main_shape, win_shape = struct(fields, reach, cols), struct(fields // 2, reach, cols)
    g_shape = struct(levels, reach, cols)
    own_shape, end_shape = struct(strips, rows, cols), struct(strips, 2 * HALO, cols)
    mains, wins, near_own, far_own, g_ext, mirror, bands = call(
        own_kernel,
        (
            main_shape,
            win_shape,
            own_shape,
            own_shape,
            g_shape,
            struct(2, fields + levels, HALO, cols),
            jax.ShapeDtypeStruct((2, 2 * cols, SWEEPS * cols), BF16),
        ),
        [hbm, VMEM, hbm],
        [pltpu.VMEM(ensemble.shape, BF16), pltpu.SemaphoreType.DMA((3,))],
    )(ensemble, grid, bands)
    near_own, far_own = swap(near_own, "gx", 0), swap(far_own, "gx", 1)
    work = (
        pltpu.VMEM((batch, reach, cols), F32),
        pltpu.VMEM((SWEEPS, batch * reach, cols), F32),
        pltpu.VMEM((batch * reach, 2 * cols), BF16),
    )
    zm_shape, zw_shape = struct(fields, reach - HALO, cols), struct(fields // 2, reach - HALO, cols)
    state_shape = struct(levels, rows, cols)
    edge_shape = struct(SWEEPS, 2 * fields, 2 * HALO, cols)
    part_shapes = (zm_shape, edge_shape, edge_shape, state_shape)
    ends = pltpu.VMEM((2 * fields, 2 * HALO, cols), F32)
    part = call(
        functools.partial(interior_kernel, batch=batch),
        part_shapes,
        3,
        (pltpu.VMEM((levels, rows, cols), F32), *work),
    )(mains, grid, bands)
    mains, wins, g_ext, near, far = call(
        halo_kernel, (main_shape, win_shape, g_shape, end_shape, end_shape), 7, input_output_aliases={3: 0, 4: 1, 5: 2}
    )(near, far, mirror, mains, wins, g_ext, part[3])
    near, far = swap(near, "gx", 0), swap(far, "gx", 1)
    gbuf = pltpu.VMEM((levels, reach, cols), F32)
    zm_one, _, _, xmain = call(
        edge_kernel, part_shapes, 7, (gbuf, ends, work[2]), input_output_aliases={3: 0, 4: 1, 5: 2, 6: 3}
    )(mains, g_ext, bands, *part)
    wins, zw_one, x_one, p, near, far, side, sums = call(
        functools.partial(first_kernel, batch=batch),
        (
            win_shape,
            zw_shape,
            struct(levels, rows, cols),
            struct(levels, rows, cols),
            struct(levels + 1, HALO, cols),
            struct(levels + 1, HALO, cols),
            struct(rows, cols),
            struct(2, 8, cols),
        ),
        9,
        (gbuf, *work, pltpu.VMEM((levels, rows, cols), F32), *[pltpu.VMEM((strips, reach, cols), F32)] * 2),
        input_output_aliases={0: 0},
    )(wins, g_ext, grid, near_own, far_own, near, far, bands, xmain)
    near, far = swap(near, "gy", 0), swap(far, "gy", 1)
    *part, zm_one = call(
        functools.partial(second_interior_kernel, batch=batch),
        (*part_shapes, zm_shape),
        5,
        (pltpu.VMEM((levels, rows, cols), F32), *work),
        input_output_aliases={3: 4},
    )(mains, p, bands, zm_one, zw_one)
    x_two, share, zm_two, _, _, _ = call(
        functools.partial(second_kernel, batch=batch),
        (state_shape, struct(devices, cols), *part_shapes),
        13,
        (
            pltpu.VMEM((levels + 1, reach, cols), F32),
            pltpu.VMEM((2, levels, reach, cols), F32),
            *work,
            pltpu.VMEM((levels, rows, cols), F32),
            pltpu.VMEM((fields // 2, reach - HALO, cols), F32),
            ends,
        ),
        input_output_aliases={9: 2, 10: 3, 11: 4, 12: 5},
    )(mains, wins, p, side, near, far, grid, bands, sums, *part)
    share = lax.all_to_all(share, ("gy", "gx"), 0, 0, tiled=True)
    chunks = 8
    return pl.pallas_call(
        final_kernel,
        out_shape=(struct(members, levels, rows, cols), struct(levels, rows, cols)),
        in_specs=[VMEM] * 5,
        out_specs=(hbm, hbm),
        scratch_shapes=[
            pltpu.VMEM((fields, rows, cols), F32),
            pltpu.VMEM((levels, rows, cols), F32),
            pltpu.SemaphoreType.DMA((chunks + 1,)),
        ],
        compiler_params=pltpu.CompilerParams(vmem_limit_bytes=16 * 2**20),
    )(share, zm_one, zm_two, x_one, x_two)


def solution(mesh):
    return jax.shard_map(
        on_device,
        mesh=mesh,
        in_specs=(
            P(None, None, "gy", "gx"),
            P("gy", "gx", None),
            P("gy", "gx", None),
            P("gy", "gx", None),
            P("gy", "gx", None),
        ),
        out_specs=(P(None, None, "gy", "gx"), P(None, "gy", "gx")),
        check_vma=False,
    )
```

```python
import functools
import math

import jax
import jax.numpy as jnp
import numpy as np
from jax import lax
from jax.experimental import pallas as pl
from jax.experimental.pallas import tpu as pltpu
from jax.sharding import PartitionSpec as P

SWEEPS = 4
KAPPA = 0.2
EPS = 1e-06
HALO = 2 * SWEEPS
WIDE = 2 * HALO
PAIR = 4 * WIDE
VMEM = pl.BlockSpec(memory_space=pltpu.VMEM)
F32 = jnp.float32
BF16 = jnp.bfloat16


def band_matrices(lanes):
    out = np.zeros((4, 2, lanes, SWEEPS * lanes), np.float32)
    lane = np.arange(lanes)
    for variant in range(4):
        for kind in range(2):
            col, part = lane, 0 * lane
            if kind == 1:
                j = lane % PAIR
                col = np.where(j < 2 * WIDE, j - WIDE, lanes - 3 * WIDE + j)
                part = lane // (2 * WIDE)
            inside = np.ones(lanes, bool)
            if variant % 2:
                inside &= col >= 0
            if variant // 2:
                inside &= col < lanes
            near = (np.abs(lane[:, None] - lane[None, :]) <= 1) & (part[:, None] == part[None, :])
            band = (near & inside[:, None] & inside[None, :]).astype(np.float64)
            power = [np.diag(inside.astype(np.float64))]
            for _ in range(SWEEPS):
                power.append(power[-1] @ band)
            for j in range(SWEEPS):
                q = sum(
                    math.comb(SWEEPS, k) * math.comb(SWEEPS - k, (SWEEPS - k - j) // 2) * power[k]
                    for k in range(SWEEPS - j + 1)
                    if (SWEEPS - k - j) % 2 == 0
                )
                out[variant, kind, :, j * lanes : (j + 1) * lanes] = q
    return out


def swap(x, axis, odd):
    count = lax.axis_size(axis)
    return lax.ppermute(x, axis, [(i + a, i + 1 - a) for i in range(odd, count - 1, 2) for a in range(2)])


def by_parity(axis, even, odd):
    me = jnp.full(even.shape, lax.axis_index(axis), jnp.int32)
    return jnp.where((me & 1) == 0, even, odd)


def turn(x, amount):
    amount %= x.shape[-1]
    return pltpu.roll(x, amount, x.ndim - 1) if amount else x


def lanes_of(x):
    return lax.broadcasted_iota(jnp.int32, x.shape, x.ndim - 1)


def scatter_kernel(ens, cell_in, level_in, innov_in, weight_in, grid, near, far, cell, level, innov, weight, first, last, sem):
    members, levels, rows, cols = ens.shape
    obs = cell.shape[-1]
    copies = [
        pltpu.make_async_copy(a, b, sem.at[i])
        for i, (a, b) in enumerate(
            (
                (cell_in, cell),
                (level_in, level),
                (innov_in, innov),
                (weight_in, weight),
                (ens.at[:, :, 0:16, :], first),
                (ens.at[:, :, rows - 16 : rows, :], last),
            )
        )
    ]
    for c in copies:
        c.start()
    for c in copies[:4]:
        c.wait()
    span = 256
    row_iota = lax.broadcasted_iota(jnp.int32, (levels * rows, span), 0)
    col_iota = lax.broadcasted_iota(jnp.int32, (cols, span), 0)
    acc = jnp.zeros((4 * levels * rows, cols), F32)
    for start in range(0, obs, span):
        at = slice(start, start + span)
        spot = cell[0, :, at]
        here = row_iota == level[0, :, at] * rows + spot // cols
        w = weight[0, :, at]
        parts = []
        for value in (w * innov[0, :, at], w):
            high = value.astype(BF16).astype(F32)
            parts += [high, value - high]
        left = jnp.concatenate([jnp.where(here, part, 0.0).astype(BF16) for part in parts], axis=0)
        right = jnp.where(col_iota == spot % cols, 1.0, 0.0).astype(BF16)
        acc += lax.dot_general(left, right, (((1,), (1,)), ((), ())), preferred_element_type=F32)
    n = levels * rows
    g = acc[:n] + acc[n : 2 * n]
    d = acc[2 * n : 3 * n] + acc[3 * n :]
    fields = members * levels
    for l in range(levels):
        grid[0, l] = g[l * rows : (l + 1) * rows]
        grid[1, l] = d[l * rows : (l + 1) * rows]
        up = g[l * rows : l * rows + HALO]
        down = g[(l + 1) * rows - HALO : (l + 1) * rows]
        near[fields + l] = by_parity("gy", down, up)
        far[fields + l] = by_parity("gy", up, down)
    for c in copies[4:]:
        c.wait()

    def edge(m, _):
        for l in range(levels):
            up = first[m, l].astype(F32)[:HALO]
            down = last[m, l].astype(F32)[16 - HALO :]
            near[l * members + m] = by_parity("gy", down, up)
            far[l * members + m] = by_parity("gy", up, down)
        return 0

    lax.fori_loop(0, members, edge, 0)


def slot_lane(t):
    return PAIR * (t % 2) + WIDE * (t // 2)


def strip(xs, at, near, far):
    lane = lanes_of(xs[0])
    west = east = jnp.zeros_like(xs[0])
    for t, x in enumerate(xs):
        base = slot_lane(t)
        here = (lane >= base) & (lane < base + WIDE)
        west = jnp.where(here, turn(x, base), west)
        east = jnp.where(here, turn(x, base + WIDE), east)
    near[at] = by_parity("gx", east, west)
    far[at] = by_parity("gx", west, east)


def arrange(u, get, mains, wins, near, far, spans):
    xs = [get(8 * u + t) for t in range(8)]
    lane = lanes_of(xs[0])

    def put(ref, f, value):
        at = 0
        for start, count in spans:
            ref[f, start : start + count, :] = value[at : at + count]
            at += count

    for t, x in enumerate(xs):
        put(mains, 8 * u + t, x)
    strip(xs, u, near, far)
    for v in range(4):
        win = jnp.zeros_like(xs[0])
        for q in range(2):
            x = xs[2 * v + q]
            at = lane - PAIR * q
            win = jnp.where((at >= WIDE) & (at < 2 * WIDE), turn(x, PAIR * q + WIDE), win)
            win = jnp.where((at >= 2 * WIDE) & (at < 3 * WIDE), turn(x, PAIR * q + 3 * WIDE), win)
        put(wins, 4 * u + v, win)


def own_kernel(ens_in, grid, bands_in, mains, wins, near, far, g_ext, mirror, bands, ens, sem):
    members, levels, rows, cols = ens.shape
    fields = members * levels
    gx = lax.axis_index("gx")
    variant = jnp.where(gx == 0, 1, 0) + jnp.where(gx == lax.axis_size("gx") - 1, 2, 0)
    copies = [pltpu.make_async_copy(ens_in, ens, sem.at[0])]
    for half in range(2):
        part = bands.at[:, half * cols : (half + 1) * cols, :]
        copies.append(pltpu.make_async_copy(bands_in.at[variant], part, sem.at[1 + half]))
    for c in copies:
        c.start()
    for c in copies:
        c.wait()
    spans = ((HALO, rows),)

    def group(u, _):
        l = 8 * u // members
        arrange(u, lambda f: ens[f - l * members, l].astype(F32), mains, wins, near, far, spans)
        return 0

    lax.fori_loop(0, fields // 8, group, 0)
    strip([grid[k, l] for k in range(2) for l in range(levels)], fields // 8, near, far)
    for l in range(levels):
        g_ext[l, HALO : HALO + rows, :] = grid[0, l]
    mirror[...] = jnp.zeros_like(mirror)
    me = lax.axis_index("gy")
    row = lax.broadcasted_iota(jnp.int32, (HALO, cols), 0)

    def flip(x, step):
        out = jnp.zeros((HALO, cols), F32)
        for j in range(1, HALO):
            if step > 0:
                out = jnp.where(row == HALO - 1 - j, x[j - 1 : j], out)
            else:
                out = jnp.where(row == j, x[HALO - j : HALO - j + 1], out)
        return out

    def side(step):
        at = 0 if step > 0 else rows - HALO
        slot = 0 if step > 0 else 1
        start = 0 if step > 0 else rows - 16
        skip = 0 if step > 0 else 16 - HALO

        def body(m, _):
            for l in range(levels):
                x = ens[m, l, start : start + 16, :].astype(F32)[skip : skip + HALO]
                mirror[slot, l * members + m] = flip(x, step)
            return 0

        lax.fori_loop(0, members, body, 0)
        for l in range(levels):
            mirror[slot, fields + l] = -flip(grid[0, l, at : at + HALO, :], step)

    pl.when(me == 0)(lambda: side(1))
    pl.when(me == lax.axis_size("gy") - 1)(lambda: side(-1))


def halo_kernel(from_near, from_far, mirror, *refs):
    mains, wins, g_ext, near, far = refs[4:]
    levels, reach, cols = g_ext.shape
    fields = mirror.shape[1] - levels
    spans = ((0, HALO), (reach - HALO, HALO))

    def get(f):
        a, b = from_near[f], from_far[f]
        return jnp.concatenate([by_parity("gy", b, a) + mirror[0, f], by_parity("gy", a, b) + mirror[1, f]], axis=0)

    def group(u, _):
        arrange(u, get, mains, wins, near, far, spans)
        return 0

    lax.fori_loop(0, fields // 8, group, 0)
    ends = [get(fields + l) for l in range(levels)]
    strip(ends, fields // 8, near, far)
    for l in range(levels):
        g_ext[l, 0:HALO, :] = ends[l][:HALO]
        g_ext[l, reach - HALO :, :] = ends[l][HALO:]


def band_products(lhs, bands, kind, out, count):
    lanes = lhs.shape[1] // 2
    for half in range(SWEEPS // 2):
        r = jnp.dot(
            lhs[0:count, :],
            bands[kind, :, half * 2 * lanes : (half + 1) * 2 * lanes],
            preferred_element_type=F32,
        )
        out[2 * half, 0:count, :] = r[:, :lanes]
        out[2 * half + 1, 0:count, :] = r[:, lanes:]


def split_into(lhs, start, x):
    count, lanes = x.shape
    high = x.astype(BF16)
    lhs[start : start + count, 0:lanes] = high
    lhs[start : start + count, lanes : 2 * lanes] = (x - high.astype(F32)).astype(BF16)


def combine(part, src, count):
    total = src(2 * SWEEPS) + src(0)
    for k in range(1, SWEEPS):
        total += part(k, SWEEPS + k) + part(k, SWEEPS - k)
    return total + part(0, SWEEPS)


def rows_of(prod, start, count):
    return lambda k, off: prod[k, pl.ds(start + off, count), :]


def field_rows(ref, f, count, base=0):
    return lambda off: ref[f, pl.ds(base + off, count), :]


def interior(pack, g, bands, kind, z, first_edge, second_edge, xacc, fbuf, prod, lhs, batch, also=None, build=None):
    count, reach, _ = pack.shape
    rows = reach - 2 * HALO
    mid, core = rows - HALO, rows - 2 * HALO
    per_level = count // g.shape[0]
    xacc[...] = jnp.zeros_like(xacc)

    def keep(edge, at, start, size):
        for k in range(SWEEPS):
            edge[k, at, HALO : 2 * HALO, :] = prod[k, start : start + HALO, :]
            edge[k, count + at, 0:HALO, :] = prod[k, start + size - HALO : start + size, :]

    def step(b, _):
        for i in range(batch):
            if build is not None:
                pack[b * batch + i, HALO : HALO + rows, :] = build(b, i, pack[b * batch + i, HALO : HALO + rows, :])
            f = pack[b * batch + i, HALO : HALO + rows, :] * g[level_at(b, i, batch, per_level)]
            fbuf[i, 0:rows, :] = f
            split_into(lhs, i * rows, f)
        band_products(lhs, bands, kind, prod, batch * rows)
        for i in range(batch):
            at = b * batch + i
            v = combine(rows_of(prod, i * rows, mid), field_rows(fbuf, i, mid), mid)
            z[at, HALO : HALO + mid, :] = v
            keep(first_edge, at, i * rows, rows)
            split_into(lhs, i * mid, v)
            if also is not None:
                also(b, i)
        band_products(lhs, bands, kind, prod, batch * mid)
        for i in range(batch):
            at = b * batch + i
            v = combine(rows_of(prod, i * mid, core), field_rows(z, at, core, HALO), core)
            keep(second_edge, at, i * mid, mid)
            level = level_at(b, i, batch, per_level)
            xacc[level, HALO : HALO + core, :] += v * pack[at, 2 * HALO : 2 * HALO + core, :]
        return 0

    lax.fori_loop(0, count // batch, step, 0)


def edge_rows(pack, g, bands, kind, z, first_edge, second_edge, xacc, ends, lhs):
    count, reach, lanes = pack.shape
    rows = reach - 2 * HALO
    per_level = count // g.shape[0]
    sides = [(side, f) for side in range(2) for f in range(count)]

    def products(edge):
        for half in range(SWEEPS // 2):
            r = jnp.dot(
                lhs[0 : 2 * count * HALO, :],
                bands[kind, :, half * 2 * lanes : (half + 1) * 2 * lanes],
                preferred_element_type=F32,
            )
            for t in range(2):
                part = r[:, t * lanes : (t + 1) * lanes].reshape(2 * count, HALO, lanes)
                edge[2 * half + t, 0:count, 0:HALO, :] = part[:count]
                edge[2 * half + t, count:, HALO : 2 * HALO, :] = part[count:]

    def near(edge, j):
        return lambda k, off: edge[k, j, pl.ds(off, HALO), :]

    for side, f in sides:
        base = side * rows
        x = pack[f, base : base + 2 * HALO, :] * g[f // per_level, base : base + 2 * HALO, :]
        j = side * count + f
        ends[j] = x
        split_into(lhs, j * HALO, x[side * HALO : (side + 1) * HALO])
    products(first_edge)
    for side, f in sides:
        j = side * count + f
        v = combine(near(first_edge, j), field_rows(ends, j, HALO), HALO)
        z[f, side * rows : side * rows + HALO, :] = v
        split_into(lhs, j * HALO, v)
    products(second_edge)
    for side in range(2):
        for level in range(g.shape[0]):
            total = jnp.zeros((HALO, lanes), F32)
            for f in range(level * per_level, (level + 1) * per_level):
                base = side * (rows - HALO)
                v = combine(near(second_edge, side * count + f), field_rows(z, f, HALO, base), HALO)
                total += v * pack[f, HALO + base : 2 * HALO + base, :]
            xacc[level, base : base + HALO, :] = total


def level_at(b, i, batch, per_level):
    return b * batch // per_level if batch <= per_level else i // per_level


def covariance(pack, bands, kind, g, z, xacc, fbuf, prod, lhs, batch, build=None, also=None):
    count, reach, _ = pack.shape
    inner, rows = reach - HALO, reach - 2 * HALO
    per_level = count // g.shape[0]
    xacc[...] = jnp.zeros_like(xacc)

    def step(b, _):
        for i in range(batch):
            at = b * batch + i
            level = level_at(b, i, batch, per_level)
            if build is not None:
                pack[at] = build(b, i, pack[at])
            f = pack[at] * g[level]
            fbuf[i] = f
            split_into(lhs, i * reach, f)
        band_products(lhs, bands, kind, prod, batch * reach)
        for i in range(batch):
            v = combine(rows_of(prod, i * reach, inner), field_rows(fbuf, i, inner), inner)
            z[b * batch + i] = v
            split_into(lhs, i * inner, v)
            if also is not None:
                also(b, i, v)
        band_products(lhs, bands, kind, prod, batch * inner)
        for i in range(batch):
            level = level_at(b, i, batch, per_level)
            v = combine(rows_of(prod, i * inner, rows), field_rows(z, b * batch + i, rows), rows)
            xacc[level] += v * pack[b * batch + i, HALO : HALO + rows, :]
        return 0

    lax.fori_loop(0, count // batch, step, 0)


def window_grid(g, west, east):
    lane = lanes_of(g)
    win = jnp.where(lane < WIDE, west, turn(g, WIDE))
    win = jnp.where(lane < 2 * WIDE, win, turn(g, 3 * WIDE))
    win = jnp.where(lane < 3 * WIDE, win, turn(east, 3 * WIDE))
    win = jnp.where(lane < PAIR, win, 0.0)
    return (win + turn(win, PAIR)) * KAPPA**SWEEPS


def fold(x):
    return jnp.sum(x.reshape(x.shape[0] // 8, 8, x.shape[1]), axis=0)


def interior_kernel(pack, g, bands, z, first_edge, second_edge, xacc, gbuf, fbuf, prod, lhs, *, batch):
    gbuf[...] = g[0] * KAPPA**SWEEPS
    interior(pack, gbuf, bands, 0, z, first_edge, second_edge, xacc, fbuf, prod, lhs, batch)


def edge_kernel(pack, g_ext, bands, *refs):
    z, first_edge, second_edge, xacc, gbuf, ends, lhs = refs[4:]
    gbuf[...] = g_ext[...] * KAPPA**SWEEPS
    edge_rows(pack, gbuf, bands, 0, z, first_edge, second_edge, xacc, ends, lhs)


def put_edges(old, win, q):
    lane = lanes_of(old)
    cols = old.shape[1]
    new = jnp.where(lane < HALO, turn(win, -WIDE - PAIR * q), old)
    return jnp.where(lane < cols - HALO, new, turn(win, cols - 3 * WIDE - PAIR * q))


def second_interior_kernel(
    pack, p, bands, z_one, zw_one,
    z, first_edge, second_edge, xacc, z_out,
    gbuf, fbuf, prod, lhs, *, batch,
):
    del z_one
    gbuf[...] = p[...] * KAPPA**SWEEPS

    def first_edges(b, i):
        at = b * batch + i
        z_out[at] = put_edges(z_out[at], zw_one[b * (batch // 2) + i // 2], i % 2)

    interior(pack, gbuf, bands, 0, z, first_edge, second_edge, xacc, fbuf, prod, lhs, batch, first_edges)


def join(main, win, cols):
    win = (win + turn(win, PAIR)) * KAPPA**SWEEPS
    lane = lanes_of(win)
    state = jnp.where(lane < HALO, turn(win, -WIDE), main * KAPPA**SWEEPS)
    return jnp.where(lane < cols - HALO, state, turn(win, cols - 3 * WIDE)), win


def window_build(west, east, batch):
    def build(b, i, old):
        u = b * (batch // 4) + i // 4
        at = lanes_of(old) & (PAIR - 1)
        old = jnp.where(at < WIDE, turn(west(u), -WIDE * (i % 4)), old)
        return jnp.where(at >= 3 * WIDE, turn(east(u), 3 * WIDE - WIDE * (i % 4)), old)

    return build


def window_interior_kernel(
    pack_in, grid, near, far, bands,
    pack, z, first_edge, second_edge, xacc,
    gbuf, fbuf, prod, lhs, *, batch,
):
    del pack_in
    levels = grid.shape[1]
    last = near.shape[0] - 1
    west, east = by_parity("gx", far[last], near[last]), by_parity("gx", near[last], far[last])
    for l in range(levels):
        gbuf[l] = window_grid(grid[0, l], turn(west, -slot_lane(l)), turn(east, -slot_lane(l)))
    build = window_build(
        lambda u: by_parity("gx", far[u], near[u]), lambda u: by_parity("gx", near[u], far[u]), batch
    )
    interior(pack, gbuf, bands, 1, z, first_edge, second_edge, xacc, fbuf, prod, lhs, batch, None, build)


def first_kernel(
    pack_in, z_in, first_in, second_in, xacc_in, g_ext, grid, near, far, near_ends, far_ends, bands, xmain,
    pack, z, first_edge, second_edge, xacc, x, p, near_out, far_out, side, sums,
    gbuf, lhs, ends, west, east, *, batch,
):
    del pack_in, z_in, first_in, second_in, xacc_in
    levels, reach, cols = g_ext.shape
    rows = reach - 2 * HALO
    last = west.shape[0] - 1
    west[:, HALO : HALO + rows, :] = by_parity("gx", far[...], near[...])
    east[:, HALO : HALO + rows, :] = by_parity("gx", near[...], far[...])
    for start, at in ((0, 0), (HALO + rows, HALO)):
        a, b = near_ends[:, at : at + HALO, :], far_ends[:, at : at + HALO, :]
        west[:, start : start + HALO, :] = by_parity("gx", b, a)
        east[:, start : start + HALO, :] = by_parity("gx", a, b)
    for l in range(levels):
        gbuf[l] = window_grid(g_ext[l], turn(west[last], -slot_lane(l)), turn(east[last], -slot_lane(l)))
    for start in (0, HALO + rows):
        span = slice(start, start + HALO)
        build = window_build(lambda u: west[u, span, :], lambda u: east[u, span, :], batch)
        for i in range(pack.shape[0]):
            pack[i, span, :] = build(0, i, pack[i, span, :])
    edge_rows(pack, gbuf, bands, 1, z, first_edge, second_edge, xacc, ends, lhs)
    lane = lax.broadcasted_iota(jnp.int32, (reach, cols), 1)
    norm = jnp.zeros((8, cols), F32)
    curve = norm
    lane = lane[:rows]
    d_west, d_east = west[last, HALO : HALO + rows, :], east[last, HALO : HALO + rows, :]
    sides = jnp.zeros((rows, cols), F32)
    for l in range(levels):
        state, win = join(xmain[l], xacc[l], cols)
        push = grid[1, l] * state
        x[l] = state
        p[l] = push
        near_out[l] = by_parity("gy", push[rows - HALO :], push[:HALO])
        far_out[l] = by_parity("gy", push[:HALO], push[rows - HALO :])
        norm += fold(grid[0, l] * state)
        curve += fold(push * state)
        base = WIDE * l
        mine = slot_lane(levels + l)
        beside = turn(win, base - HALO) * turn(d_west, base - mine - HALO)
        sides = jnp.where((lane >= base) & (lane < base + HALO), beside, sides)
        beside = turn(win, base + HALO - 3 * WIDE) * turn(d_east, base + HALO - mine)
        sides = jnp.where((lane >= base + HALO) & (lane < base + WIDE), beside, sides)
    side[...] = sides
    near_out[levels] = by_parity("gy", sides[rows - HALO :], sides[:HALO])
    far_out[levels] = by_parity("gy", sides[:HALO], sides[rows - HALO :])
    sums[0] = norm
    sums[1] = curve


def second_kernel(
    mains, wins, p, side, near, far, grid, bands, sums, z_in, first_in, second_in, xmain_in,
    x, share, zm, first_edge, second_edge, xmain,
    ext, gbuf, fbuf, prod, lhs, xacc, zw, ends, *, batch,
):
    del z_in, first_in, second_in, xmain_in
    levels, rows, cols = p.shape
    reach = rows + 2 * HALO
    for l in range(levels + 1):
        ext[l, HALO : HALO + rows, :] = p[l] if l < levels else side[...]
        ext[l, 0:HALO, :] = by_parity("gy", far[l], near[l])
        ext[l, HALO + rows :, :] = by_parity("gy", near[l], far[l])
    me = lax.axis_index("gy")

    def reflect(base, step):
        for l in range(levels + 1):
            for j in range(1, HALO):
                ext[l, base - step * j : base - step * j + 1, :] = -ext[l, base + step * j : base + step * j + 1, :]

    pl.when(me == 0)(lambda: reflect(HALO - 1, 1))
    pl.when(me == lax.axis_size("gy") - 1)(lambda: reflect(HALO + rows, -1))
    lane = lax.broadcasted_iota(jnp.int32, (reach, cols), 1)
    for l in range(levels):
        gbuf[0, l] = ext[l] * KAPPA**SWEEPS
        west = jnp.where(lane < HALO, 0.0, turn(ext[levels], HALO - WIDE * l))
        east = jnp.where(lane < HALO, turn(ext[levels], -HALO - WIDE * l), 0.0)
        gbuf[1, l] = window_grid(ext[l], west, east)

    def second_edges(b, i, v):
        for q in range(2):
            at = 2 * (b * batch + i) + q
            zm[at] = put_edges(zm[at], v, q)

    edge_rows(mains, gbuf.at[0], bands, 0, zm, first_edge, second_edge, xmain, ends, lhs)
    covariance(wins, bands, 1, gbuf.at[1], zw, xacc, fbuf, prod, lhs, batch, None, second_edges)
    cross = jnp.zeros((8, cols), F32)
    curve = cross
    for l in range(levels):
        state, _ = join(xmain[l], xacc[l], cols)
        x[l] = state
        cross += fold(p[l] * state)
        curve += fold(grid[1, l] * state * state)
    out = jnp.zeros((1, cols), F32)
    place = lax.broadcasted_iota(jnp.int32, (1, cols), 1)
    for i, part in enumerate((sums[0], sums[1], cross, curve)):
        out = jnp.where(place == i, jnp.sum(jnp.sum(part, axis=0, keepdims=True), axis=1, keepdims=True), out)
    share[...] = jnp.broadcast_to(out, share.shape)


def final_kernel(share, z_one, z_two, x_one, x_two, control, increment, stage, x_stage, sems):
    members, levels, rows, cols = control.shape
    total = jnp.sum(share[...], axis=0, keepdims=True)
    place = lax.broadcasted_iota(jnp.int32, (1, cols), 1)
    n0, c1, c2, c3 = (jnp.sum(jnp.where(place == i, total, 0.0), axis=1, keepdims=True) for i in range(4))
    bn2 = n0 + EPS
    alpha_one = (n0 + c1) / bn2
    t = (EPS - c1) / bn2
    rr = jnp.maximum((c2 + 2.0 * t * c1 + t * t * n0) / bn2, 0.0)
    beta_sq = rr + EPS
    alpha_two = (rr + jnp.maximum((c3 + 2.0 * t * c2 + t * t * c1) / bn2, 0.0)) / beta_sq
    det = alpha_one * alpha_two - beta_sq
    coef_b = -1.0 / det
    coef_a = (alpha_two - t) / det
    copies = []
    part = stage.shape[0] // (sems.shape[0] - 1)
    for c in range(sems.shape[0] - 1):

        def body(i, _):
            f = c * part + i
            one, two = z_one[f, SWEEPS : SWEEPS + rows, :], z_two[f, SWEEPS : SWEEPS + rows, :]
            stage[f] = coef_a * one + coef_b * two
            return 0

        lax.fori_loop(0, part, body, 0, unroll=4)
        level, first = divmod(c * part, members)
        copies.append(
            pltpu.make_async_copy(
                stage.at[pl.ds(c * part, part)], control.at[pl.ds(first, part), level], sems.at[c]
            )
        )
        copies[-1].start()
    x_stage[...] = coef_a * x_one[...] + coef_b * x_two[...]
    copies.append(pltpu.make_async_copy(x_stage, increment, sems.at[sems.shape[0] - 1]))
    copies[-1].start()
    for copy in copies:
        copy.wait()


def on_device(ensemble, obs_cell, obs_level, innovation, obs_weight):
    members, levels, rows, cols = ensemble.shape
    fields = members * levels
    reach = rows + 2 * HALO
    batch = 32
    strips = fields // 8 + 1
    devices = lax.axis_size("gy") * lax.axis_size("gx")
    hbm = pl.BlockSpec(memory_space=pltpu.HBM)

    def struct(*shape):
        return jax.ShapeDtypeStruct(shape, F32)

    def call(kernel, outs, ins, scratch=(), limit=24, work=2, **kw):
        return pl.pallas_call(
            kernel,
            out_shape=outs,
            in_specs=[VMEM] * ins if isinstance(ins, int) else ins,
            out_specs=jax.tree.map(lambda _: VMEM, outs),
            scratch_shapes=scratch,
            compiler_params=pltpu.CompilerParams(vmem_limit_bytes=limit * 2**20),
            cost_estimate=pl.CostEstimate(flops=work * 10**9, bytes_accessed=10**6, transcendentals=0),
            **kw,
        )

    bands = jnp.asarray(band_matrices(cols), BF16)
    obs = obs_cell.shape
    edge = pltpu.VMEM((members, levels, 16, cols), BF16)
    grid, near, far = call(
        scatter_kernel,
        (struct(2, levels, rows, cols), struct(fields + levels, HALO, cols), struct(fields + levels, HALO, cols)),
        [hbm] * 5,
        [pltpu.VMEM(obs, jnp.int32)] * 2 + [pltpu.VMEM(obs, F32)] * 2 + [edge, edge, pltpu.SemaphoreType.DMA((6,))],
        limit=60,
    )(ensemble, obs_cell, obs_level, innovation, obs_weight)
    near, far = swap(near, "gy", 0), swap(far, "gy", 1)
    main_shape, win_shape = struct(fields, reach, cols), struct(fields // 2, reach, cols)
    g_shape = struct(levels, reach, cols)
    own_shape, end_shape = struct(strips, rows, cols), struct(strips, 2 * HALO, cols)
    mains, wins, near_own, far_own, g_ext, mirror, bands = call(
        own_kernel,
        (
            main_shape,
            win_shape,
            own_shape,
            own_shape,
            g_shape,
            struct(2, fields + levels, HALO, cols),
            jax.ShapeDtypeStruct((2, 2 * cols, SWEEPS * cols), BF16),
        ),
        [hbm, VMEM, hbm],
        [pltpu.VMEM(ensemble.shape, BF16), pltpu.SemaphoreType.DMA((3,))],
    )(ensemble, grid, bands)
    near_own, far_own = swap(near_own, "gx", 0), swap(far_own, "gx", 1)
    work = (
        pltpu.VMEM((batch, reach, cols), F32),
        pltpu.VMEM((SWEEPS, batch * reach, cols), F32),
        pltpu.VMEM((batch * reach, 2 * cols), BF16),
    )
    zm_shape, zw_shape = struct(fields, reach - HALO, cols), struct(fields // 2, reach - HALO, cols)
    state_shape = struct(levels, rows, cols)
    edge_shape = struct(SWEEPS, 2 * fields, 2 * HALO, cols)
    part_shapes = (zm_shape, edge_shape, edge_shape, state_shape)
    ends = pltpu.VMEM((2 * fields, 2 * HALO, cols), F32)
    part = call(
        functools.partial(interior_kernel, batch=batch),
        part_shapes,
        3,
        (pltpu.VMEM((levels, rows, cols), F32), *work),
    )(mains, grid, bands)
    mains, wins, g_ext, near, far = call(
        halo_kernel, (main_shape, win_shape, g_shape, end_shape, end_shape), 7, input_output_aliases={3: 0, 4: 1, 5: 2}
    )(near, far, mirror, mains, wins, g_ext, part[3])
    near, far = swap(near, "gx", 0), swap(far, "gx", 1)
    gbuf = pltpu.VMEM((levels, reach, cols), F32)
    zm_one, _, _, xmain = call(
        edge_kernel, part_shapes, 7, (gbuf, ends, work[2]), input_output_aliases={3: 0, 4: 1, 5: 2, 6: 3}
    )(mains, g_ext, bands, *part)
    win_edge = struct(SWEEPS, fields, 2 * HALO, cols)
    win_parts = (win_shape, zw_shape, win_edge, win_edge, state_shape)
    wins_part = call(
        functools.partial(window_interior_kernel, batch=batch),
        win_parts,
        5,
        (pltpu.VMEM((levels, rows, cols), F32), *work),
        input_output_aliases={0: 0},
    )(wins, grid, near_own, far_own, bands)
    wins, zw_one, _, _, _, x_one, p, near, far, side, sums = call(
        functools.partial(first_kernel, batch=batch),
        (
            *win_parts,
            state_shape,
            state_shape,
            struct(levels + 1, HALO, cols),
            struct(levels + 1, HALO, cols),
            struct(rows, cols),
            struct(2, 8, cols),
        ),
        13,
        (
            gbuf,
            work[2],
            pltpu.VMEM((fields, 2 * HALO, cols), F32),
            *[pltpu.VMEM((strips, reach, cols), F32)] * 2,
        ),
        input_output_aliases={i: i for i in range(5)},
    )(*wins_part, g_ext, grid, near_own, far_own, near, far, bands, xmain)
    near, far = swap(near, "gy", 0), swap(far, "gy", 1)
    *part, zm_one = call(
        functools.partial(second_interior_kernel, batch=batch),
        (*part_shapes, zm_shape),
        5,
        (pltpu.VMEM((levels, rows, cols), F32), *work),
        input_output_aliases={3: 4},
    )(mains, p, bands, zm_one, zw_one)
    x_two, share, zm_two, _, _, _ = call(
        functools.partial(second_kernel, batch=batch),
        (state_shape, struct(devices, cols), *part_shapes),
        13,
        (
            pltpu.VMEM((levels + 1, reach, cols), F32),
            pltpu.VMEM((2, levels, reach, cols), F32),
            *work,
            pltpu.VMEM((levels, rows, cols), F32),
            pltpu.VMEM((fields // 2, reach - HALO, cols), F32),
            ends,
        ),
        input_output_aliases={9: 2, 10: 3, 11: 4, 12: 5},
    )(mains, wins, p, side, near, far, grid, bands, sums, *part)
    share = lax.all_to_all(share, ("gy", "gx"), 0, 0, tiled=True)
    chunks = 8
    return pl.pallas_call(
        final_kernel,
        out_shape=(struct(members, levels, rows, cols), struct(levels, rows, cols)),
        in_specs=[VMEM] * 5,
        out_specs=(hbm, hbm),
        scratch_shapes=[
            pltpu.VMEM((fields, rows, cols), F32),
            pltpu.VMEM((levels, rows, cols), F32),
            pltpu.SemaphoreType.DMA((chunks + 1,)),
        ],
        compiler_params=pltpu.CompilerParams(vmem_limit_bytes=16 * 2**20),
    )(share, zm_one, zm_two, x_one, x_two)


def solution(mesh):
    return jax.shard_map(
        on_device,
        mesh=mesh,
        in_specs=(
            P(None, None, "gy", "gx"),
            P("gy", "gx", None),
            P("gy", "gx", None),
            P("gy", "gx", None),
            P("gy", "gx", None),
        ),
        out_specs=(P(None, None, "gy", "gx"), P(None, "gy", "gx")),
        check_vma=False,
    )
```

```python
import functools
import math

import jax
import jax.numpy as jnp
import numpy as np
from jax import lax
from jax.experimental import pallas as pl
from jax.experimental.pallas import tpu as pltpu
from jax.sharding import PartitionSpec as P

SWEEPS = 4
KAPPA = 0.2
EPS = 1e-06
HALO = 2 * SWEEPS
WIDE = 2 * HALO
PAIR = 4 * WIDE
VMEM = pl.BlockSpec(memory_space=pltpu.VMEM)
F32 = jnp.float32
BF16 = jnp.bfloat16


def band_matrices(lanes):
    out = np.zeros((4, 2, lanes, SWEEPS * lanes), np.float32)
    lane = np.arange(lanes)
    for variant in range(4):
        for kind in range(2):
            col, part = lane, 0 * lane
            if kind == 1:
                j = lane % PAIR
                col = np.where(j < 2 * WIDE, j - WIDE, lanes - 3 * WIDE + j)
                part = lane // (2 * WIDE)
            inside = np.ones(lanes, bool)
            if variant % 2:
                inside &= col >= 0
            if variant // 2:
                inside &= col < lanes
            near = (np.abs(lane[:, None] - lane[None, :]) <= 1) & (part[:, None] == part[None, :])
            band = (near & inside[:, None] & inside[None, :]).astype(np.float64)
            power = [np.diag(inside.astype(np.float64))]
            for _ in range(SWEEPS):
                power.append(power[-1] @ band)
            for j in range(SWEEPS):
                q = sum(
                    math.comb(SWEEPS, k) * math.comb(SWEEPS - k, (SWEEPS - k - j) // 2) * power[k]
                    for k in range(SWEEPS - j + 1)
                    if (SWEEPS - k - j) % 2 == 0
                )
                out[variant, kind, :, j * lanes : (j + 1) * lanes] = q
    return out


def swap(x, axis, odd):
    count = lax.axis_size(axis)
    return lax.ppermute(x, axis, [(i + a, i + 1 - a) for i in range(odd, count - 1, 2) for a in range(2)])


def by_parity(axis, even, odd):
    me = jnp.full(even.shape, lax.axis_index(axis), jnp.int32)
    return jnp.where((me & 1) == 0, even, odd)


def turn(x, amount):
    amount %= x.shape[-1]
    return pltpu.roll(x, amount, x.ndim - 1) if amount else x


def lanes_of(x):
    return lax.broadcasted_iota(jnp.int32, x.shape, x.ndim - 1)


def scatter_kernel(ens, cell_in, level_in, innov_in, weight_in, grid, near, far, cell, level, innov, weight, first, last, sem):
    members, levels, rows, cols = ens.shape
    obs = cell.shape[-1]
    copies = [
        pltpu.make_async_copy(a, b, sem.at[i])
        for i, (a, b) in enumerate(
            (
                (cell_in, cell),
                (level_in, level),
                (innov_in, innov),
                (weight_in, weight),
                (ens.at[:, :, 0:16, :], first),
                (ens.at[:, :, rows - 16 : rows, :], last),
            )
        )
    ]
    for c in copies:
        c.start()
    for c in copies[:4]:
        c.wait()
    span = 256
    row_iota = lax.broadcasted_iota(jnp.int32, (levels * rows, span), 0)
    col_iota = lax.broadcasted_iota(jnp.int32, (cols, span), 0)
    acc = jnp.zeros((4 * levels * rows, cols), F32)
    for start in range(0, obs, span):
        at = slice(start, start + span)
        spot = cell[0, :, at]
        here = row_iota == level[0, :, at] * rows + spot // cols
        w = weight[0, :, at]
        parts = []
        for value in (w * innov[0, :, at], w):
            high = value.astype(BF16).astype(F32)
            parts += [high, value - high]
        left = jnp.concatenate([jnp.where(here, part, 0.0).astype(BF16) for part in parts], axis=0)
        right = jnp.where(col_iota == spot % cols, 1.0, 0.0).astype(BF16)
        acc += lax.dot_general(left, right, (((1,), (1,)), ((), ())), preferred_element_type=F32)
    n = levels * rows
    g = acc[:n] + acc[n : 2 * n]
    d = acc[2 * n : 3 * n] + acc[3 * n :]
    fields = members * levels
    for l in range(levels):
        grid[0, l] = g[l * rows : (l + 1) * rows]
        grid[1, l] = d[l * rows : (l + 1) * rows]
        up = g[l * rows : l * rows + HALO]
        down = g[(l + 1) * rows - HALO : (l + 1) * rows]
        near[fields + l] = by_parity("gy", down, up)
        far[fields + l] = by_parity("gy", up, down)
    for c in copies[4:]:
        c.wait()

    def edge(m, _):
        for l in range(levels):
            up = first[m, l].astype(F32)[:HALO]
            down = last[m, l].astype(F32)[16 - HALO :]
            near[l * members + m] = by_parity("gy", down, up)
            far[l * members + m] = by_parity("gy", up, down)
        return 0

    lax.fori_loop(0, members, edge, 0)


def slot_lane(t):
    return PAIR * (t % 2) + WIDE * (t // 2)


def strip(xs, at, near, far):
    lane = lanes_of(xs[0])
    west = east = jnp.zeros_like(xs[0])
    for t, x in enumerate(xs):
        base = slot_lane(t)
        here = (lane >= base) & (lane < base + WIDE)
        west = jnp.where(here, turn(x, base), west)
        east = jnp.where(here, turn(x, base + WIDE), east)
    near[at] = by_parity("gx", east, west)
    far[at] = by_parity("gx", west, east)


def arrange(u, get, mains, wins, near, far, spans):
    xs = [get(8 * u + t) for t in range(8)]
    lane = lanes_of(xs[0])

    def put(ref, f, value):
        at = 0
        for start, count in spans:
            ref[f, start : start + count, :] = value[at : at + count]
            at += count

    for t, x in enumerate(xs):
        put(mains, 8 * u + t, x)
    strip(xs, u, near, far)
    for v in range(4):
        win = jnp.zeros_like(xs[0])
        for q in range(2):
            x = xs[2 * v + q]
            at = lane - PAIR * q
            win = jnp.where((at >= WIDE) & (at < 2 * WIDE), turn(x, PAIR * q + WIDE), win)
            win = jnp.where((at >= 2 * WIDE) & (at < 3 * WIDE), turn(x, PAIR * q + 3 * WIDE), win)
        put(wins, 4 * u + v, win)


def own_kernel(ens_in, grid, bands_in, mains, wins, near, far, g_ext, mirror, bands, ens, sem):
    members, levels, rows, cols = ens.shape
    fields = members * levels
    gx = lax.axis_index("gx")
    variant = jnp.where(gx == 0, 1, 0) + jnp.where(gx == lax.axis_size("gx") - 1, 2, 0)
    copies = [pltpu.make_async_copy(ens_in, ens, sem.at[0])]
    for half in range(2):
        part = bands.at[:, half * cols : (half + 1) * cols, :]
        copies.append(pltpu.make_async_copy(bands_in.at[variant], part, sem.at[1 + half]))
    for c in copies:
        c.start()
    for c in copies:
        c.wait()
    spans = ((HALO, rows),)

    def group(u, _):
        l = 8 * u // members
        arrange(u, lambda f: ens[f - l * members, l].astype(F32), mains, wins, near, far, spans)
        return 0

    lax.fori_loop(0, fields // 8, group, 0)
    strip([grid[k, l] for k in range(2) for l in range(levels)], fields // 8, near, far)
    for l in range(levels):
        g_ext[l, HALO : HALO + rows, :] = grid[0, l]
    mirror[...] = jnp.zeros_like(mirror)
    me = lax.axis_index("gy")
    row = lax.broadcasted_iota(jnp.int32, (HALO, cols), 0)

    def flip(x, step):
        out = jnp.zeros((HALO, cols), F32)
        for j in range(1, HALO):
            if step > 0:
                out = jnp.where(row == HALO - 1 - j, x[j - 1 : j], out)
            else:
                out = jnp.where(row == j, x[HALO - j : HALO - j + 1], out)
        return out

    def side(step):
        at = 0 if step > 0 else rows - HALO
        slot = 0 if step > 0 else 1
        start = 0 if step > 0 else rows - 16
        skip = 0 if step > 0 else 16 - HALO

        def body(m, _):
            for l in range(levels):
                x = ens[m, l, start : start + 16, :].astype(F32)[skip : skip + HALO]
                mirror[slot, l * members + m] = flip(x, step)
            return 0

        lax.fori_loop(0, members, body, 0)
        for l in range(levels):
            mirror[slot, fields + l] = -flip(grid[0, l, at : at + HALO, :], step)

    pl.when(me == 0)(lambda: side(1))
    pl.when(me == lax.axis_size("gy") - 1)(lambda: side(-1))


def halo_kernel(from_near, from_far, mirror, *refs):
    mains, wins, g_ext, near, far = refs[4:]
    levels, reach, cols = g_ext.shape
    fields = mirror.shape[1] - levels
    spans = ((0, HALO), (reach - HALO, HALO))

    def get(f):
        a, b = from_near[f], from_far[f]
        return jnp.concatenate([by_parity("gy", b, a) + mirror[0, f], by_parity("gy", a, b) + mirror[1, f]], axis=0)

    def group(u, _):
        arrange(u, get, mains, wins, near, far, spans)
        return 0

    lax.fori_loop(0, fields // 8, group, 0)
    ends = [get(fields + l) for l in range(levels)]
    strip(ends, fields // 8, near, far)
    for l in range(levels):
        g_ext[l, 0:HALO, :] = ends[l][:HALO]
        g_ext[l, reach - HALO :, :] = ends[l][HALO:]


def band_products(lhs, bands, kind, out, count):
    lanes = lhs.shape[1] // 2
    for half in range(SWEEPS // 2):
        r = jnp.dot(
            lhs[0:count, :],
            bands[kind, :, half * 2 * lanes : (half + 1) * 2 * lanes],
            preferred_element_type=F32,
        )
        out[2 * half, 0:count, :] = r[:, :lanes]
        out[2 * half + 1, 0:count, :] = r[:, lanes:]


def split_into(lhs, start, x):
    count, lanes = x.shape
    high = x.astype(BF16)
    lhs[start : start + count, 0:lanes] = high
    lhs[start : start + count, lanes : 2 * lanes] = (x - high.astype(F32)).astype(BF16)


def combine(part, src, count):
    total = src(2 * SWEEPS) + src(0)
    for k in range(1, SWEEPS):
        total += part(k, SWEEPS + k) + part(k, SWEEPS - k)
    return total + part(0, SWEEPS)


def rows_of(prod, start, count):
    return lambda k, off: prod[k, pl.ds(start + off, count), :]


def field_rows(ref, f, count, base=0):
    return lambda off: ref[f, pl.ds(base + off, count), :]


def interior(pack, g, bands, kind, z, first_edge, second_edge, xacc, fbuf, prod, lhs, batch, also=None, build=None):
    count, reach, _ = pack.shape
    rows = reach - 2 * HALO
    mid, core = rows - HALO, rows - 2 * HALO
    per_level = count // g.shape[0]
    xacc[...] = jnp.zeros_like(xacc)

    def keep(edge, at, start, size):
        for k in range(SWEEPS):
            edge[k, at, HALO : 2 * HALO, :] = prod[k, start : start + HALO, :]
            edge[k, count + at, 0:HALO, :] = prod[k, start + size - HALO : start + size, :]

    def step(b, _):
        for i in range(batch):
            if build is not None:
                pack[b * batch + i, HALO : HALO + rows, :] = build(b, i, pack[b * batch + i, HALO : HALO + rows, :])
            f = pack[b * batch + i, HALO : HALO + rows, :] * g[level_at(b, i, batch, per_level)]
            fbuf[i, 0:rows, :] = f
            split_into(lhs, i * rows, f)
        band_products(lhs, bands, kind, prod, batch * rows)
        for i in range(batch):
            at = b * batch + i
            v = combine(rows_of(prod, i * rows, mid), field_rows(fbuf, i, mid), mid)
            z[at, HALO : HALO + mid, :] = v
            keep(first_edge, at, i * rows, rows)
            split_into(lhs, i * mid, v)
            if also is not None:
                also(b, i)
        band_products(lhs, bands, kind, prod, batch * mid)
        for i in range(batch):
            at = b * batch + i
            v = combine(rows_of(prod, i * mid, core), field_rows(z, at, core, HALO), core)
            keep(second_edge, at, i * mid, mid)
            level = level_at(b, i, batch, per_level)
            xacc[level, HALO : HALO + core, :] += v * pack[at, 2 * HALO : 2 * HALO + core, :]
        return 0

    lax.fori_loop(0, count // batch, step, 0)


def edge_rows(pack, g, bands, kind, z, first_edge, second_edge, xacc, ends, lhs):
    count, reach, lanes = pack.shape
    rows = reach - 2 * HALO
    per_level = count // g.shape[0]
    sides = [(side, f) for side in range(2) for f in range(count)]

    def products(edge):
        for half in range(SWEEPS // 2):
            r = jnp.dot(
                lhs[0 : 2 * count * HALO, :],
                bands[kind, :, half * 2 * lanes : (half + 1) * 2 * lanes],
                preferred_element_type=F32,
            )
            for t in range(2):
                part = r[:, t * lanes : (t + 1) * lanes].reshape(2 * count, HALO, lanes)
                edge[2 * half + t, 0:count, 0:HALO, :] = part[:count]
                edge[2 * half + t, count:, HALO : 2 * HALO, :] = part[count:]

    def near(edge, j):
        return lambda k, off: edge[k, j, pl.ds(off, HALO), :]

    for side, f in sides:
        base = side * rows
        x = pack[f, base : base + 2 * HALO, :] * g[f // per_level, base : base + 2 * HALO, :]
        j = side * count + f
        ends[j] = x
        split_into(lhs, j * HALO, x[side * HALO : (side + 1) * HALO])
    products(first_edge)
    for side, f in sides:
        j = side * count + f
        v = combine(near(first_edge, j), field_rows(ends, j, HALO), HALO)
        z[f, side * rows : side * rows + HALO, :] = v
        split_into(lhs, j * HALO, v)
    products(second_edge)
    for side in range(2):
        for level in range(g.shape[0]):
            total = jnp.zeros((HALO, lanes), F32)
            for f in range(level * per_level, (level + 1) * per_level):
                base = side * (rows - HALO)
                v = combine(near(second_edge, side * count + f), field_rows(z, f, HALO, base), HALO)
                total += v * pack[f, HALO + base : 2 * HALO + base, :]
            xacc[level, base : base + HALO, :] = total


def level_at(b, i, batch, per_level):
    return b * batch // per_level if batch <= per_level else i // per_level


def covariance(pack, bands, kind, g, z, xacc, fbuf, prod, lhs, batch, build=None, also=None):
    count, reach, _ = pack.shape
    inner, rows = reach - HALO, reach - 2 * HALO
    per_level = count // g.shape[0]
    xacc[...] = jnp.zeros_like(xacc)

    def step(b, _):
        for i in range(batch):
            at = b * batch + i
            level = level_at(b, i, batch, per_level)
            if build is not None:
                pack[at] = build(b, i, pack[at])
            f = pack[at] * g[level]
            fbuf[i] = f
            split_into(lhs, i * reach, f)
        band_products(lhs, bands, kind, prod, batch * reach)
        for i in range(batch):
            v = combine(rows_of(prod, i * reach, inner), field_rows(fbuf, i, inner), inner)
            z[b * batch + i] = v
            split_into(lhs, i * inner, v)
            if also is not None:
                also(b, i, v)
        band_products(lhs, bands, kind, prod, batch * inner)
        for i in range(batch):
            level = level_at(b, i, batch, per_level)
            v = combine(rows_of(prod, i * inner, rows), field_rows(z, b * batch + i, rows), rows)
            xacc[level] += v * pack[b * batch + i, HALO : HALO + rows, :]
        return 0

    lax.fori_loop(0, count // batch, step, 0)


def window_grid(g, west, east):
    lane = lanes_of(g)
    win = jnp.where(lane < WIDE, west, turn(g, WIDE))
    win = jnp.where(lane < 2 * WIDE, win, turn(g, 3 * WIDE))
    win = jnp.where(lane < 3 * WIDE, win, turn(east, 3 * WIDE))
    win = jnp.where(lane < PAIR, win, 0.0)
    return (win + turn(win, PAIR)) * KAPPA**SWEEPS


def fold(x):
    return jnp.sum(x.reshape(x.shape[0] // 8, 8, x.shape[1]), axis=0)


def interior_kernel(pack, g, bands, z, first_edge, second_edge, xacc, gbuf, fbuf, prod, lhs, *, batch):
    gbuf[...] = g[0] * KAPPA**SWEEPS
    interior(pack, gbuf, bands, 0, z, first_edge, second_edge, xacc, fbuf, prod, lhs, batch)


def edge_kernel(pack, g_ext, bands, *refs):
    z, first_edge, second_edge, xacc, gbuf, ends, lhs = refs[4:]
    gbuf[...] = g_ext[...] * KAPPA**SWEEPS
    edge_rows(pack, gbuf, bands, 0, z, first_edge, second_edge, xacc, ends, lhs)


def put_edges(old, win, q):
    lane = lanes_of(old)
    cols = old.shape[1]
    new = jnp.where(lane < HALO, turn(win, -WIDE - PAIR * q), old)
    return jnp.where(lane < cols - HALO, new, turn(win, cols - 3 * WIDE - PAIR * q))


def second_interior_kernel(
    pack, p, bands, z_one, zw_one,
    z, first_edge, second_edge, xacc, z_out,
    gbuf, fbuf, prod, lhs, *, batch,
):
    del z_one
    gbuf[...] = p[...] * KAPPA**SWEEPS

    def first_edges(b, i):
        at = b * batch + i
        z_out[at] = put_edges(z_out[at], zw_one[b * (batch // 2) + i // 2], i % 2)

    interior(pack, gbuf, bands, 0, z, first_edge, second_edge, xacc, fbuf, prod, lhs, batch, first_edges)


def join(main, win, cols):
    win = (win + turn(win, PAIR)) * KAPPA**SWEEPS
    lane = lanes_of(win)
    state = jnp.where(lane < HALO, turn(win, -WIDE), main * KAPPA**SWEEPS)
    return jnp.where(lane < cols - HALO, state, turn(win, cols - 3 * WIDE)), win


def window_build(west, east, batch):
    def build(b, i, old):
        u = b * (batch // 4) + i // 4
        at = lanes_of(old) & (PAIR - 1)
        old = jnp.where(at < WIDE, turn(west(u), -WIDE * (i % 4)), old)
        return jnp.where(at >= 3 * WIDE, turn(east(u), 3 * WIDE - WIDE * (i % 4)), old)

    return build


def window_interior_kernel(
    pack_in, grid, near, far, bands,
    pack, z, first_edge, second_edge, xacc,
    gbuf, fbuf, prod, lhs, *, batch,
):
    del pack_in
    levels = grid.shape[1]
    last = near.shape[0] - 1
    west, east = by_parity("gx", far[last], near[last]), by_parity("gx", near[last], far[last])
    for l in range(levels):
        gbuf[l] = window_grid(grid[0, l], turn(west, -slot_lane(l)), turn(east, -slot_lane(l)))
    build = window_build(
        lambda u: by_parity("gx", far[u], near[u]), lambda u: by_parity("gx", near[u], far[u]), batch
    )
    interior(pack, gbuf, bands, 1, z, first_edge, second_edge, xacc, fbuf, prod, lhs, batch, None, build)


def first_kernel(
    pack_in, z_in, first_in, second_in, xacc_in, g_ext, grid, near, far, near_ends, far_ends, bands, xmain,
    pack, z, first_edge, second_edge, xacc, x, p, near_out, far_out, side, sums,
    gbuf, lhs, ends, west, east, *, batch,
):
    del pack_in, z_in, first_in, second_in, xacc_in
    levels, reach, cols = g_ext.shape
    rows = reach - 2 * HALO
    last = west.shape[0] - 1
    west[:, HALO : HALO + rows, :] = by_parity("gx", far[...], near[...])
    east[:, HALO : HALO + rows, :] = by_parity("gx", near[...], far[...])
    for start, at in ((0, 0), (HALO + rows, HALO)):
        a, b = near_ends[:, at : at + HALO, :], far_ends[:, at : at + HALO, :]
        west[:, start : start + HALO, :] = by_parity("gx", b, a)
        east[:, start : start + HALO, :] = by_parity("gx", a, b)
    for l in range(levels):
        gbuf[l] = window_grid(g_ext[l], turn(west[last], -slot_lane(l)), turn(east[last], -slot_lane(l)))
    for start in (0, HALO + rows):
        span = slice(start, start + HALO)
        build = window_build(lambda u: west[u, span, :], lambda u: east[u, span, :], batch)
        for i in range(pack.shape[0]):
            pack[i, span, :] = build(0, i, pack[i, span, :])
    edge_rows(pack, gbuf, bands, 1, z, first_edge, second_edge, xacc, ends, lhs)
    lane = lax.broadcasted_iota(jnp.int32, (reach, cols), 1)
    norm = jnp.zeros((8, cols), F32)
    curve = norm
    lane = lane[:rows]
    d_west, d_east = west[last, HALO : HALO + rows, :], east[last, HALO : HALO + rows, :]
    sides = jnp.zeros((rows, cols), F32)
    for l in range(levels):
        state, win = join(xmain[l], xacc[l], cols)
        push = grid[1, l] * state
        x[l] = state
        p[l] = push
        near_out[l] = by_parity("gy", push[rows - HALO :], push[:HALO])
        far_out[l] = by_parity("gy", push[:HALO], push[rows - HALO :])
        norm += fold(grid[0, l] * state)
        curve += fold(push * state)
        base = WIDE * l
        mine = slot_lane(levels + l)
        beside = turn(win, base - HALO) * turn(d_west, base - mine - HALO)
        sides = jnp.where((lane >= base) & (lane < base + HALO), beside, sides)
        beside = turn(win, base + HALO - 3 * WIDE) * turn(d_east, base + HALO - mine)
        sides = jnp.where((lane >= base + HALO) & (lane < base + WIDE), beside, sides)
    side[...] = sides
    near_out[levels] = by_parity("gy", sides[rows - HALO :], sides[:HALO])
    far_out[levels] = by_parity("gy", sides[:HALO], sides[rows - HALO :])
    sums[0] = norm
    sums[1] = curve


def second_kernel(
    mains, wins, p, side, near, far, grid, bands, sums, z_in, first_in, second_in, xmain_in,
    x, share, zm, first_edge, second_edge, xmain,
    ext, gbuf, fbuf, prod, lhs, xacc, zw, ends, *, batch,
):
    del z_in, first_in, second_in, xmain_in
    levels, rows, cols = p.shape
    reach = rows + 2 * HALO
    for l in range(levels + 1):
        ext[l, HALO : HALO + rows, :] = p[l] if l < levels else side[...]
        ext[l, 0:HALO, :] = by_parity("gy", far[l], near[l])
        ext[l, HALO + rows :, :] = by_parity("gy", near[l], far[l])
    me = lax.axis_index("gy")

    def reflect(base, step):
        for l in range(levels + 1):
            for j in range(1, HALO):
                ext[l, base - step * j : base - step * j + 1, :] = -ext[l, base + step * j : base + step * j + 1, :]

    pl.when(me == 0)(lambda: reflect(HALO - 1, 1))
    pl.when(me == lax.axis_size("gy") - 1)(lambda: reflect(HALO + rows, -1))
    lane = lax.broadcasted_iota(jnp.int32, (reach, cols), 1)
    for l in range(levels):
        gbuf[0, l] = ext[l] * KAPPA**SWEEPS
        west = jnp.where(lane < HALO, 0.0, turn(ext[levels], HALO - WIDE * l))
        east = jnp.where(lane < HALO, turn(ext[levels], -HALO - WIDE * l), 0.0)
        gbuf[1, l] = window_grid(ext[l], west, east)

    def second_edges(b, i, v):
        for q in range(2):
            at = 2 * (b * batch + i) + q
            zm[at] = put_edges(zm[at], v, q)

    edge_rows(mains, gbuf.at[0], bands, 0, zm, first_edge, second_edge, xmain, ends, lhs)
    covariance(wins, bands, 1, gbuf.at[1], zw, xacc, fbuf, prod, lhs, batch, None, second_edges)
    cross = jnp.zeros((8, cols), F32)
    curve = cross
    for l in range(levels):
        state, _ = join(xmain[l], xacc[l], cols)
        x[l] = state
        cross += fold(p[l] * state)
        curve += fold(grid[1, l] * state * state)
    out = jnp.zeros((1, cols), F32)
    place = lax.broadcasted_iota(jnp.int32, (1, cols), 1)
    for i, part in enumerate((sums[0], sums[1], cross, curve)):
        out = jnp.where(place == i, jnp.sum(jnp.sum(part, axis=0, keepdims=True), axis=1, keepdims=True), out)
    share[...] = jnp.broadcast_to(out, share.shape)


def final_kernel(share, z_one, z_two, x_one, x_two, control, increment, stage, x_stage, sems):
    members, levels, rows, cols = control.shape
    total = jnp.sum(share[...], axis=0, keepdims=True)
    place = lax.broadcasted_iota(jnp.int32, (1, cols), 1)
    n0, c1, c2, c3 = (jnp.sum(jnp.where(place == i, total, 0.0), axis=1, keepdims=True) for i in range(4))
    bn2 = n0 + EPS
    alpha_one = (n0 + c1) / bn2
    t = (EPS - c1) / bn2
    rr = jnp.maximum((c2 + 2.0 * t * c1 + t * t * n0) / bn2, 0.0)
    beta_sq = rr + EPS
    alpha_two = (rr + jnp.maximum((c3 + 2.0 * t * c2 + t * t * c1) / bn2, 0.0)) / beta_sq
    det = alpha_one * alpha_two - beta_sq
    coef_b = -1.0 / det
    coef_a = (alpha_two - t) / det
    copies = []
    part = stage.shape[0] // (sems.shape[0] - 1)
    for c in range(sems.shape[0] - 1):

        def body(i, _):
            f = c * part + i
            one, two = z_one[f, SWEEPS : SWEEPS + rows, :], z_two[f, SWEEPS : SWEEPS + rows, :]
            stage[f] = coef_a * one + coef_b * two
            return 0

        lax.fori_loop(0, part, body, 0, unroll=True)
        level, first = divmod(c * part, members)
        copies.append(
            pltpu.make_async_copy(
                stage.at[pl.ds(c * part, part)], control.at[pl.ds(first, part), level], sems.at[c]
            )
        )
        copies[-1].start()
    x_stage[...] = coef_a * x_one[...] + coef_b * x_two[...]
    copies.append(pltpu.make_async_copy(x_stage, increment, sems.at[sems.shape[0] - 1]))
    copies[-1].start()
    for copy in copies:
        copy.wait()


def on_device(ensemble, obs_cell, obs_level, innovation, obs_weight):
    members, levels, rows, cols = ensemble.shape
    fields = members * levels
    reach = rows + 2 * HALO
    batch = 32
    strips = fields // 8 + 1
    devices = lax.axis_size("gy") * lax.axis_size("gx")
    hbm = pl.BlockSpec(memory_space=pltpu.HBM)

    def struct(*shape):
        return jax.ShapeDtypeStruct(shape, F32)

    def call(kernel, outs, ins, scratch=(), limit=24, work=2, **kw):
        return pl.pallas_call(
            kernel,
            out_shape=outs,
            in_specs=[VMEM] * ins if isinstance(ins, int) else ins,
            out_specs=jax.tree.map(lambda _: VMEM, outs),
            scratch_shapes=scratch,
            compiler_params=pltpu.CompilerParams(vmem_limit_bytes=limit * 2**20),
            cost_estimate=pl.CostEstimate(flops=work * 10**9, bytes_accessed=10**6, transcendentals=0),
            **kw,
        )

    bands = jnp.asarray(band_matrices(cols), BF16)
    obs = obs_cell.shape
    edge = pltpu.VMEM((members, levels, 16, cols), BF16)
    grid, near, far = call(
        scatter_kernel,
        (struct(2, levels, rows, cols), struct(fields + levels, HALO, cols), struct(fields + levels, HALO, cols)),
        [hbm] * 5,
        [pltpu.VMEM(obs, jnp.int32)] * 2 + [pltpu.VMEM(obs, F32)] * 2 + [edge, edge, pltpu.SemaphoreType.DMA((6,))],
        limit=60,
    )(ensemble, obs_cell, obs_level, innovation, obs_weight)
    near, far = swap(near, "gy", 0), swap(far, "gy", 1)
    main_shape, win_shape = struct(fields, reach, cols), struct(fields // 2, reach, cols)
    g_shape = struct(levels, reach, cols)
    own_shape, end_shape = struct(strips, rows, cols), struct(strips, 2 * HALO, cols)
    mains, wins, near_own, far_own, g_ext, mirror, bands = call(
        own_kernel,
        (
            main_shape,
            win_shape,
            own_shape,
            own_shape,
            g_shape,
            struct(2, fields + levels, HALO, cols),
            jax.ShapeDtypeStruct((2, 2 * cols, SWEEPS * cols), BF16),
        ),
        [hbm, VMEM, hbm],
        [pltpu.VMEM(ensemble.shape, BF16), pltpu.SemaphoreType.DMA((3,))],
    )(ensemble, grid, bands)
    near_own, far_own = swap(near_own, "gx", 0), swap(far_own, "gx", 1)
    work = (
        pltpu.VMEM((batch, reach, cols), F32),
        pltpu.VMEM((SWEEPS, batch * reach, cols), F32),
        pltpu.VMEM((batch * reach, 2 * cols), BF16),
    )
    zm_shape, zw_shape = struct(fields, reach - HALO, cols), struct(fields // 2, reach - HALO, cols)
    state_shape = struct(levels, rows, cols)
    edge_shape = struct(SWEEPS, 2 * fields, 2 * HALO, cols)
    part_shapes = (zm_shape, edge_shape, edge_shape, state_shape)
    ends = pltpu.VMEM((2 * fields, 2 * HALO, cols), F32)
    part = call(
        functools.partial(interior_kernel, batch=batch),
        part_shapes,
        3,
        (pltpu.VMEM((levels, rows, cols), F32), *work),
    )(mains, grid, bands)
    mains, wins, g_ext, near, far = call(
        halo_kernel, (main_shape, win_shape, g_shape, end_shape, end_shape), 7, input_output_aliases={3: 0, 4: 1, 5: 2}
    )(near, far, mirror, mains, wins, g_ext, part[3])
    near, far = swap(near, "gx", 0), swap(far, "gx", 1)
    gbuf = pltpu.VMEM((levels, reach, cols), F32)
    zm_one, _, _, xmain = call(
        edge_kernel, part_shapes, 7, (gbuf, ends, work[2]), input_output_aliases={3: 0, 4: 1, 5: 2, 6: 3}
    )(mains, g_ext, bands, *part)
    win_edge = struct(SWEEPS, fields, 2 * HALO, cols)
    win_parts = (win_shape, zw_shape, win_edge, win_edge, state_shape)
    wins_part = call(
        functools.partial(window_interior_kernel, batch=batch),
        win_parts,
        5,
        (pltpu.VMEM((levels, rows, cols), F32), *work),
        input_output_aliases={0: 0},
    )(wins, grid, near_own, far_own, bands)
    wins, zw_one, _, _, _, x_one, p, near, far, side, sums = call(
        functools.partial(first_kernel, batch=batch),
        (
            *win_parts,
            state_shape,
            state_shape,
            struct(levels + 1, HALO, cols),
            struct(levels + 1, HALO, cols),
            struct(rows, cols),
            struct(2, 8, cols),
        ),
        13,
        (
            gbuf,
            work[2],
            pltpu.VMEM((fields, 2 * HALO, cols), F32),
            *[pltpu.VMEM((strips, reach, cols), F32)] * 2,
        ),
        input_output_aliases={i: i for i in range(5)},
    )(*wins_part, g_ext, grid, near_own, far_own, near, far, bands, xmain)
    near, far = swap(near, "gy", 0), swap(far, "gy", 1)
    *part, zm_one = call(
        functools.partial(second_interior_kernel, batch=batch),
        (*part_shapes, zm_shape),
        5,
        (pltpu.VMEM((levels, rows, cols), F32), *work),
        input_output_aliases={3: 4},
    )(mains, p, bands, zm_one, zw_one)
    x_two, share, zm_two, _, _, _ = call(
        functools.partial(second_kernel, batch=batch),
        (state_shape, struct(devices, cols), *part_shapes),
        13,
        (
            pltpu.VMEM((levels + 1, reach, cols), F32),
            pltpu.VMEM((2, levels, reach, cols), F32),
            *work,
            pltpu.VMEM((levels, rows, cols), F32),
            pltpu.VMEM((fields // 2, reach - HALO, cols), F32),
            ends,
        ),
        input_output_aliases={9: 2, 10: 3, 11: 4, 12: 5},
    )(mains, wins, p, side, near, far, grid, bands, sums, *part)
    share = lax.all_to_all(share, ("gy", "gx"), 0, 0, tiled=True)
    chunks = 8
    return pl.pallas_call(
        final_kernel,
        out_shape=(struct(members, levels, rows, cols), struct(levels, rows, cols)),
        in_specs=[VMEM] * 5,
        out_specs=(hbm, hbm),
        scratch_shapes=[
            pltpu.VMEM((fields, rows, cols), F32),
            pltpu.VMEM((levels, rows, cols), F32),
            pltpu.SemaphoreType.DMA((chunks + 1,)),
        ],
        compiler_params=pltpu.CompilerParams(vmem_limit_bytes=16 * 2**20),
    )(share, zm_one, zm_two, x_one, x_two)


def solution(mesh):
    return jax.shard_map(
        on_device,
        mesh=mesh,
        in_specs=(
            P(None, None, "gy", "gx"),
            P("gy", "gx", None),
            P("gy", "gx", None),
            P("gy", "gx", None),
            P("gy", "gx", None),
        ),
        out_specs=(P(None, None, "gy", "gx"), P(None, "gy", "gx")),
        check_vma=False,
    )
```
